128 devices in a mesh: section: 2 (over x_hi), dp: 16 (over z, y), mp: 4 (over x_lo, core).
Axes of the slice: x: 4 (x_hi: 2, x_lo: 2; x = x_hi * 2 + x_lo), y: 4, z: 4, core: 2. Of those that a mesh axis runs over, the one named last changes fastest.
Arguments:
- text_feats: bfloat16 [16384, 512], P('dp'), may hold values from -48 to 48
- image_feats: bfloat16 [16384, 512], P(('dp', 'mp')), may hold values from -48 to 48
- logit_scale: float32 [1], replicated, may hold values from 10 to 320
- layer_inputs: bfloat16 [2, 16384, 512], P('section', 'dp'), may hold values from -6 to 6
- w_in: bfloat16 [2, 512, 2048], P('section', None, 'mp'), may hold values from -0.25 to 0.25
- w_out: bfloat16 [2, 2048, 512], P('section', 'mp'), may hold values from -0.125 to 0.125
Outputs:
- image_grad: bfloat16 [16384, 512], P(('dp', 'mp'))
- input_grad: bfloat16 [16384, 512], P('dp', 'section')
- w_in_grad: float32 [2, 512, 2048], P('section', 'dp', 'mp')
- w_out_grad_t: float32 [2, 512, 2048], P('section', 'dp', 'mp')
The draws below stay inside these ranges and needn't reach their ends.
All inputs are finite; a program needn't handle non-finite values.
Results may differ from the reference program's by a relative error of at most 0.017.
Values may be sent and summed in bfloat16 or wider, within the bound.
A program may use at most 128 MiB of HBM per device.

```python
import jax
import jax.numpy as jnp
from jax import lax

D = 512
FF = 2048
PAIRS_DEV = 1024
PAIRS = 16384
LAYERS = 2


def joint_feats(key):
    folded = jax.random.fold_in(key, 11)
    key_shared, key_text, key_image, key_scale = jax.random.split(folded, 4)
    shared = jnp.clip(jax.random.normal(key_shared, (PAIRS, D), jnp.float32), -4.0, 4.0)
    text_noise = jnp.clip(jax.random.normal(key_text, (PAIRS, D), jnp.float32), -4.0, 4.0)
    image_noise = jnp.clip(jax.random.normal(key_image, (PAIRS, D), jnp.float32), -4.0, 4.0)
    text_rows = shared + text_noise
    image_rows = shared + image_noise
    return (text_rows, image_rows)


def draw_text_feats(key, part):
    text_rows, image_rows = joint_feats(key)
    return text_rows.astype(jnp.bfloat16)


def draw_image_feats(key, part):
    text_rows, image_rows = joint_feats(key)
    return image_rows.astype(jnp.bfloat16)


def draw_logit_scale(key, part):
    folded = jax.random.fold_in(key, 23)
    return jax.random.uniform(folded, (1,), jnp.float32, 10.0, 30.0)


def block_levels(rng, dims, cuts, smallest, top_value):
    factor_of, own = 1.0, jax.random.fold_in(rng, 6)
    for dim, parts in cuts:
        steps = jnp.exp(jax.random.uniform(jax.random.fold_in(own, dim), (parts,), jnp.float32, smallest / len(cuts), top_value / len(cuts)))
        factor_of = factor_of * jnp.repeat(steps, dims[dim] // parts).reshape([-1 if axis == dim else 1 for axis in range(len(dims))])
    return factor_of


def gaussian(key, extent, deviation, limit, cuts=(), kind=jnp.bfloat16):
    entries = jax.random.normal(key, extent, jnp.float32) * deviation
    if len(cuts) > 0:
        entries = block_levels(key, extent, cuts, -0.22, 0.18) * entries
    return jnp.clip(entries, min=-limit, max=limit).astype(kind)


def setup_inputs(seed: int = 0) -> dict:
    splits = jax.random.split(jax.random.key(seed), 7)
    text_feats = draw_text_feats(jax.random.fold_in(splits[6], 71), 0)
    image_feats = draw_image_feats(jax.random.fold_in(splits[6], 71), 0)
    logit_scale = draw_logit_scale(jax.random.fold_in(splits[6], 71), 0)
    layer_inputs = gaussian(splits[3], (LAYERS, PAIRS, D), 1.0, 6.0, ((0, 2), (1, 16)))
    w_in = gaussian(splits[4], (LAYERS, D, FF), D ** -0.5, 0.25, ((0, 2), (2, 4)))
    w_out = gaussian(splits[5], (LAYERS, FF, D), FF ** -0.5, 0.125, ((0, 2), (1, 4)))
    return {"text_feats": text_feats, "image_feats": image_feats, "logit_scale": logit_scale, "layer_inputs": layer_inputs, "w_in": w_in, "w_out": w_out}


def unit_rows(values):
    wide = values.astype(jnp.float32)
    length = jnp.sqrt(lax.optimization_barrier(jnp.sum(wide * wide, axis=1, keepdims=True)) + 1.0)
    return (wide / length, length)

def unit_backward(unit, length, grad_unit):
    return (grad_unit - unit * lax.optimization_barrier(jnp.sum(unit * grad_unit, axis=1, keepdims=True))) / length

def quick_gelu(values):
    return values * jax.nn.sigmoid(1.702 * values)

def quick_slope(values):
    sigm = jax.nn.sigmoid(1.702 * values)
    return sigm + 1.702 * values * sigm * (1.0 - sigm)

def reference(text_feats, image_feats, logit_scale, layer_inputs, w_in, w_out):
    logit_mult = logit_scale[0]
    text_unit, text_length = unit_rows(text_feats)
    image_unit, image_length = unit_rows(image_feats)
    text_low = text_unit.astype(jnp.bfloat16)
    image_low = image_unit.astype(jnp.bfloat16)
    block_count = PAIRS // PAIRS_DEV
    text_blocks = text_low.reshape(block_count, PAIRS_DEV, D)
    block_ids = jnp.arange(block_count, dtype=jnp.int32)
    column_ids = jnp.arange(PAIRS, dtype=jnp.int32)

    def stats_step(state_pair, text_block):
        column_peak, column_total = state_pair
        scores = logit_mult * jnp.dot(text_block, image_low.T, preferred_element_type=jnp.float32)
        row_peak = lax.optimization_barrier(jnp.max(scores, axis=1))
        row_total = lax.optimization_barrier(jnp.sum(jnp.exp(scores - row_peak[:, None]), axis=1))
        new_peak = jnp.maximum(column_peak, lax.optimization_barrier(jnp.max(scores, axis=0)))
        column_total = column_total * jnp.exp(column_peak - new_peak) + lax.optimization_barrier(jnp.sum(jnp.exp(scores - new_peak[None, :]), axis=0))
        return ((new_peak, column_total), (row_peak, row_total))
    start_pair = (jnp.full((PAIRS,), -1e+30, jnp.float32), jnp.zeros((PAIRS,), jnp.float32))
    (column_peak, column_total), (row_peaks, row_totals) = lax.scan(stats_step, start_pair, text_blocks)

    def grad_step(image_acc, inputs):
        text_block, row_peak, row_total, block_id = inputs
        scores = logit_mult * jnp.dot(text_block, image_low.T, preferred_element_type=jnp.float32)
        text_ids = (block_id * PAIRS_DEV + jnp.arange(PAIRS_DEV, dtype=jnp.int32)).astype(jnp.int32)
        positive = (text_ids[:, None] == column_ids[None, :]).astype(jnp.float32)
        row_prob = jnp.exp(scores - row_peak[:, None]) / row_total[:, None]
        column_prob = jnp.exp(scores - column_peak[None, :]) / column_total[None, :]
        score_grad = (0.5 * (row_prob + column_prob) - positive).astype(jnp.bfloat16)
        text_part = logit_mult * jnp.dot(score_grad, image_low, preferred_element_type=jnp.float32)
        image_acc = image_acc + logit_mult * jnp.dot(score_grad.T, text_block, preferred_element_type=jnp.float32)
        return (image_acc, text_part)
    image_unit_grad, text_parts = lax.scan(grad_step, jnp.zeros((PAIRS, D), jnp.float32), (text_blocks, row_peaks, row_totals, block_ids))
    text_unit_grad = text_parts.reshape(PAIRS, D)
    top_grad = unit_backward(text_unit, text_length, text_unit_grad).astype(jnp.bfloat16)
    image_grad = unit_backward(image_unit, image_length, image_unit_grad).astype(jnp.bfloat16)
    layer_grad = top_grad
    first_grads = []
    second_grads = []
    for layer in reversed(range(LAYERS)):
        inputs_now = layer_inputs[layer]
        pre_act = jnp.dot(inputs_now, w_in[layer], preferred_element_type=jnp.float32)
        activation = quick_gelu(pre_act).astype(jnp.bfloat16)
        back_grad = jnp.dot(layer_grad, w_out[layer].T, preferred_element_type=jnp.float32)
        pre_grad = (back_grad * quick_slope(pre_act)).astype(jnp.bfloat16)
        first_grads.insert(0, jnp.dot(inputs_now.T, pre_grad, preferred_element_type=jnp.float32))
        second_grads.insert(0, jnp.dot(layer_grad.T, activation, preferred_element_type=jnp.float32))
        layer_grad = (layer_grad.astype(jnp.float32) + jnp.dot(pre_grad, w_in[layer].T, preferred_element_type=jnp.float32)).astype(jnp.bfloat16)
    return (image_grad, layer_grad, jnp.stack(first_grads), jnp.stack(second_grads))
```

```python
import jax
import jax.numpy as jnp
from jax import lax
from jax.experimental import pallas as pl
from jax.experimental.pallas import tpu as pltpu
from jax.sharding import PartitionSpec as P

MESH = pl.DeviceIdType.MESH
F32 = jnp.float32
BF16 = jnp.bfloat16
GELU = 1.702
LOG2E = 1.4426950408889634
LANES = 128
CORES = 2


def unit_rows(values):
    wide = values.astype(F32)
    length = jnp.sqrt(jnp.sum(wide * wide, axis=1, keepdims=True) + 1.0)
    return (wide / length, length)


def unit_backward(unit, length, grad_unit):
    return (grad_unit - unit * jnp.sum(unit * grad_unit, axis=1, keepdims=True)) / length


def dot_nn(a, b):
    return lax.dot_general(a, b, (((1,), (0,)), ((), ())), preferred_element_type=F32)


def dot_nt(a, b):
    return lax.dot_general(a, b, (((1,), (1,)), ((), ())), preferred_element_type=F32)


def dot_tn(a, b):
    return lax.dot_general(a, b, (((0,), (0,)), ((), ())), preferred_element_type=F32)


def tile(index, size):
    return pl.ds(pl.multiple_of(index * size, size), size)


def make_kernel(n_sec, n_dp, n_mp):
    chips = n_mp // CORES
    line = n_sec * chips
    n_el = n_sec * n_mp

    def kernel(
        text, image, scale_ref, hidden, w_in, w_out,
        image_out, input_out, first_out, second_out,
        text_low, cols, scores, sgrad, row_max, row_lse, col_lse, row_st, row_rx, col_st, col_rx,
        wi_all, wo_all, h_own, t_full, t_keep, t_sx, t_sr, t_tx, t_rx,
        g_st, g_all, g_acc, in_st, act_all, slope_all, pre_all,
        w_tx, w_rx, i_tx, i_rx,
        gat_s, gat_r, cs_s, cs_r, rs_s, rs_r, ww_s, ww_r, h_s, h_r,
        ts_s, ts_r, tc_s, tc_r, gs_s, gs_r, gr_s, in_s, in_r, ir_s,
        w_s, w_r, im_s, im_r, io_s, io_r,
    ):
        s = lax.axis_index("section")
        d = lax.axis_index("dp")
        m = lax.axis_index("mp")
        rows, feats = text.shape
        own = image.shape[0]
        half = own // n_sec
        chunk = rows // n_el
        pair = rows // line
        share = feats // n_dp
        width = feats // n_sec
        mult = scale_ref[0]
        mult2 = mult * LOG2E
        core = lax.rem(m, CORES)
        sib = 1 - core
        spot = s * chips + m // CORES
        e = s * n_mp + m

        def at(place, who):
            return {"section": place // chips, "mp": lax.rem(place, chips) * CORES + who}

        def far(step):
            return lax.rem(spot + step, line)

        def copy(src, dst, send, recv, where):
            return pltpu.make_async_remote_copy(
                src_ref=src, dst_ref=dst, send_sem=send, recv_sem=recv,
                device_id=where, device_id_type=MESH,
            )

        def arrived(ref, recv):
            copy(ref, ref, h_s, recv, at(spot, sib)).wait_recv()

        def others(mine, count):
            return [lax.rem(mine + k, count) for k in range(1, count)]

        def sources(mine, count):
            return [lax.rem(mine + count - k, count) for k in range(1, count)]

        sent = []

        def push(*args):
            c = copy(*args)
            c.start()
            sent.append(c)

        with jax.named_scope("a_barrier"):
            barrier = pltpu.get_barrier_semaphore()
            for p in others(d, n_dp):
                pl.semaphore_signal(barrier, inc=1, device_id={"dp": p}, device_id_type=MESH)
            for q in others(e, n_el):
                pl.semaphore_signal(
                    barrier, inc=1, device_id={"section": q // n_mp, "mp": lax.rem(q, n_mp)},
                    device_id_type=MESH,
                )
            own_unit, _ = unit_rows(image[tile(s, half), :])
            cols[tile(d, half), :] = own_unit.astype(BF16)
            h_own[s] = hidden[tile(e, chunk), :]
            wi_all[e] = w_in[...]
            wo_all[e] = w_out[...]
            pl.semaphore_wait(barrier, n_dp + n_el - 2)

        for p in others(d, n_dp):
            push(cols.at[tile(d, half), :], cols.at[tile(d, half), :], gat_s.at[p], gat_r.at[d],
                 {"dp": p})

        mate = (1 - s) * n_mp + m
        push(hidden.at[tile(mate, chunk), :], h_own.at[s], h_s, h_r, {"section": 1 - s})
        ww = ((w_in, wi_all), (w_out, wo_all))
        for which in (0, 1):
            push(ww[which][0], ww[which][1].at[e], ww_s.at[which, 1], ww_r.at[which, e],
                 at(far(line - 1), core))
            push(ww[1 - which][0], ww[1 - which][1].at[e], ww_s.at[1 - which, 2],
                 ww_r.at[1 - which, e], at(far(1), core))
        for which in (0, 1):
            push(ww[which][0], ww[which][1].at[e], ww_s.at[which, 0], ww_r.at[which, e],
                 at(spot, sib))

        def relay_weight(which, step, slot, onward=None):
            index = far(step) * CORES + core
            buf = ww[which][1].at[index]
            arrived(buf, ww_r.at[which, index])
            if onward is not None:
                push(buf, buf, ww_s.at[which, 3], ww_r.at[which, index], at(far(onward), core))
            push(buf, buf, ww_s.at[which, slot], ww_r.at[which, index], at(spot, sib))

        def sigmoid(pre):
            return 1.0 / (1.0 + jnp.exp(-GELU * pre))

        with jax.named_scope("b_pre"):
            @pl.loop(0, line)
            def _(r):
                unit, _ = unit_rows(text[tile(r, pair), :])
                text_low[tile(r, pair), :] = unit.astype(BF16)

            @pl.loop(0, line)
            def _(r):
                pre = dot_nn(hidden[tile(r, pair), :], w_in[...])
                sigm = sigmoid(pre)
                act_all[tile(r, pair), :] = (pre * sigm).astype(BF16)
                slope_all[tile(r, pair), :] = sigm + GELU * pre * sigm * (1.0 - sigm)

        row_max[...] = jnp.full(row_max.shape, -1e30, F32)

        def block_scores(p):
            piece = cols[tile(p, half), :]

            def part(r, peak):
                value = mult2 * dot_nt(text_low[tile(r, pair), :], piece)
                scores[p, tile(r, pair), :] = value
                row_max[tile(r, pair), :] = jnp.maximum(row_max[tile(r, pair), :], value)
                return jnp.maximum(peak, jnp.max(value, axis=0, keepdims=True))

            peak = lax.fori_loop(0, line, part, jnp.full((1, half), -1e30, F32))

            def total(r, acc):
                value = scores[p, tile(r, pair), :]
                return acc + jnp.sum(jnp.exp2(value - peak), axis=0, keepdims=True)

            acc = lax.fori_loop(0, line, total, jnp.zeros((1, half), F32))
            col_st[pl.ds(p, 1), :] = peak
            col_st[pl.ds(n_dp + p, 1), :] = acc

        with jax.named_scope("c_blocks"):
            block_scores(d)
            for k, p in enumerate(sources(d, n_dp)):
                arrived(cols.at[tile(p, half), :], gat_r.at[p])
                block_scores(p)
                if k == n_dp // 2:
                    relay_weight(0, 1, 4, line - 1)
                    relay_weight(1, line - 1, 4, 1)

        with jax.named_scope("d_colsend"):
            col_rx[d] = col_st[...]
            for p in others(d, n_dp):
                push(col_st, col_rx.at[d], cs_s.at[p], cs_r.at[d], {"dp": p})

        with jax.named_scope("e_rowstat"):
            for r in range(n_el):
                part = pl.ds(r * chunk, chunk)
                peak = jnp.max(row_max[part, :], axis=1, keepdims=True)

                def total(p, acc):
                    return acc + jnp.exp2(scores[p, part, :] - peak)

                acc = lax.fori_loop(0, n_dp, total, jnp.zeros((chunk, LANES), F32))
                acc = jnp.sum(acc, axis=1, keepdims=True)
                row_st[r : r + 1, :] = jnp.broadcast_to(peak, (chunk, LANES)).T[0:1, :]
                row_st[n_el + r : n_el + r + 1, :] = jnp.broadcast_to(acc, (chunk, LANES)).T[0:1, :]
            row_rx[e] = row_st[...]
            for q in others(e, n_el):
                push(row_st, row_rx.at[e], rs_s.at[q], rs_r.at[e],
                     {"section": q // n_mp, "mp": lax.rem(q, n_mp)})

        def merge(rx, count, n):
            peak = rx[0, 0:n, :]
            for k in range(1, count):
                peak = jnp.maximum(peak, rx[k, 0:n, :])
            acc = jnp.zeros(peak.shape, F32)
            for k in range(count):
                acc = acc + rx[k, n : 2 * n, :] * jnp.exp2(rx[k, 0:n, :] - peak)
            return peak + (jnp.log(acc) * LOG2E + 1.0)

        with jax.named_scope("f_relay"):
            relay_weight(1, 1, 5)
            relay_weight(0, line - 1, 5)

        with jax.named_scope("f_merge"):
            for p in sources(d, n_dp):
                arrived(col_rx.at[p], cs_r.at[p])
            col_lse[...] = merge(col_rx, n_dp, n_dp)
            for q in sources(e, n_el):
                arrived(row_rx.at[q], rs_r.at[q])
            merged = merge(row_rx, n_el, n_el)
            for r in range(n_el):
                row_lse[r * chunk : (r + 1) * chunk, :] = jnp.broadcast_to(
                    merged[r : r + 1, :], (LANES, chunk)).T

        def score_rows(r):
            base = row_lse[tile(r, pair), :]
            for p in range(n_dp):
                value = scores[p, tile(r, pair), :]
                both = jnp.exp2(value - base) + jnp.exp2(value - col_lse[p : p + 1, :])
                sgrad[tile(r, pair), p * half : (p + 1) * half] = both.astype(BF16)

            @pl.when(r == m)
            def _():
                line_at = tile(m * n_sec + s, half)
                value = scores[d, line_at, :]
                both = jnp.exp2(value - row_lse[line_at, :]) + jnp.exp2(
                    value - col_lse[pl.ds(d, 1), :])
                diagonal = lax.broadcasted_iota(jnp.int32, (half, half), 0) == (
                    lax.broadcasted_iota(jnp.int32, (half, half), 1))
                sgrad[line_at, tile(d, half)] = (
                    both - jnp.where(diagonal, 1.0, 0.0)).astype(BF16)

        def join(where):
            arrived(t_sr.at[where], ts_r.at[where])
            return t_keep[where] + t_sr[where].astype(F32)

        hops = (2, 3, 1, 0) if line == 4 else tuple(range(line - 1, -1, -1))

        def t_send(where, slot):
            return copy(t_tx.at[where], t_rx.at[spot], tc_s.at[slot], tc_r.at[spot],
                        at(where, core))

        with jax.named_scope("g_scorerows"):
            for i, hop in enumerate(hops):
                where = far(hop)
                score_rows(where)
                t_full[...] = dot_nn(sgrad[tile(where, pair), :], cols[...])
                t_sx[where] = t_full[tile(sib, chunk), :].astype(BF16)
                push(t_sx.at[where], t_sr.at[where], ts_s.at[i], ts_r.at[where], at(spot, sib))
                t_keep[where] = t_full[tile(core, chunk), :]
                if i > 0:
                    last = far(hops[i - 1])
                    t_tx[last] = join(last).astype(BF16)
                    push(t_tx.at[last], t_rx.at[spot], tc_s.at[i], tc_r.at[spot],
                         at(last, core))

        def image_part(p):
            return dot_tn(sgrad[:, tile(p, half)], text_low[...])

        with jax.named_scope("h_image"):
            for p in others(d, n_dp):
                i_tx[p] = image_part(p).astype(BF16)
                push(i_tx.at[p], i_rx.at[d], im_s.at[p], im_r.at[d], {"dp": p})

        mine = tile(e, chunk)

        with jax.named_scope("i_topgrad"):
            total = join(spot)
            for hop in hops[:-1]:
                where = far(hop)
                arrived(t_rx.at[where], tc_r.at[where])
                total = total + t_rx[where].astype(F32)
            unit, length = unit_rows(text[mine, :])
            g_st[n_sec - 1] = unit_backward(unit, length, mult * total).astype(BF16)

        with jax.named_scope("j_weights"):
            arrived(h_own.at[1 - s], h_r)
            relay_weight(0, 2, 6)
            relay_weight(1, 2, 6)
            for step in range(line):
                index = far(step) * CORES + sib
                for which in (0, 1):
                    arrived(ww[which][1].at[index], ww_r.at[which, index])

        def spread(layer):
            for c in range(chips):
                place = layer * chips + c

                @pl.when(spot != place)
                def _():
                    copy(g_st.at[layer], g_all.at[e], gs_s.at[layer, c], gs_r.at[e],
                         at(place, core)).start()

            @pl.when(s == layer)
            def _():
                g_all[e] = g_st[layer]
                copy(g_st.at[layer], g_all.at[e], gs_s.at[layer, chips], gs_r.at[e],
                     at(spot, sib)).start()

        def drain_spread(layer):
            for c in range(chips):
                place = layer * chips + c

                @pl.when(spot != place)
                def _():
                    copy(g_st.at[layer], g_all.at[e], gs_s.at[layer, c], gs_r.at[e],
                         at(place, core)).wait_send()

            @pl.when(s == layer)
            def _():
                copy(g_st.at[layer], g_all.at[e], gs_s.at[layer, chips], gs_r.at[e],
                     at(spot, sib)).wait_send()

        def feed_forward(layer):
            spread(layer)
            g_acc[...] = g_st[layer].astype(F32)

            @pl.loop(0, n_mp)
            def _(j):
                index = layer * n_mp + j
                pre = dot_nn(h_own[layer], wi_all[index])
                back = dot_nt(g_st[layer], wo_all[index])
                sigm = sigmoid(pre)
                grad = (back * (sigm + GELU * pre * sigm * (1.0 - sigm))).astype(BF16)
                g_acc[...] += dot_nt(grad, wi_all[index])

            if layer > 0:
                g_st[layer - 1] = g_acc[...].astype(BF16)

        def slab(k):
            return input_out.at[tile(k, chunk), :]

        with jax.named_scope("k_ffn"):
            for layer in range(n_sec - 1, -1, -1):
                feed_forward(layer)

        with jax.named_scope("l_inspread"):
            for t in range(n_sec):
                in_st[t] = g_acc[:, t * width : (t + 1) * width].astype(BF16)
            input_out[mine, :] = in_st[s]
            push(in_st.at[s], slab(e), in_s.at[0], in_r.at[e], at(spot, sib))
            for hop in hops[:-1]:
                where = far(hop)
                push(in_st.at[where // chips], slab(e), in_s.at[hop], in_r.at[e],
                     at(where, core))

        def weight_rows(k):
            back = dot_nt(g_all[k], w_out[...])
            pre_all[tile(k, chunk), :] = (back * slope_all[tile(k, chunk), :]).astype(BF16)

        with jax.named_scope("m_weightrows"):
            weight_rows(e)
            for hop in (1, 3, 2) if line == 4 else range(1, line):
                index = far(hop) * CORES + core
                arrived(g_all.at[index], gs_r.at[index])
                push(g_all.at[index], g_all.at[index], gr_s.at[hop], gs_r.at[index],
                     at(spot, sib))
                weight_rows(index)
            for hop in (0, 1, 3, 2) if line == 4 else range(line):
                index = far(hop) * CORES + sib
                arrived(g_all.at[index], gs_r.at[index])
                weight_rows(index)

        def send_weights(which):
            for p in others(d, n_dp):
                push(w_tx.at[p, which], w_rx.at[d, which], w_s.at[which, p], w_r.at[which, d],
                     {"dp": p})

        with jax.named_scope("n_wgrad"):
            g_rows = g_all[...].reshape(rows, feats)
            grad_second = dot_tn(g_rows, act_all[...])
            for p in range(n_dp):
                w_tx[p, 1] = grad_second[p * share : (p + 1) * share, :].astype(BF16)
            send_weights(1)
            grad_first = dot_tn(hidden[...], pre_all[...])
            for p in range(n_dp):
                w_tx[p, 0] = grad_first[p * share : (p + 1) * share, :].astype(BF16)
            send_weights(0)

        with jax.named_scope("o_inrelay"):
            for hop in hops[:-1]:
                index = far(hop) * CORES + core
                arrived(slab(index), in_r.at[index])
                push(slab(index), slab(index), ir_s.at[hop], in_r.at[index], at(spot, sib))

        with jax.named_scope("p_image"):
            image_half = tile(s, half)
            total = image_part(d)
            for p in sources(d, n_dp):
                arrived(i_rx.at[p], im_r.at[p])
                total = total + i_rx[p].astype(F32)
            unit, length = unit_rows(image[image_half, :])
            image_out[image_half, :] = unit_backward(unit, length, mult * total).astype(BF16)
            push(image_out.at[image_half, :], image_out.at[image_half, :], io_s, io_r,
                 {"section": 1 - s})

        with jax.named_scope("q_wsum"):
            for which, out in ((1, second_out), (0, first_out)):
                total = w_tx[d, which].astype(F32)
                for p in sources(d, n_dp):
                    arrived(w_rx.at[p, which], w_r.at[which, p])
                    total = total + w_rx[p, which].astype(F32)
                out[...] = total

        with jax.named_scope("r_drain"):
            for step in range(line):
                index = far(step) * CORES + sib
                arrived(slab(index), in_r.at[index])
            arrived(image_out.at[tile(1 - s, half), :], io_r)
            for c in sent:
                c.wait_send()
            for layer in range(n_sec):
                drain_spread(layer)

    return kernel


def solution(mesh):
    n_sec, n_dp, n_mp = mesh.shape["section"], mesh.shape["dp"], mesh.shape["mp"]

    def body(text, image, scale, hidden, w_in, w_out):
        rows, feats = text.shape
        own = image.shape[0]
        hid = w_in.shape[2]
        half, share = own // n_sec, feats // n_dp
        columns = half * n_dp
        line = n_sec * n_mp // CORES
        n_el = n_sec * n_mp
        chunk = rows // n_el
        dma = pltpu.SemaphoreType.DMA
        vmem = pl.BlockSpec(memory_space=pltpu.VMEM)
        out = pl.pallas_call(
            make_kernel(n_sec, n_dp, n_mp),
            out_shape=(
                jax.ShapeDtypeStruct((own, feats), BF16),
                jax.ShapeDtypeStruct((rows, feats // n_sec), BF16),
                jax.ShapeDtypeStruct((share, hid), F32),
                jax.ShapeDtypeStruct((share, hid), F32),
            ),
            in_specs=[vmem, vmem, pl.BlockSpec(memory_space=pltpu.SMEM), vmem, vmem, vmem],
            out_specs=(vmem,) * 4,
            scratch_shapes=[
                pltpu.VMEM((rows, feats), BF16),
                pltpu.VMEM((columns, feats), BF16),
                pltpu.VMEM((n_dp, rows, half), F32),
                pltpu.VMEM((rows, columns), BF16),
                pltpu.VMEM((rows, LANES), F32),
                pltpu.VMEM((rows, LANES), F32),
                pltpu.VMEM((n_dp, half), F32),
                pltpu.VMEM((2 * n_el, chunk), F32),
                pltpu.VMEM((n_el, 2 * n_el, chunk), F32),
                pltpu.VMEM((2 * n_dp, half), F32),
                pltpu.VMEM((n_dp, 2 * n_dp, half), F32),
                pltpu.VMEM((n_el, feats, hid), BF16),
                pltpu.VMEM((n_el, hid, feats), BF16),
                pltpu.VMEM((n_sec, chunk, feats), BF16),
                pltpu.VMEM((CORES * chunk, feats), F32),
                pltpu.VMEM((line, chunk, feats), F32),
                pltpu.VMEM((line, chunk, feats), BF16),
                pltpu.VMEM((line, chunk, feats), BF16),
                pltpu.VMEM((line, chunk, feats), BF16),
                pltpu.VMEM((line, chunk, feats), BF16),
                pltpu.VMEM((n_sec, chunk, feats), BF16),
                pltpu.VMEM((n_el, chunk, feats), BF16),
                pltpu.VMEM((chunk, feats), F32),
                pltpu.VMEM((n_sec, chunk, feats // n_sec), BF16),
                pltpu.VMEM((rows, hid), BF16),
                pltpu.VMEM((rows, hid), F32),
                pltpu.VMEM((rows, hid), BF16),
                pltpu.VMEM((n_dp, 2, share, hid), BF16),
                pltpu.VMEM((n_dp, 2, share, hid), BF16),
                pltpu.VMEM((n_dp, half, feats), BF16),
                pltpu.VMEM((n_dp, half, feats), BF16),
                dma((n_dp,)), dma((n_dp,)),
                dma((n_dp,)), dma((n_dp,)),
                dma((n_el,)), dma((n_el,)),
                dma((2, 7)), dma((2, n_el)),
                dma, dma,
                dma((line,)), dma((line,)),
                dma((line,)), dma((line,)),
                dma((n_sec, line + 1)), dma((n_el,)),
                dma((line,)),
                dma((line,)), dma((n_el,)),
                dma((line,)),
                dma((2, n_dp)), dma((2, n_dp)),
                dma((n_dp,)), dma((n_dp,)),
                dma, dma,
            ],
            compiler_params=pltpu.CompilerParams(
                collective_id=0, has_side_effects=True, vmem_limit_bytes=63000000
            ),
        )(text, image, scale, hidden[0], w_in[0], w_out[0])
        image_grad, input_grad, first, second = out
        return (image_grad, input_grad, first[None], second[None])

    return jax.shard_map(
        body,
        mesh=mesh,
        in_specs=(
            P("dp", None),
            P(("dp", "mp"), None),
            P(),
            P("section", "dp", None),
            P("section", None, "mp"),
            P("section", "mp", None),
        ),
        out_specs=(
            P(("dp", "mp"), None),
            P("dp", "section"),
            P("section", "dp", "mp"),
            P("section", "dp", "mp"),
        ),
        check_vma=False,
    )
```

```python
import jax
import jax.numpy as jnp
from jax import lax
from jax.experimental import pallas as pl
from jax.experimental.pallas import tpu as pltpu
from jax.sharding import PartitionSpec as P

MESH = pl.DeviceIdType.MESH
F32 = jnp.float32
BF16 = jnp.bfloat16
GELU = 1.702
LOG2E = 1.4426950408889634
LANES = 128
CORES = 2
RING = 4


def unit_rows(values):
    wide = values.astype(F32)
    length = jnp.sqrt(jnp.sum(wide * wide, axis=1, keepdims=True) + 1.0)
    return (wide / length, length)


def unit_backward(unit, length, grad_unit):
    return (grad_unit - unit * jnp.sum(unit * grad_unit, axis=1, keepdims=True)) / length


def dot_nn(a, b):
    return lax.dot_general(a, b, (((1,), (0,)), ((), ())), preferred_element_type=F32)


def dot_nt(a, b):
    return lax.dot_general(a, b, (((1,), (1,)), ((), ())), preferred_element_type=F32)


def dot_tn(a, b):
    return lax.dot_general(a, b, (((0,), (0,)), ((), ())), preferred_element_type=F32)


def tile(index, size):
    return pl.ds(pl.multiple_of(index * size, size), size)


def make_kernel(n_sec, n_dp, n_mp):
    chips = n_mp // CORES
    line = n_sec * chips
    n_el = n_sec * n_mp

    def kernel(
        text, image, scale_ref, hidden, w_in, w_out,
        image_out, input_out, first_out, second_out,
        text_low, cols, scores, sgrad, row_max, row_sum, row_lse, col_lse, row_st, row_rx, col_st, col_rx,
        wi_all, wo_all, h_own, t_full, t_keep, t_sx, t_sr, t_tx, t_rx,
        g_st, g_all, g_acc, in_st, act_all, slope_all, pre_all,
        w_tx, w_rx, i_tx, i_rx, i_own,
        gat_s, gat_r, cs_s, cs_r, rs_s, rs_r, ww_s, ww_r, h_s, h_r,
        ts_s, ts_r, tc_s, tc_r, gs_s, gs_r, gr_s, in_s, in_r, ir_s,
        w_s, w_r, im_s, im_r, io_s, io_r,
    ):
        s = lax.axis_index("section")
        d = lax.axis_index("dp")
        m = lax.axis_index("mp")
        rows, feats = text.shape
        own = image.shape[0]
        half = own // n_sec
        chunk = rows // n_el
        pair = rows // line
        share = feats // n_dp
        width = feats // n_sec
        mult = scale_ref[0]
        mult2 = mult * LOG2E
        core = lax.rem(m, CORES)
        sib = 1 - core
        spot = s * chips + m // CORES
        e = s * n_mp + m

        def at(place, who):
            return {"section": place // chips, "mp": lax.rem(place, chips) * CORES + who}

        def far(step):
            return lax.rem(spot + step, line)

        def copy(src, dst, send, recv, where):
            return pltpu.make_async_remote_copy(
                src_ref=src, dst_ref=dst, send_sem=send, recv_sem=recv,
                device_id=where, device_id_type=MESH,
            )

        def arrived(ref, recv):
            copy(ref, ref, h_s, recv, at(spot, sib)).wait_recv()

        def shift(step):
            dz, dy = step[0] % RING, step[1] % RING
            z = lax.rem(d // RING + dz, RING)
            return z * RING + lax.rem(lax.rem(d, RING) + dy, RING)

        def slot(step):
            return (step[0] % RING) * RING + step[1] % RING

        steps = [(a, b) for a in range(RING) for b in range(RING)]

        def away(step):
            return (-step[0] % RING, -step[1] % RING)

        def others(mine, count):
            return [lax.rem(mine + k, count) for k in range(1, count)]

        def sources(mine, count):
            return [lax.rem(mine + count - k, count) for k in range(1, count)]

        sent = []

        def push(*args):
            c = copy(*args)
            c.start()
            sent.append(c)

        with jax.named_scope("a_barrier"):
            barrier = pltpu.get_barrier_semaphore()
            for p in others(d, n_dp):
                pl.semaphore_signal(barrier, inc=1, device_id={"dp": p}, device_id_type=MESH)
            for q in others(e, n_el):
                pl.semaphore_signal(
                    barrier, inc=1, device_id={"section": q // n_mp, "mp": lax.rem(q, n_mp)},
                    device_id_type=MESH,
                )
            own_unit, _ = unit_rows(image[tile(s, half), :])
            cols[0:half, :] = own_unit.astype(BF16)
            h_own[s] = hidden[tile(e, chunk), :]
            wi_all[e] = w_in[...]
            wo_all[e] = w_out[...]
            pl.semaphore_wait(barrier, n_dp + n_el - 2)

        quarter = half // 4
        spans = {"A": (0, 2), "B": (2, 2), "A0": (0, 1), "A1": (1, 1), "B0": (2, 1), "B1": (3, 1)}
        ahead = {"Y-": (0, -1), "Y+": (0, 1), "Z-": (-1, 0), "Z+": (1, 0)}
        passed = []

        def piece_of(step, name):
            first, count = spans[name]
            base = slot(step) * half + first * quarter
            return cols.at[base : base + count * quarter, :]

        def forward(step, name, *directions):
            for way in directions:
                move = ahead[way]
                lands = (step[0] - move[0], step[1] - move[1])
                c = copy(piece_of(step, name), piece_of(lands, name), gat_s.at[len(passed)],
                         gat_r.at[slot(lands), spans[name][0]], {"dp": shift(move)})
                c.start()
                passed.append(c)

        def landed(step, name):
            arrived(piece_of(step, name), gat_r.at[slot(step), spans[name][0]])

        for way in ("Y-", "Y+"):
            forward((0, 0), "A", way)
        for way in ("Z-", "Z+"):
            forward((0, 0), "B", way)
        for way in ("Y-", "Y+"):
            forward((0, 0), "B", way)
        for way in ("Z-", "Z+"):
            forward((0, 0), "A", way)

        mate = (1 - s) * n_mp + m
        push(hidden.at[tile(mate, chunk), :], h_own.at[s], h_s, h_r, {"section": 1 - s})
        ww = ((w_in, wi_all), (w_out, wo_all))
        for which in (0, 1):
            push(ww[which][0], ww[which][1].at[e], ww_s.at[which, 1], ww_r.at[which, e],
                 at(far(line - 1), core))
            push(ww[1 - which][0], ww[1 - which][1].at[e], ww_s.at[1 - which, 2],
                 ww_r.at[1 - which, e], at(far(1), core))
        for which in (0, 1):
            push(ww[which][0], ww[which][1].at[e], ww_s.at[which, 0], ww_r.at[which, e],
                 at(spot, sib))

        def relay_weight(which, step, slot, onward=None):
            index = far(step) * CORES + core
            buf = ww[which][1].at[index]
            arrived(buf, ww_r.at[which, index])
            if onward is not None:
                push(buf, buf, ww_s.at[which, 3], ww_r.at[which, index], at(far(onward), core))
            push(buf, buf, ww_s.at[which, slot], ww_r.at[which, index], at(spot, sib))

        def sigmoid(pre):
            return 1.0 / (1.0 + jnp.exp(-GELU * pre))

        with jax.named_scope("b_pre"):
            @pl.loop(0, line)
            def _(r):
                unit, _ = unit_rows(text[tile(r, pair), :])
                text_low[tile(r, pair), :] = unit.astype(BF16)

            @pl.loop(0, line)
            def _(r):
                pre = dot_nn(hidden[tile(r, pair), :], w_in[...])
                sigm = sigmoid(pre)
                act_all[tile(r, pair), :] = (pre * sigm).astype(BF16)
                slope_all[tile(r, pair), :] = sigm + GELU * pre * sigm * (1.0 - sigm)

        def pair_scores(one, two, fresh):
            piece = jnp.concatenate(
                [cols[slot(k) * half : (slot(k) + 1) * half, :] for k in (one, two)], axis=0)
            peak = total = None
            for r in range(line):
                part = pl.ds(r * pair, pair)
                value = mult2 * dot_nt(text_low[part, :], piece)
                left, right = value[:, 0:half], value[:, half : 2 * half]
                scores[slot(one), part, :] = left
                scores[slot(two), part, :] = right
                best = jnp.maximum(left, right)
                if not fresh:
                    best = jnp.maximum(best, row_max[part, :])
                mass = jnp.exp2(left - best) + jnp.exp2(right - best)
                if not fresh:
                    mass = mass + row_sum[part, :] * jnp.exp2(row_max[part, :] - best)
                row_max[part, :] = best
                row_sum[part, :] = mass
                top = jnp.max(value, axis=0, keepdims=True)
                if peak is None:
                    peak = top
                    total = jnp.sum(jnp.exp2(value - peak), axis=0, keepdims=True)
                else:
                    top = jnp.maximum(peak, top)
                    total = total * jnp.exp2(peak - top) + jnp.sum(
                        jnp.exp2(value - top), axis=0, keepdims=True)
                    peak = top
            for k, step in enumerate((one, two)):
                p = shift(step)
                col_st[pl.ds(p, 1), :] = peak[:, k * half : (k + 1) * half]
                col_st[pl.ds(n_dp + p, 1), :] = total[:, k * half : (k + 1) * half]

        with jax.named_scope("c_blocks"):
            landed((0, 1), "A")
            forward((0, 1), "A0", "Y-")
            forward((0, 1), "A", "Z-", "Z+")
            landed((1, 0), "B")
            forward((1, 0), "B0", "Z-")
            forward((1, 0), "B", "Y-", "Y+")
            landed((0, 3), "A")
            forward((0, 3), "A1", "Y+")
            forward((0, 3), "A", "Z-", "Z+")
            landed((3, 0), "B")
            forward((3, 0), "B1", "Z+")
            forward((3, 0), "B", "Y-", "Y+")
            landed((0, 1), "B")
            forward((0, 1), "B0", "Y-")
            landed((1, 0), "A")
            forward((1, 0), "A0", "Z-")
            landed((0, 3), "B")
            forward((0, 3), "B1", "Y+")
            landed((3, 0), "A")
            forward((3, 0), "A1", "Z+")
            pair_scores((0, 0), (0, 1), True)
            for name, way in (("A0", "Y-"), ("A1", "Y+")):
                landed((0, 2), name)
                forward((0, 2), name, "Z-", "Z+")
            for name in ("B0", "B1"):
                landed((2, 0), name)
                forward((2, 0), name, "Y-", "Y+")
            pair_scores((0, 3), (1, 0), False)
            for dy in (1, 3):
                landed((1, dy), "A")
                forward((1, dy), "A0", "Z-")
                landed((3, dy), "A")
                forward((3, dy), "A1", "Z+")
            for dz in (1, 3):
                landed((dz, 1), "B")
                forward((dz, 1), "B0", "Y-")
                landed((dz, 3), "B")
                forward((dz, 3), "B1", "Y+")
            pair_scores((3, 0), (1, 1), False)
            relay_weight(0, 1, 4, line - 1)
            relay_weight(1, line - 1, 4, 1)
            for name in ("A0", "A1"):
                landed((1, 2), name)
                landed((3, 2), name)
            forward((1, 2), "A0", "Z-")
            forward((3, 2), "A1", "Z+")
            for name in ("B0", "B1"):
                landed((2, 1), name)
                landed((2, 3), name)
            forward((2, 1), "B0", "Y-")
            forward((2, 3), "B1", "Y+")
            pair_scores((1, 3), (3, 1), False)
            for name in ("B0", "B1"):
                landed((0, 2), name)
            for name in ("A0", "A1"):
                landed((2, 0), name)
            pair_scores((3, 3), (0, 2), False)
            for name in ("B0", "B1"):
                landed((1, 2), name)
            pair_scores((2, 0), (1, 2), False)
            for name in ("B0", "B1"):
                landed((3, 2), name)
            for name in ("A0", "A1"):
                landed((2, 1), name)
            pair_scores((3, 2), (2, 1), False)
            for name in ("A0", "A1"):
                landed((2, 3), name)
            for name in ("A0", "A1", "B0", "B1"):
                landed((2, 2), name)
            pair_scores((2, 3), (2, 2), False)

        with jax.named_scope("d_colsend"):
            col_rx[d] = col_st[...]
            for p in others(d, n_dp):
                push(col_st, col_rx.at[d], cs_s.at[p], cs_r.at[d], {"dp": p})

        with jax.named_scope("e_rowstat"):
            for r in range(n_el):
                part = pl.ds(r * chunk, chunk)
                peak = jnp.max(row_max[part, :], axis=1, keepdims=True)
                acc = jnp.sum(row_sum[part, :] * jnp.exp2(row_max[part, :] - peak), axis=1,
                              keepdims=True)
                row_st[r : r + 1, :] = jnp.broadcast_to(peak, (chunk, LANES)).T[0:1, :]
                row_st[n_el + r : n_el + r + 1, :] = jnp.broadcast_to(acc, (chunk, LANES)).T[0:1, :]
            row_rx[e] = row_st[...]
            for q in others(e, n_el):
                push(row_st, row_rx.at[e], rs_s.at[q], rs_r.at[e],
                     {"section": q // n_mp, "mp": lax.rem(q, n_mp)})

        def merge(rx, count, n):
            peak = rx[0, 0:n, :]
            for k in range(1, count):
                peak = jnp.maximum(peak, rx[k, 0:n, :])
            acc = jnp.zeros(peak.shape, F32)
            for k in range(count):
                acc = acc + rx[k, n : 2 * n, :] * jnp.exp2(rx[k, 0:n, :] - peak)
            return peak + (jnp.log(acc) * LOG2E + 1.0)

        with jax.named_scope("f_relay"):
            relay_weight(1, 1, 5)
            relay_weight(0, line - 1, 5)

        with jax.named_scope("f_merge"):
            for p in sources(d, n_dp):
                arrived(col_rx.at[p], cs_r.at[p])
            col_lse[...] = merge(col_rx, n_dp, n_dp)
            for q in sources(e, n_el):
                arrived(row_rx.at[q], rs_r.at[q])
            merged = merge(row_rx, n_el, n_el)
            for r in range(n_el):
                row_lse[r * chunk : (r + 1) * chunk, :] = jnp.broadcast_to(
                    merged[r : r + 1, :], (LANES, chunk)).T

        def score_rows(r):
            base = row_lse[tile(r, pair), :]
            for step in steps:
                k = slot(step)
                value = scores[k, tile(r, pair), :]
                low = col_lse[pl.ds(shift(step), 1), :]
                both = jnp.exp2(value - base) + jnp.exp2(value - low)
                sgrad[tile(r, pair), k * half : (k + 1) * half] = both.astype(BF16)

            @pl.when(r == m)
            def _():
                line_at = tile(m * n_sec + s, half)
                value = scores[0, line_at, :]
                both = jnp.exp2(value - row_lse[line_at, :]) + jnp.exp2(
                    value - col_lse[pl.ds(d, 1), :])
                diagonal = lax.broadcasted_iota(jnp.int32, (half, half), 0) == (
                    lax.broadcasted_iota(jnp.int32, (half, half), 1))
                sgrad[line_at, 0:half] = (both - jnp.where(diagonal, 1.0, 0.0)).astype(BF16)

        def join(where):
            arrived(t_sr.at[where], ts_r.at[where])
            return t_keep[where] + t_sr[where].astype(F32)

        hops = (2, 3, 1, 0) if line == 4 else tuple(range(line - 1, -1, -1))

        def t_send(where, slot):
            return copy(t_tx.at[where], t_rx.at[spot], tc_s.at[slot], tc_r.at[spot],
                        at(where, core))

        with jax.named_scope("g_scorerows"):
            for i, hop in enumerate(hops):
                where = far(hop)
                score_rows(where)
                t_full[...] = dot_nn(sgrad[tile(where, pair), :], cols[...])
                t_sx[where] = t_full[tile(sib, chunk), :].astype(BF16)
                push(t_sx.at[where], t_sr.at[where], ts_s.at[i], ts_r.at[where], at(spot, sib))
                t_keep[where] = t_full[tile(core, chunk), :]
                if i > 0:
                    last = far(hops[i - 1])
                    t_tx[last] = join(last).astype(BF16)
                    push(t_tx.at[last], t_rx.at[spot], tc_s.at[i], tc_r.at[spot],
                         at(last, core))

        with jax.named_scope("h_image"):
            for g in range(RING):
                part = dot_tn(sgrad[:, g * RING * half : (g + 1) * RING * half], text_low[...])
                for k in range(RING):
                    step = (g, k)
                    if step == (0, 0):
                        i_own[...] = part[0:half, :]
                        continue
                    i_tx[slot(step)] = part[k * half : (k + 1) * half, :].astype(BF16)
                    push(i_tx.at[slot(step)], i_rx.at[slot(away(step))], im_s.at[slot(step)],
                         im_r.at[slot(away(step))], {"dp": shift(step)})

        mine = tile(e, chunk)

        with jax.named_scope("i_topgrad"):
            total = join(spot)
            for hop in hops[:-1]:
                where = far(hop)
                arrived(t_rx.at[where], tc_r.at[where])
                total = total + t_rx[where].astype(F32)
            unit, length = unit_rows(text[mine, :])
            g_st[n_sec - 1] = unit_backward(unit, length, mult * total).astype(BF16)

        with jax.named_scope("j_weights"):
            arrived(h_own.at[1 - s], h_r)
            relay_weight(0, 2, 6)
            relay_weight(1, 2, 6)
            for step in range(line):
                index = far(step) * CORES + sib
                for which in (0, 1):
                    arrived(ww[which][1].at[index], ww_r.at[which, index])

        def spread(layer):
            for c in range(chips):
                place = layer * chips + c

                @pl.when(spot != place)
                def _():
                    copy(g_st.at[layer], g_all.at[e], gs_s.at[layer, c], gs_r.at[e],
                         at(place, core)).start()

            @pl.when(s == layer)
            def _():
                g_all[e] = g_st[layer]
                copy(g_st.at[layer], g_all.at[e], gs_s.at[layer, chips], gs_r.at[e],
                     at(spot, sib)).start()

        def drain_spread(layer):
            for c in range(chips):
                place = layer * chips + c

                @pl.when(spot != place)
                def _():
                    copy(g_st.at[layer], g_all.at[e], gs_s.at[layer, c], gs_r.at[e],
                         at(place, core)).wait_send()

            @pl.when(s == layer)
            def _():
                copy(g_st.at[layer], g_all.at[e], gs_s.at[layer, chips], gs_r.at[e],
                     at(spot, sib)).wait_send()

        def feed_forward(layer):
            spread(layer)
            g_acc[...] = g_st[layer].astype(F32)

            for j in range(n_mp):
                index = layer * n_mp + j
                pre = dot_nn(h_own[layer], wi_all[index])
                back = dot_nt(g_st[layer], wo_all[index])
                sigm = sigmoid(pre)
                grad = (back * (sigm + GELU * pre * sigm * (1.0 - sigm))).astype(BF16)
                g_acc[...] += dot_nt(grad, wi_all[index])

            if layer > 0:
                g_st[layer - 1] = g_acc[...].astype(BF16)

        def slab(k):
            return input_out.at[tile(k, chunk), :]

        with jax.named_scope("k_ffn"):
            for layer in range(n_sec - 1, -1, -1):
                feed_forward(layer)

        with jax.named_scope("l_inspread"):
            for t in range(n_sec):
                in_st[t] = g_acc[:, t * width : (t + 1) * width].astype(BF16)
            input_out[mine, :] = in_st[s]
            push(in_st.at[s], slab(e), in_s.at[0], in_r.at[e], at(spot, sib))
            for hop in hops[:-1]:
                where = far(hop)
                push(in_st.at[where // chips], slab(e), in_s.at[hop], in_r.at[e],
                     at(where, core))

        def weight_rows(k):
            back = dot_nt(g_all[k], w_out[...])
            pre_all[tile(k, chunk), :] = (back * slope_all[tile(k, chunk), :]).astype(BF16)

        with jax.named_scope("m_weightrows"):
            weight_rows(e)
            for hop in (1, 3, 2) if line == 4 else range(1, line):
                index = far(hop) * CORES + core
                arrived(g_all.at[index], gs_r.at[index])
                push(g_all.at[index], g_all.at[index], gr_s.at[hop], gs_r.at[index],
                     at(spot, sib))
                weight_rows(index)
            for hop in (0, 1, 3, 2) if line == 4 else range(line):
                index = far(hop) * CORES + sib
                arrived(g_all.at[index], gs_r.at[index])
                weight_rows(index)

        def send_weights(which):
            for p in others(d, n_dp):
                push(w_tx.at[p, which], w_rx.at[d, which], w_s.at[which, p], w_r.at[which, d],
                     {"dp": p})

        with jax.named_scope("n_wgrad"):
            g_rows = g_all[...].reshape(rows, feats)
            grad_second = dot_tn(g_rows, act_all[...])
            for p in range(n_dp):
                w_tx[p, 1] = grad_second[p * share : (p + 1) * share, :].astype(BF16)
            send_weights(1)
            grad_first = dot_tn(hidden[...], pre_all[...])
            for p in range(n_dp):
                w_tx[p, 0] = grad_first[p * share : (p + 1) * share, :].astype(BF16)
            send_weights(0)

        with jax.named_scope("o_inrelay"):
            for hop in hops[:-1]:
                index = far(hop) * CORES + core
                arrived(slab(index), in_r.at[index])
                push(slab(index), slab(index), ir_s.at[hop], in_r.at[index], at(spot, sib))

        with jax.named_scope("p_image"):
            image_half = tile(s, half)
            total = i_own[...]
            for k in range(1, n_dp):
                arrived(i_rx.at[k], im_r.at[k])
                total = total + i_rx[k].astype(F32)
            unit, length = unit_rows(image[image_half, :])
            image_out[image_half, :] = unit_backward(unit, length, mult * total).astype(BF16)
            push(image_out.at[image_half, :], image_out.at[image_half, :], io_s, io_r,
                 {"section": 1 - s})

        with jax.named_scope("q_wsum"):
            for which, out in ((1, second_out), (0, first_out)):
                total = w_tx[d, which].astype(F32)
                for p in sources(d, n_dp):
                    arrived(w_rx.at[p, which], w_r.at[which, p])
                    total = total + w_rx[p, which].astype(F32)
                out[...] = total

        with jax.named_scope("r_drain"):
            for step in range(line):
                index = far(step) * CORES + sib
                arrived(slab(index), in_r.at[index])
            arrived(image_out.at[tile(1 - s, half), :], io_r)
            for c in sent + passed:
                c.wait_send()
            for layer in range(n_sec):
                drain_spread(layer)

    return kernel


def solution(mesh):
    n_sec, n_dp, n_mp = mesh.shape["section"], mesh.shape["dp"], mesh.shape["mp"]

    def body(text, image, scale, hidden, w_in, w_out):
        rows, feats = text.shape
        own = image.shape[0]
        hid = w_in.shape[2]
        half, share = own // n_sec, feats // n_dp
        columns = half * n_dp
        line = n_sec * n_mp // CORES
        n_el = n_sec * n_mp
        chunk = rows // n_el
        dma = pltpu.SemaphoreType.DMA
        vmem = pl.BlockSpec(memory_space=pltpu.VMEM)
        out = pl.pallas_call(
            make_kernel(n_sec, n_dp, n_mp),
            out_shape=(
                jax.ShapeDtypeStruct((own, feats), BF16),
                jax.ShapeDtypeStruct((rows, feats // n_sec), BF16),
                jax.ShapeDtypeStruct((share, hid), F32),
                jax.ShapeDtypeStruct((share, hid), F32),
            ),
            in_specs=[vmem, vmem, pl.BlockSpec(memory_space=pltpu.SMEM), vmem, vmem, vmem],
            out_specs=(vmem,) * 4,
            scratch_shapes=[
                pltpu.VMEM((rows, feats), BF16),
                pltpu.VMEM((columns, feats), BF16),
                pltpu.VMEM((n_dp, rows, half), F32),
                pltpu.VMEM((rows, columns), BF16),
                pltpu.VMEM((rows, LANES), F32),
                pltpu.VMEM((rows, LANES), F32),
                pltpu.VMEM((rows, LANES), F32),
                pltpu.VMEM((n_dp, half), F32),
                pltpu.VMEM((2 * n_el, chunk), F32),
                pltpu.VMEM((n_el, 2 * n_el, chunk), F32),
                pltpu.VMEM((2 * n_dp, half), F32),
                pltpu.VMEM((n_dp, 2 * n_dp, half), F32),
                pltpu.VMEM((n_el, feats, hid), BF16),
                pltpu.VMEM((n_el, hid, feats), BF16),
                pltpu.VMEM((n_sec, chunk, feats), BF16),
                pltpu.VMEM((CORES * chunk, feats), F32),
                pltpu.VMEM((line, chunk, feats), F32),
                pltpu.VMEM((line, chunk, feats), BF16),
                pltpu.VMEM((line, chunk, feats), BF16),
                pltpu.VMEM((line, chunk, feats), BF16),
                pltpu.VMEM((line, chunk, feats), BF16),
                pltpu.VMEM((n_sec, chunk, feats), BF16),
                pltpu.VMEM((n_el, chunk, feats), BF16),
                pltpu.VMEM((chunk, feats), F32),
                pltpu.VMEM((n_sec, chunk, feats // n_sec), BF16),
                pltpu.VMEM((rows, hid), BF16),
                pltpu.VMEM((rows, hid), F32),
                pltpu.VMEM((rows, hid), BF16),
                pltpu.VMEM((n_dp, 2, share, hid), BF16),
                pltpu.VMEM((n_dp, 2, share, hid), BF16),
                pltpu.VMEM((n_dp, half, feats), BF16),
                pltpu.VMEM((n_dp, half, feats), BF16),
                pltpu.VMEM((half, feats), F32),
                dma((44,)), dma((n_dp, 4)),
                dma((n_dp,)), dma((n_dp,)),
                dma((n_el,)), dma((n_el,)),
                dma((2, 7)), dma((2, n_el)),
                dma, dma,
                dma((line,)), dma((line,)),
                dma((line,)), dma((line,)),
                dma((n_sec, line + 1)), dma((n_el,)),
                dma((line,)),
                dma((line,)), dma((n_el,)),
                dma((line,)),
                dma((2, n_dp)), dma((2, n_dp)),
                dma((n_dp,)), dma((n_dp,)),
                dma, dma,
            ],
            compiler_params=pltpu.CompilerParams(
                collective_id=0, has_side_effects=True, vmem_limit_bytes=63000000
            ),
        )(text, image, scale, hidden[0], w_in[0], w_out[0])
        image_grad, input_grad, first, second = out
        return (image_grad, input_grad, first[None], second[None])

    return jax.shard_map(
        body,
        mesh=mesh,
        in_specs=(
            P("dp", None),
            P(("dp", "mp"), None),
            P(),
            P("section", "dp", None),
            P("section", None, "mp"),
            P("section", "mp", None),
        ),
        out_specs=(
            P(("dp", "mp"), None),
            P("dp", "section"),
            P("section", "dp", "mp"),
            P("section", "dp", "mp"),
        ),
        check_vma=False,
    )
```

```python
import jax
import jax.numpy as jnp
from jax import lax
from jax.experimental import pallas as pl
from jax.experimental.pallas import tpu as pltpu
from jax.sharding import PartitionSpec as P

MESH = pl.DeviceIdType.MESH
F32 = jnp.float32
BF16 = jnp.bfloat16
GELU = 1.702
LOG2E = 1.4426950408889634
LANES = 128
CORES = 2
RING = 4


def unit_rows(values):
    wide = values.astype(F32)
    length = jnp.sqrt(jnp.sum(wide * wide, axis=1, keepdims=True) + 1.0)
    return (wide / length, length)


def unit_backward(unit, length, grad_unit):
    return (grad_unit - unit * jnp.sum(unit * grad_unit, axis=1, keepdims=True)) / length


def dot_nn(a, b):
    return lax.dot_general(a, b, (((1,), (0,)), ((), ())), preferred_element_type=F32)


def dot_nt(a, b):
    return lax.dot_general(a, b, (((1,), (1,)), ((), ())), preferred_element_type=F32)


def dot_tn(a, b):
    return lax.dot_general(a, b, (((0,), (0,)), ((), ())), preferred_element_type=F32)


def tile(index, size):
    return pl.ds(pl.multiple_of(index * size, size), size)


def make_kernel(n_sec, n_dp, n_mp):
    chips = n_mp // CORES
    line = n_sec * chips
    n_el = n_sec * n_mp

    def kernel(
        text, image, scale_ref, hidden, w_in, w_out,
        image_out, input_out, first_out, second_out,
        text_low, cols, scores, sgrad, row_max, row_sum, row_lse, col_lse, row_st, row_rx, col_st, col_rx,
        wi_all, wo_all, h_own, t_full, t_keep, t_sx, t_sr, t_tx, t_rx,
        g_st, g_all, g_acc, in_st, act_all, slope_all, pre_all,
        w_full, w_tx, w_rx, w_sum, w_st, w_end, i_tx, i_rx, i_own, i_st, i_end,
        gat_s, gat_r, cs_s, cs_r, rs_s, rs_r, ww_s, ww_r, h_s, h_r,
        ts_s, ts_r, tc_s, tc_r, gs_s, gs_r, gr_s, in_s, in_r, ir_s,
        wc_s, wc_r, w_s, w_r, im_s, im_r, io_s, io_r,
    ):
        s = lax.axis_index("section")
        d = lax.axis_index("dp")
        m = lax.axis_index("mp")
        rows, feats = text.shape
        own = image.shape[0]
        half = own // n_sec
        chunk = rows // n_el
        pair = rows // line
        share = feats // n_dp
        width = feats // n_sec
        mult = scale_ref[0]
        mult2 = mult * LOG2E
        core = lax.rem(m, CORES)
        sib = 1 - core
        spot = s * chips + m // CORES
        e = s * n_mp + m

        def at(place, who):
            return {"section": place // chips, "mp": lax.rem(place, chips) * CORES + who}

        def far(step):
            return lax.rem(spot + step, line)

        def copy(src, dst, send, recv, where):
            return pltpu.make_async_remote_copy(
                src_ref=src, dst_ref=dst, send_sem=send, recv_sem=recv,
                device_id=where, device_id_type=MESH,
            )

        def arrived(ref, recv):
            copy(ref, ref, h_s, recv, at(spot, sib)).wait_recv()

        def shift(step):
            dz, dy = step[0] % RING, step[1] % RING
            z = lax.rem(d // RING + dz, RING)
            return z * RING + lax.rem(lax.rem(d, RING) + dy, RING)

        def slot(step):
            return (step[0] % RING) * RING + step[1] % RING

        steps = [(a, b) for a in range(RING) for b in range(RING)]

        def away(step):
            return (-step[0] % RING, -step[1] % RING)

        def others(mine, count):
            return [lax.rem(mine + k, count) for k in range(1, count)]

        def sources(mine, count):
            return [lax.rem(mine + count - k, count) for k in range(1, count)]

        sent = []

        def push(*args):
            c = copy(*args)
            c.start()
            sent.append(c)

        with jax.named_scope("a_barrier"):
            barrier = pltpu.get_barrier_semaphore()
            for p in others(d, n_dp):
                pl.semaphore_signal(barrier, inc=1, device_id={"dp": p}, device_id_type=MESH)
            for q in others(e, n_el):
                pl.semaphore_signal(
                    barrier, inc=1, device_id={"section": q // n_mp, "mp": lax.rem(q, n_mp)},
                    device_id_type=MESH,
                )
            own_unit, _ = unit_rows(image[tile(s, half), :])
            cols[0:half, :] = own_unit.astype(BF16)
            h_own[s] = hidden[tile(e, chunk), :]
            wi_all[e] = w_in[...]
            wo_all[e] = w_out[...]
            pl.semaphore_wait(barrier, n_dp + n_el - 2)

        quarter = half // 4
        spans = {"A": (0, 2), "B": (2, 2), "A0": (0, 1), "A1": (1, 1), "B0": (2, 1), "B1": (3, 1)}
        ahead = {"Y-": (0, -1), "Y+": (0, 1), "Z-": (-1, 0), "Z+": (1, 0)}
        passed = []

        def piece_of(step, name):
            first, count = spans[name]
            base = slot(step) * half + first * quarter
            return cols.at[base : base + count * quarter, :]

        def forward(step, name, *directions):
            for way in directions:
                move = ahead[way]
                lands = (step[0] - move[0], step[1] - move[1])
                c = copy(piece_of(step, name), piece_of(lands, name), gat_s.at[len(passed)],
                         gat_r.at[slot(lands), spans[name][0]], {"dp": shift(move)})
                c.start()
                passed.append(c)

        def landed(step, name):
            arrived(piece_of(step, name), gat_r.at[slot(step), spans[name][0]])

        for way in ("Y-", "Y+"):
            forward((0, 0), "A", way)
        for way in ("Z-", "Z+"):
            forward((0, 0), "B", way)
        for way in ("Y-", "Y+"):
            forward((0, 0), "B", way)
        for way in ("Z-", "Z+"):
            forward((0, 0), "A", way)

        mate = (1 - s) * n_mp + m
        push(hidden.at[tile(mate, chunk), :], h_own.at[s], h_s, h_r, {"section": 1 - s})
        ww = ((w_in, wi_all), (w_out, wo_all))
        z_at, y_at = d // RING, lax.rem(d, RING)
        cell = (z_at * RING + y_at, y_at * RING + z_at)
        band = (z_at, y_at)
        cross = far(2) * CORES + core
        bit = w_in.shape[0] // n_dp

        def along(which, step):
            return {"dp": shift((0, step) if which == 0 else (step, 0))}

        for which in (0, 1):
            part = tile(cell[which], bit)
            push(ww[which][0].at[part, :], ww[which][1].at[e, part, :], wc_s.at[which, 0],
                 wc_r.at[which, 0], at(far(2), core))
        for which in (0, 1):
            push(ww[which][0], ww[which][1].at[e], ww_s.at[which, 1], ww_r.at[which, e],
                 at(far(line - 1), core))
            push(ww[1 - which][0], ww[1 - which][1].at[e], ww_s.at[1 - which, 2],
                 ww_r.at[1 - which, e], at(far(1), core))
        for which in (0, 1):
            push(ww[which][0], ww[which][1].at[e], ww_s.at[which, 0], ww_r.at[which, e],
                 at(spot, sib))

        def cross_first(which):
            mine_bit = ww[which][1].at[cross, tile(cell[which], bit), :]
            arrived(mine_bit, wc_r.at[which, 0])
            for k in range(1, RING):
                push(mine_bit, mine_bit, wc_s.at[which, k], wc_r.at[which, RING - k],
                     along(which, k))

        def cross_second(which):
            for k in range(1, RING):
                other = band[which] * RING + lax.rem(band[1 - which] + k, RING)
                arrived(ww[which][1].at[cross, tile(other, bit), :], wc_r.at[which, k])
            group = ww[which][1].at[cross, tile(band[which], RING * bit), :]
            for k in range(1, RING):
                push(group, group, wc_s.at[which, RING + k], wc_r.at[which, 2 * RING - k],
                     along(1 - which, k))

        def cross_third(which):
            for k in range(1, RING):
                other = lax.rem(band[which] + k, RING)
                arrived(ww[which][1].at[cross, tile(other, RING * bit), :],
                        wc_r.at[which, RING + k])
            push(ww[which][1].at[cross], ww[which][1].at[cross], ww_s.at[which, 6],
                 ww_r.at[which, cross], at(spot, sib))

        def relay_weight(which, step, slot):
            index = far(step) * CORES + core
            buf = ww[which][1].at[index]
            arrived(buf, ww_r.at[which, index])
            push(buf, buf, ww_s.at[which, slot], ww_r.at[which, index], at(spot, sib))

        def sigmoid(pre):
            return 1.0 / (1.0 + jnp.exp(-GELU * pre))

        with jax.named_scope("b_pre"):
            @pl.loop(0, line)
            def _(r):
                unit, _ = unit_rows(text[tile(r, pair), :])
                text_low[tile(r, pair), :] = unit.astype(BF16)

            @pl.loop(0, line)
            def _(r):
                pre = dot_nn(hidden[tile(r, pair), :], w_in[...])
                sigm = sigmoid(pre)
                act_all[tile(r, pair), :] = (pre * sigm).astype(BF16)
                slope_all[tile(r, pair), :] = sigm + GELU * pre * sigm * (1.0 - sigm)

        def pair_scores(one, two, fresh):
            piece = jnp.concatenate(
                [cols[slot(k) * half : (slot(k) + 1) * half, :] for k in (one, two)], axis=0)
            peak = total = None
            for r in range(line):
                part = pl.ds(r * pair, pair)
                value = mult2 * dot_nt(text_low[part, :], piece)
                left, right = value[:, 0:half], value[:, half : 2 * half]
                scores[slot(one), part, :] = left
                scores[slot(two), part, :] = right
                best = jnp.maximum(left, right)
                if not fresh:
                    best = jnp.maximum(best, row_max[part, :])
                mass = jnp.exp2(left - best) + jnp.exp2(right - best)
                if not fresh:
                    mass = mass + row_sum[part, :] * jnp.exp2(row_max[part, :] - best)
                row_max[part, :] = best
                row_sum[part, :] = mass
                top = jnp.max(value, axis=0, keepdims=True)
                if peak is None:
                    peak = top
                    total = jnp.sum(jnp.exp2(value - peak), axis=0, keepdims=True)
                else:
                    top = jnp.maximum(peak, top)
                    total = total * jnp.exp2(peak - top) + jnp.sum(
                        jnp.exp2(value - top), axis=0, keepdims=True)
                    peak = top
            for k, step in enumerate((one, two)):
                p = shift(step)
                col_st[pl.ds(p, 1), :] = peak[:, k * half : (k + 1) * half]
                col_st[pl.ds(n_dp + p, 1), :] = total[:, k * half : (k + 1) * half]

        with jax.named_scope("c_blocks"):
            landed((0, 1), "A")
            forward((0, 1), "A0", "Y-")
            forward((0, 1), "A", "Z-", "Z+")
            landed((1, 0), "B")
            forward((1, 0), "B0", "Z-")
            forward((1, 0), "B", "Y-", "Y+")
            landed((0, 3), "A")
            forward((0, 3), "A1", "Y+")
            forward((0, 3), "A", "Z-", "Z+")
            landed((3, 0), "B")
            forward((3, 0), "B1", "Z+")
            forward((3, 0), "B", "Y-", "Y+")
            landed((0, 1), "B")
            forward((0, 1), "B0", "Y-")
            landed((1, 0), "A")
            forward((1, 0), "A0", "Z-")
            landed((0, 3), "B")
            forward((0, 3), "B1", "Y+")
            landed((3, 0), "A")
            forward((3, 0), "A1", "Z+")
            pair_scores((0, 0), (0, 1), True)
            for name, way in (("A0", "Y-"), ("A1", "Y+")):
                landed((0, 2), name)
                forward((0, 2), name, "Z-", "Z+")
            for name in ("B0", "B1"):
                landed((2, 0), name)
                forward((2, 0), name, "Y-", "Y+")
            pair_scores((0, 3), (1, 0), False)
            for dy in (1, 3):
                landed((1, dy), "A")
                forward((1, dy), "A0", "Z-")
                landed((3, dy), "A")
                forward((3, dy), "A1", "Z+")
            for dz in (1, 3):
                landed((dz, 1), "B")
                forward((dz, 1), "B0", "Y-")
                landed((dz, 3), "B")
                forward((dz, 3), "B1", "Y+")
            pair_scores((3, 0), (1, 1), False)
            cross_first(0)
            cross_first(1)
            for name in ("A0", "A1"):
                landed((1, 2), name)
                landed((3, 2), name)
            forward((1, 2), "A0", "Z-")
            forward((3, 2), "A1", "Z+")
            for name in ("B0", "B1"):
                landed((2, 1), name)
                landed((2, 3), name)
            forward((2, 1), "B0", "Y-")
            forward((2, 3), "B1", "Y+")
            pair_scores((1, 3), (3, 1), False)
            for name in ("B0", "B1"):
                landed((0, 2), name)
            for name in ("A0", "A1"):
                landed((2, 0), name)
            pair_scores((3, 3), (0, 2), False)
            for name in ("B0", "B1"):
                landed((1, 2), name)
            pair_scores((2, 0), (1, 2), False)
            for name in ("B0", "B1"):
                landed((3, 2), name)
            for name in ("A0", "A1"):
                landed((2, 1), name)
            pair_scores((3, 2), (2, 1), False)
            for name in ("A0", "A1"):
                landed((2, 3), name)
            for name in ("A0", "A1", "B0", "B1"):
                landed((2, 2), name)
            pair_scores((2, 3), (2, 2), False)

        with jax.named_scope("d_colsend"):
            col_rx[d] = col_st[...]
            for p in others(d, n_dp):
                push(col_st, col_rx.at[d], cs_s.at[p], cs_r.at[d], {"dp": p})

        with jax.named_scope("e_rowstat"):
            for r in range(n_el):
                part = pl.ds(r * chunk, chunk)
                peak = jnp.max(row_max[part, :], axis=1, keepdims=True)
                acc = jnp.sum(row_sum[part, :] * jnp.exp2(row_max[part, :] - peak), axis=1,
                              keepdims=True)
                row_st[r : r + 1, :] = jnp.broadcast_to(peak, (chunk, LANES)).T[0:1, :]
                row_st[n_el + r : n_el + r + 1, :] = jnp.broadcast_to(acc, (chunk, LANES)).T[0:1, :]
            row_rx[e] = row_st[...]
            for q in others(e, n_el):
                push(row_st, row_rx.at[e], rs_s.at[q], rs_r.at[e],
                     {"section": q // n_mp, "mp": lax.rem(q, n_mp)})

        def merge(rx, count, n):
            peak = rx[0, 0:n, :]
            for k in range(1, count):
                peak = jnp.maximum(peak, rx[k, 0:n, :])
            acc = jnp.zeros(peak.shape, F32)
            for k in range(count):
                acc = acc + rx[k, n : 2 * n, :] * jnp.exp2(rx[k, 0:n, :] - peak)
            return peak + (jnp.log(acc) * LOG2E + 1.0)

        with jax.named_scope("f_cross"):
            cross_second(0)
            cross_second(1)

        with jax.named_scope("f_merge"):
            for p in sources(d, n_dp):
                arrived(col_rx.at[p], cs_r.at[p])
            col_lse[...] = merge(col_rx, n_dp, n_dp)
            for q in sources(e, n_el):
                arrived(row_rx.at[q], rs_r.at[q])
            merged = merge(row_rx, n_el, n_el)
            for r in range(n_el):
                row_lse[r * chunk : (r + 1) * chunk, :] = jnp.broadcast_to(
                    merged[r : r + 1, :], (LANES, chunk)).T

        def score_rows(r):
            base = row_lse[tile(r, pair), :]
            for step in steps:
                k = slot(step)
                value = scores[k, tile(r, pair), :]
                low = col_lse[pl.ds(shift(step), 1), :]
                both = jnp.exp2(value - base) + jnp.exp2(value - low)
                sgrad[tile(r, pair), k * half : (k + 1) * half] = both.astype(BF16)

            @pl.when(r == m)
            def _():
                line_at = tile(m * n_sec + s, half)
                value = scores[0, line_at, :]
                both = jnp.exp2(value - row_lse[line_at, :]) + jnp.exp2(
                    value - col_lse[pl.ds(d, 1), :])
                diagonal = lax.broadcasted_iota(jnp.int32, (half, half), 0) == (
                    lax.broadcasted_iota(jnp.int32, (half, half), 1))
                sgrad[line_at, 0:half] = (both - jnp.where(diagonal, 1.0, 0.0)).astype(BF16)

        def join(where):
            arrived(t_sr.at[where], ts_r.at[where])
            return t_keep[where] + t_sr[where].astype(F32)

        hops = (2, 3, 1, 0) if line == 4 else tuple(range(line - 1, -1, -1))

        def t_send(where, slot):
            return copy(t_tx.at[where], t_rx.at[spot], tc_s.at[slot], tc_r.at[spot],
                        at(where, core))

        with jax.named_scope("g_scorerows"):
            for i, hop in enumerate(hops):
                where = far(hop)
                score_rows(where)
                t_full[...] = dot_nn(sgrad[tile(where, pair), :], cols[...])
                t_sx[where] = t_full[tile(sib, chunk), :].astype(BF16)
                push(t_sx.at[where], t_sr.at[where], ts_s.at[i], ts_r.at[where], at(spot, sib))
                t_keep[where] = t_full[tile(core, chunk), :]
                if i > 0:
                    last = far(hops[i - 1])
                    t_tx[last] = join(last).astype(BF16)
                    push(t_tx.at[last], t_rx.at[spot], tc_s.at[i], tc_r.at[spot],
                         at(last, core))

        with jax.named_scope("g_relay"):
            relay_weight(1, 1, 3)
            relay_weight(0, line - 1, 3)
            relay_weight(0, 1, 4)
            relay_weight(1, line - 1, 4)

        fold = half // 2

        with jax.named_scope("h_image"):
            for g in (2, 1, 3, 0):
                part = dot_tn(sgrad[:, g * RING * half : (g + 1) * RING * half], text_low[...])
                for k in range(RING):
                    low = part[k * half : k * half + fold, :]
                    high = part[k * half + fold : (k + 1) * half, :]
                    if g == 0:
                        i_own[0, k] = low
                    else:
                        i_tx[0, g, k] = low.astype(BF16)
                    if k == 0:
                        i_own[1, g] = high
                    else:
                        i_tx[1, k, g] = high.astype(BF16)
                if g > 0:
                    push(i_tx.at[0, g], i_rx.at[0, RING - g], im_s.at[0, g], im_r.at[0, RING - g],
                         along(1, g))
            for k in (2, 1, 3):
                push(i_tx.at[1, k], i_rx.at[1, RING - k], im_s.at[1, k], im_r.at[1, RING - k],
                     along(0, k))

        def image_second():
            for which in (0, 1):
                for k in (1, 3, 2):
                    arrived(i_rx.at[which, k], im_r.at[which, k])
                for g in (2, 1, 3, 0):
                    total = i_own[which, g]
                    for k in range(1, RING):
                        total = total + i_rx[which, k, g].astype(F32)
                    if g == 0:
                        i_own[which, 0] = total
                    else:
                        i_st[which, g] = total.astype(BF16)
                        push(i_st.at[which, g], i_end.at[which, RING - g],
                             im_s.at[which, RING + g], im_r.at[which, 2 * RING - g],
                             along(which, g))

        mine = tile(e, chunk)

        with jax.named_scope("h_cross"):
            cross_third(0)
            cross_third(1)

        with jax.named_scope("i_topgrad"):
            total = join(spot)
            for hop in hops[:-1]:
                where = far(hop)
                arrived(t_rx.at[where], tc_r.at[where])
                total = total + t_rx[where].astype(F32)
            unit, length = unit_rows(text[mine, :])
            g_st[n_sec - 1] = unit_backward(unit, length, mult * total).astype(BF16)

        with jax.named_scope("j_weights"):
            arrived(h_own.at[1 - s], h_r)
            for step in range(line):
                index = far(step) * CORES + sib
                for which in (0, 1):
                    arrived(ww[which][1].at[index], ww_r.at[which, index])

        def spread(layer):
            for c in range(chips):
                place = layer * chips + c

                @pl.when(spot != place)
                def _():
                    copy(g_st.at[layer], g_all.at[e], gs_s.at[layer, c], gs_r.at[e],
                         at(place, core)).start()

            @pl.when(s == layer)
            def _():
                g_all[e] = g_st[layer]
                copy(g_st.at[layer], g_all.at[e], gs_s.at[layer, chips], gs_r.at[e],
                     at(spot, sib)).start()

        def drain_spread(layer):
            for c in range(chips):
                place = layer * chips + c

                @pl.when(spot != place)
                def _():
                    copy(g_st.at[layer], g_all.at[e], gs_s.at[layer, c], gs_r.at[e],
                         at(place, core)).wait_send()

            @pl.when(s == layer)
            def _():
                copy(g_st.at[layer], g_all.at[e], gs_s.at[layer, chips], gs_r.at[e],
                     at(spot, sib)).wait_send()

        def feed_forward(layer):
            spread(layer)
            g_acc[...] = g_st[layer].astype(F32)

            for j in range(n_mp):
                index = layer * n_mp + j
                pre = dot_nn(h_own[layer], wi_all[index])
                back = dot_nt(g_st[layer], wo_all[index])
                sigm = sigmoid(pre)
                grad = (back * (sigm + GELU * pre * sigm * (1.0 - sigm))).astype(BF16)
                g_acc[...] += dot_nt(grad, wi_all[index])

            if layer > 0:
                g_st[layer - 1] = g_acc[...].astype(BF16)

        def slab(k):
            return input_out.at[tile(k, chunk), :]

        with jax.named_scope("k_ffn"):
            for layer in range(n_sec - 1, -1, -1):
                feed_forward(layer)

        with jax.named_scope("l_inspread"):
            for t in range(n_sec):
                in_st[t] = g_acc[:, t * width : (t + 1) * width].astype(BF16)
            input_out[mine, :] = in_st[s]
            push(in_st.at[s], slab(e), in_s.at[0], in_r.at[e], at(spot, sib))
            for hop in hops[:-1]:
                where = far(hop)
                push(in_st.at[where // chips], slab(e), in_s.at[hop], in_r.at[e],
                     at(where, core))

        def weight_rows(k):
            back = dot_nt(g_all[k], w_out[...])
            pre_all[tile(k, chunk), :] = (back * slope_all[tile(k, chunk), :]).astype(BF16)

        with jax.named_scope("m_weightrows"):
            weight_rows(e)
            for hop in (1, 3, 2) if line == 4 else range(1, line):
                index = far(hop) * CORES + core
                arrived(g_all.at[index], gs_r.at[index])
                push(g_all.at[index], g_all.at[index], gr_s.at[hop], gs_r.at[index],
                     at(spot, sib))
                weight_rows(index)
            for hop in (0, 1, 3, 2) if line == 4 else range(line):
                index = far(hop) * CORES + sib
                arrived(g_all.at[index], gs_r.at[index])
                weight_rows(index)

        def send_weights(which):
            for k in (2, 1, 3):
                other = lax.rem(band[which] + k, RING)
                push(w_tx.at[which, tile(other, RING * share), :], w_rx.at[which, RING - k],
                     w_s.at[which, k], w_r.at[which, RING - k], along(1 - which, k))

        def weight_second(which):
            total = w_full[which, tile(band[which], RING * share), :]
            for k in (1, 3, 2):
                arrived(w_rx.at[which, k], w_r.at[which, k])
                total = total + w_rx[which, k].astype(F32)
            w_sum[which] = total
            w_st[which] = total.astype(BF16)
            for k in (2, 1, 3):
                other = lax.rem(band[1 - which] + k, RING)
                push(w_st.at[which, tile(other, share), :], w_end.at[which, RING - k],
                     w_s.at[which, RING + k], w_r.at[which, 2 * RING - k], along(which, k))

        def weight_last(which, out):
            total = w_sum[which, tile(band[1 - which], share), :]
            for k in (1, 3, 2):
                arrived(w_end.at[which, k], w_r.at[which, RING + k])
                total = total + w_end[which, k].astype(F32)
            out[...] = total

        with jax.named_scope("n_wgrad"):
            g_rows = g_all[...].reshape(rows, feats)
            grad = dot_tn(g_rows, act_all[...])
            for p in range(n_dp):
                q = (p % RING) * RING + p // RING
                w_full[1, q * share : (q + 1) * share, :] = grad[p * share : (p + 1) * share, :]
                w_tx[1, q * share : (q + 1) * share, :] = grad[
                    p * share : (p + 1) * share, :].astype(BF16)
            send_weights(1)
            grad = dot_tn(hidden[...], pre_all[...])
            w_full[0] = grad
            w_tx[0] = grad.astype(BF16)
            send_weights(0)

        with jax.named_scope("o_inrelay"):
            for hop in hops[:-1]:
                index = far(hop) * CORES + core
                arrived(slab(index), in_r.at[index])
                push(slab(index), slab(index), ir_s.at[hop], in_r.at[index], at(spot, sib))

        with jax.named_scope("p_second"):
            image_second()
        with jax.named_scope("p_wsecond"):
            weight_second(1)
            weight_second(0)

        with jax.named_scope("q_image"):
            image_half = tile(s, half)
            unit, length = unit_rows(image[image_half, :])
            for which in (0, 1):
                total = i_own[which, 0]
                for k in (1, 3, 2):
                    arrived(i_end.at[which, k], im_r.at[which, RING + k])
                    total = total + i_end[which, k].astype(F32)
                part = slice(which * fold, (which + 1) * fold)
                image_out[tile(2 * s + which, fold), :] = unit_backward(
                    unit[part, :], length[part, :], mult * total).astype(BF16)
            push(image_out.at[image_half, :], image_out.at[image_half, :], io_s, io_r,
                 {"section": 1 - s})

        with jax.named_scope("q_wsum"):
            weight_last(1, second_out)
            weight_last(0, first_out)

        with jax.named_scope("r_drain"):
            for step in range(line):
                index = far(step) * CORES + sib
                arrived(slab(index), in_r.at[index])
            arrived(image_out.at[tile(1 - s, half), :], io_r)
            for c in sent + passed:
                c.wait_send()
            for layer in range(n_sec):
                drain_spread(layer)

    return kernel


def solution(mesh):
    n_sec, n_dp, n_mp = mesh.shape["section"], mesh.shape["dp"], mesh.shape["mp"]

    def body(text, image, scale, hidden, w_in, w_out):
        rows, feats = text.shape
        own = image.shape[0]
        hid = w_in.shape[2]
        half, share = own // n_sec, feats // n_dp
        columns = half * n_dp
        line = n_sec * n_mp // CORES
        n_el = n_sec * n_mp
        chunk = rows // n_el
        dma = pltpu.SemaphoreType.DMA
        vmem = pl.BlockSpec(memory_space=pltpu.VMEM)
        out = pl.pallas_call(
            make_kernel(n_sec, n_dp, n_mp),
            out_shape=(
                jax.ShapeDtypeStruct((own, feats), BF16),
                jax.ShapeDtypeStruct((rows, feats // n_sec), BF16),
                jax.ShapeDtypeStruct((share, hid), F32),
                jax.ShapeDtypeStruct((share, hid), F32),
            ),
            in_specs=[vmem, vmem, pl.BlockSpec(memory_space=pltpu.SMEM), vmem, vmem, vmem],
            out_specs=(vmem,) * 4,
            scratch_shapes=[
                pltpu.VMEM((rows, feats), BF16),
                pltpu.VMEM((columns, feats), BF16),
                pltpu.VMEM((n_dp, rows, half), F32),
                pltpu.VMEM((rows, columns), BF16),
                pltpu.VMEM((rows, LANES), F32),
                pltpu.VMEM((rows, LANES), F32),
                pltpu.VMEM((rows, LANES), F32),
                pltpu.VMEM((n_dp, half), F32),
                pltpu.VMEM((2 * n_el, chunk), F32),
                pltpu.VMEM((n_el, 2 * n_el, chunk), F32),
                pltpu.VMEM((2 * n_dp, half), F32),
                pltpu.VMEM((n_dp, 2 * n_dp, half), F32),
                pltpu.VMEM((n_el, feats, hid), BF16),
                pltpu.VMEM((n_el, hid, feats), BF16),
                pltpu.VMEM((n_sec, chunk, feats), BF16),
                pltpu.VMEM((CORES * chunk, feats), F32),
                pltpu.VMEM((line, chunk, feats), F32),
                pltpu.VMEM((line, chunk, feats), BF16),
                pltpu.VMEM((line, chunk, feats), BF16),
                pltpu.VMEM((line, chunk, feats), BF16),
                pltpu.VMEM((line, chunk, feats), BF16),
                pltpu.VMEM((n_sec, chunk, feats), BF16),
                pltpu.VMEM((n_el, chunk, feats), BF16),
                pltpu.VMEM((chunk, feats), F32),
                pltpu.VMEM((n_sec, chunk, feats // n_sec), BF16),
                pltpu.VMEM((rows, hid), BF16),
                pltpu.VMEM((rows, hid), F32),
                pltpu.VMEM((rows, hid), BF16),
                pltpu.VMEM((2, feats, hid), F32),
                pltpu.VMEM((2, feats, hid), BF16),
                pltpu.VMEM((2, RING, RING * share, hid), BF16),
                pltpu.VMEM((2, RING * share, hid), F32),
                pltpu.VMEM((2, RING * share, hid), BF16),
                pltpu.VMEM((2, RING, share, hid), BF16),
                pltpu.VMEM((2, RING, RING, half // 2, feats), BF16),
                pltpu.VMEM((2, RING, RING, half // 2, feats), BF16),
                pltpu.VMEM((2, RING, half // 2, feats), F32),
                pltpu.VMEM((2, RING, half // 2, feats), BF16),
                pltpu.VMEM((2, RING, half // 2, feats), BF16),
                dma((44,)), dma((n_dp, 4)),
                dma((n_dp,)), dma((n_dp,)),
                dma((n_el,)), dma((n_el,)),
                dma((2, 7)), dma((2, n_el)),
                dma, dma,
                dma((line,)), dma((line,)),
                dma((line,)), dma((line,)),
                dma((n_sec, line + 1)), dma((n_el,)),
                dma((line,)),
                dma((line,)), dma((n_el,)),
                dma((line,)),
                dma((2, 2 * RING)), dma((2, 2 * RING)),
                dma((2, 2 * RING)), dma((2, 2 * RING)),
                dma((2, 2 * RING)), dma((2, 2 * RING)),
                dma, dma,
            ],
            compiler_params=pltpu.CompilerParams(
                collective_id=0, has_side_effects=True, vmem_limit_bytes=63000000
            ),
        )(text, image, scale, hidden[0], w_in[0], w_out[0])
        image_grad, input_grad, first, second = out
        return (image_grad, input_grad, first[None], second[None])

    return jax.shard_map(
        body,
        mesh=mesh,
        in_specs=(
            P("dp", None),
            P(("dp", "mp"), None),
            P(),
            P("section", "dp", None),
            P("section", None, "mp"),
            P("section", "mp", None),
        ),
        out_specs=(
            P(("dp", "mp"), None),
            P("dp", "section"),
            P("section", "dp", "mp"),
            P("section", "dp", "mp"),
        ),
        check_vma=False,
    )
```

```python
import jax
import jax.numpy as jnp
from jax import lax
from jax.experimental import pallas as pl
from jax.experimental.pallas import tpu as pltpu
from jax.sharding import PartitionSpec as P

MESH = pl.DeviceIdType.MESH
F32 = jnp.float32
BF16 = jnp.bfloat16
GELU = 1.702
LOG2E = 1.4426950408889634
LANES = 128
CORES = 2
RING = 4


def unit_rows(values):
    wide = values.astype(F32)
    length = jnp.sqrt(jnp.sum(wide * wide, axis=1, keepdims=True) + 1.0)
    return (wide / length, length)


def unit_backward(unit, length, grad_unit):
    return (grad_unit - unit * jnp.sum(unit * grad_unit, axis=1, keepdims=True)) / length


def dot_nn(a, b):
    return lax.dot_general(a, b, (((1,), (0,)), ((), ())), preferred_element_type=F32)


def dot_nt(a, b):
    return lax.dot_general(a, b, (((1,), (1,)), ((), ())), preferred_element_type=F32)


def dot_tn(a, b):
    return lax.dot_general(a, b, (((0,), (0,)), ((), ())), preferred_element_type=F32)


def tile(index, size):
    return pl.ds(pl.multiple_of(index * size, size), size)


def make_kernel(n_sec, n_dp, n_mp):
    chips = n_mp // CORES
    line = n_sec * chips
    n_el = n_sec * n_mp

    def kernel(
        text, image, scale_ref, hidden, w_in, w_out,
        image_out, input_out, first_out, second_out,
        text_low, cols, scores, sgrad, row_max, row_sum, row_lse, col_lse, row_st, row_rx, col_st, col_rx,
        wi_all, wo_all, h_own, t_full, t_keep, t_sx, t_sr, t_tx, t_rx,
        g_st, g_all, slope_own, in_st, act_all, slope_all, pre_all,
        w_full, w_tx, w_rx, w_sum, w_st, w_end, i_tx, i_rx, i_own, i_st, i_end,
        gat_s, gat_r, cs_s, cs_r, rs_s, rs_r, ww_s, ww_r, h_s, h_r,
        ts_s, ts_r, tc_s, tc_r, gs_s, gs_r, gr_s, in_s, in_r, ir_s,
        wc_s, wc_r, w_s, w_r, im_s, im_r, io_s, io_r,
    ):
        s = lax.axis_index("section")
        d = lax.axis_index("dp")
        m = lax.axis_index("mp")
        rows, feats = text.shape
        own = image.shape[0]
        half = own // n_sec
        chunk = rows // n_el
        pair = rows // line
        share = feats // n_dp
        width = feats // n_sec
        mult = scale_ref[0]
        mult2 = mult * LOG2E
        core = lax.rem(m, CORES)
        sib = 1 - core
        spot = s * chips + m // CORES
        e = s * n_mp + m

        def at(place, who):
            return {"section": place // chips, "mp": lax.rem(place, chips) * CORES + who}

        def far(step):
            return lax.rem(spot + step, line)

        def copy(src, dst, send, recv, where):
            return pltpu.make_async_remote_copy(
                src_ref=src, dst_ref=dst, send_sem=send, recv_sem=recv,
                device_id=where, device_id_type=MESH,
            )

        def arrived(ref, recv):
            copy(ref, ref, h_s, recv, at(spot, sib)).wait_recv()

        def shift(step):
            dz, dy = step[0] % RING, step[1] % RING
            z = lax.rem(d // RING + dz, RING)
            return z * RING + lax.rem(lax.rem(d, RING) + dy, RING)

        def slot(step):
            return (step[0] % RING) * RING + step[1] % RING

        steps = [(a, b) for a in range(RING) for b in range(RING)]

        def away(step):
            return (-step[0] % RING, -step[1] % RING)

        def others(mine, count):
            return [lax.rem(mine + k, count) for k in range(1, count)]

        def sources(mine, count):
            return [lax.rem(mine + count - k, count) for k in range(1, count)]

        sent = []

        def push(*args):
            c = copy(*args)
            c.start()
            sent.append(c)

        with jax.named_scope("a_barrier"):
            barrier = pltpu.get_barrier_semaphore()
            for p in others(d, n_dp):
                pl.semaphore_signal(barrier, inc=1, device_id={"dp": p}, device_id_type=MESH)
            for q in others(e, n_el):
                pl.semaphore_signal(
                    barrier, inc=1, device_id={"section": q // n_mp, "mp": lax.rem(q, n_mp)},
                    device_id_type=MESH,
                )
            own_unit, _ = unit_rows(image[tile(s, half), :])
            cols[0:half, :] = own_unit.astype(BF16)
            h_own[s] = hidden[tile(e, chunk), :]
            wi_all[e] = w_in[...]
            wo_all[e] = w_out[...]
            pl.semaphore_wait(barrier, n_dp + n_el - 2)

        quarter = half // 4
        spans = {"A": (0, 2), "B": (2, 2), "A0": (0, 1), "A1": (1, 1), "B0": (2, 1), "B1": (3, 1)}
        ahead = {"Y-": (0, -1), "Y+": (0, 1), "Z-": (-1, 0), "Z+": (1, 0)}
        passed = []

        def piece_of(step, name):
            first, count = spans[name]
            base = slot(step) * half + first * quarter
            return cols.at[base : base + count * quarter, :]

        def forward(step, name, *directions):
            for way in directions:
                move = ahead[way]
                lands = (step[0] - move[0], step[1] - move[1])
                c = copy(piece_of(step, name), piece_of(lands, name), gat_s.at[len(passed)],
                         gat_r.at[slot(lands), spans[name][0]], {"dp": shift(move)})
                c.start()
                passed.append(c)

        def landed(step, name):
            arrived(piece_of(step, name), gat_r.at[slot(step), spans[name][0]])

        for way in ("Y-", "Y+"):
            forward((0, 0), "A", way)
        for way in ("Z-", "Z+"):
            forward((0, 0), "B", way)
        for way in ("Y-", "Y+"):
            forward((0, 0), "B", way)
        for way in ("Z-", "Z+"):
            forward((0, 0), "A", way)

        mate = (1 - s) * n_mp + m
        push(hidden.at[tile(mate, chunk), :], h_own.at[s], h_s, h_r, {"section": 1 - s})
        ww = ((w_in, wi_all), (w_out, wo_all))
        z_at, y_at = d // RING, lax.rem(d, RING)
        cell = (z_at * RING + y_at, y_at * RING + z_at)
        band = (z_at, y_at)
        cross = far(2) * CORES + core
        bit = w_in.shape[0] // n_dp

        def along(which, step):
            return {"dp": shift((0, step) if which == 0 else (step, 0))}

        for which in (0, 1):
            part = tile(cell[which], bit)
            push(ww[which][0].at[part, :], ww[which][1].at[e, part, :], wc_s.at[which, 0],
                 wc_r.at[which, 0], at(far(2), core))
        top = pl.ds(0, w_in.shape[0] // 2)
        rest = pl.ds(w_in.shape[0] // 2, w_in.shape[0] // 2)

        def neighbour(which, toward, part, lane):
            push(ww[which][0].at[part, :], ww[which][1].at[e, part, :], ww_s.at[which, lane],
                 ww_r.at[which, n_el + lane], at(far(toward), core))

        for part, lane in ((top, 0), (rest, 2)):
            neighbour(0, line - 1, part, 1 + lane)
            neighbour(1, 1, part, 2 + lane)
        neighbour(1, line - 1, top, 1)
        neighbour(0, 1, top, 2)

        for which in (0, 1):
            push(ww[which][0], ww[which][1].at[e], ww_s.at[which, 0], ww_r.at[which, e],
                 at(spot, sib))

        def cross_first(which):
            mine_bit = ww[which][1].at[cross, tile(cell[which], bit), :]
            arrived(mine_bit, wc_r.at[which, 0])
            for k in range(1, RING):
                push(mine_bit, mine_bit, wc_s.at[which, k], wc_r.at[which, RING - k],
                     along(which, k))

        def cross_second(which):
            for k in range(1, RING):
                other = band[which] * RING + lax.rem(band[1 - which] + k, RING)
                arrived(ww[which][1].at[cross, tile(other, bit), :], wc_r.at[which, k])
            group = ww[which][1].at[cross, tile(band[which], RING * bit), :]
            for k in range(1, RING):
                push(group, group, wc_s.at[which, RING + k], wc_r.at[which, 2 * RING - k],
                     along(1 - which, k))

        def cross_third(which):
            for k in range(1, RING):
                other = lax.rem(band[which] + k, RING)
                arrived(ww[which][1].at[cross, tile(other, RING * bit), :],
                        wc_r.at[which, RING + k])
            push(ww[which][1].at[cross], ww[which][1].at[cross], ww_s.at[which, 6],
                 ww_r.at[which, cross], at(spot, sib))

        def relay_weight(which, step):
            index = far(step) * CORES + core
            buf = ww[which][1].at[index]
            for part, lane in ((top, 0), (rest, 2)):
                arrived(ww[which][1].at[index, part, :],
                        ww_r.at[which, n_el + lane + (1 if step == 1 else 2)])
            push(buf, buf, ww_s.at[which, 5 if step == 1 else 7], ww_r.at[which, index],
                 at(spot, sib))

        def sigmoid(pre):
            return 1.0 / (1.0 + jnp.exp(-GELU * pre))

        with jax.named_scope("b_pre"):
            @pl.loop(0, line)
            def _(r):
                unit, _ = unit_rows(text[tile(r, pair), :])
                text_low[tile(r, pair), :] = unit.astype(BF16)

            @pl.loop(0, line)
            def _(r):
                pre = dot_nn(hidden[tile(r, pair), :], w_in[...])
                sigm = sigmoid(pre)
                act_all[tile(r, pair), :] = (pre * sigm).astype(BF16)
                slope_all[tile(r, pair), :] = sigm + GELU * pre * sigm * (1.0 - sigm)

        def pair_scores(one, two, fresh):
            piece = jnp.concatenate(
                [cols[slot(k) * half : (slot(k) + 1) * half, :] for k in (one, two)], axis=0)
            peak = total = None
            for r in range(line):
                part = pl.ds(r * pair, pair)
                value = mult2 * dot_nt(text_low[part, :], piece)
                left, right = value[:, 0:half], value[:, half : 2 * half]
                scores[slot(one), part, :] = left
                scores[slot(two), part, :] = right
                best = jnp.maximum(left, right)
                if not fresh:
                    best = jnp.maximum(best, row_max[part, :])
                mass = jnp.exp2(left - best) + jnp.exp2(right - best)
                if not fresh:
                    mass = mass + row_sum[part, :] * jnp.exp2(row_max[part, :] - best)
                row_max[part, :] = best
                row_sum[part, :] = mass
                top = jnp.max(value, axis=0, keepdims=True)
                if peak is None:
                    peak = top
                    total = jnp.sum(jnp.exp2(value - peak), axis=0, keepdims=True)
                else:
                    top = jnp.maximum(peak, top)
                    total = total * jnp.exp2(peak - top) + jnp.sum(
                        jnp.exp2(value - top), axis=0, keepdims=True)
                    peak = top
            for k, step in enumerate((one, two)):
                p = shift(step)
                col_st[pl.ds(p, 1), :] = peak[:, k * half : (k + 1) * half]
                col_st[pl.ds(n_dp + p, 1), :] = total[:, k * half : (k + 1) * half]

        with jax.named_scope("c_blocks"):
            landed((0, 1), "A")
            forward((0, 1), "A0", "Y-")
            forward((0, 1), "A", "Z-", "Z+")
            landed((1, 0), "B")
            forward((1, 0), "B0", "Z-")
            forward((1, 0), "B", "Y-", "Y+")
            landed((0, 3), "A")
            forward((0, 3), "A1", "Y+")
            forward((0, 3), "A", "Z-", "Z+")
            landed((3, 0), "B")
            forward((3, 0), "B1", "Z+")
            forward((3, 0), "B", "Y-", "Y+")
            landed((0, 1), "B")
            forward((0, 1), "B0", "Y-")
            landed((1, 0), "A")
            forward((1, 0), "A0", "Z-")
            landed((0, 3), "B")
            forward((0, 3), "B1", "Y+")
            landed((3, 0), "A")
            forward((3, 0), "A1", "Z+")
            pair_scores((0, 0), (0, 1), True)
            for name, way in (("A0", "Y-"), ("A1", "Y+")):
                landed((0, 2), name)
                forward((0, 2), name, "Z-", "Z+")
            for name in ("B0", "B1"):
                landed((2, 0), name)
                forward((2, 0), name, "Y-", "Y+")
            pair_scores((0, 3), (1, 0), False)
            for dy in (1, 3):
                landed((1, dy), "A")
                forward((1, dy), "A0", "Z-")
                landed((3, dy), "A")
                forward((3, dy), "A1", "Z+")
            for dz in (1, 3):
                landed((dz, 1), "B")
                forward((dz, 1), "B0", "Y-")
                landed((dz, 3), "B")
                forward((dz, 3), "B1", "Y+")
            pair_scores((3, 0), (1, 1), False)
            cross_first(0)
            cross_first(1)
            for name in ("A0", "A1"):
                landed((1, 2), name)
                landed((3, 2), name)
            forward((1, 2), "A0", "Z-")
            forward((3, 2), "A1", "Z+")
            for name in ("B0", "B1"):
                landed((2, 1), name)
                landed((2, 3), name)
            forward((2, 1), "B0", "Y-")
            forward((2, 3), "B1", "Y+")
            pair_scores((1, 3), (3, 1), False)
            for name in ("B0", "B1"):
                landed((0, 2), name)
            for name in ("A0", "A1"):
                landed((2, 0), name)
            pair_scores((3, 3), (0, 2), False)
            for name in ("B0", "B1"):
                landed((1, 2), name)
            pair_scores((2, 0), (1, 2), False)
            for name in ("B0", "B1"):
                landed((3, 2), name)
            for name in ("A0", "A1"):
                landed((2, 1), name)
            pair_scores((3, 2), (2, 1), False)
            for name in ("A0", "A1"):
                landed((2, 3), name)
            for name in ("A0", "A1", "B0", "B1"):
                landed((2, 2), name)
            pair_scores((2, 3), (2, 2), False)

        with jax.named_scope("d_colsend"):
            col_rx[d] = col_st[...]
            for p in others(d, n_dp):
                push(col_st, col_rx.at[d], cs_s.at[p], cs_r.at[d], {"dp": p})

        with jax.named_scope("e_rowstat"):
            for r in range(n_el):
                part = pl.ds(r * chunk, chunk)
                peak = jnp.max(row_max[part, :], axis=1, keepdims=True)
                acc = jnp.sum(row_sum[part, :] * jnp.exp2(row_max[part, :] - peak), axis=1,
                              keepdims=True)
                row_st[r : r + 1, :] = jnp.broadcast_to(peak, (chunk, LANES)).T[0:1, :]
                row_st[n_el + r : n_el + r + 1, :] = jnp.broadcast_to(acc, (chunk, LANES)).T[0:1, :]
            row_rx[e] = row_st[...]
            for q in others(e, n_el):
                push(row_st, row_rx.at[e], rs_s.at[q], rs_r.at[e],
                     {"section": q // n_mp, "mp": lax.rem(q, n_mp)})
            neighbour(1, line - 1, rest, 3)
            neighbour(0, 1, rest, 4)

        def merge(rx, count, n):
            peak = rx[0, 0:n, :]
            for k in range(1, count):
                peak = jnp.maximum(peak, rx[k, 0:n, :])
            acc = jnp.zeros(peak.shape, F32)
            for k in range(count):
                acc = acc + rx[k, n : 2 * n, :] * jnp.exp2(rx[k, 0:n, :] - peak)
            return peak + (jnp.log(acc) * LOG2E + 1.0)

        with jax.named_scope("f_cross"):
            cross_second(0)
            cross_second(1)

        with jax.named_scope("f_merge"):
            for p in sources(d, n_dp):
                arrived(col_rx.at[p], cs_r.at[p])
            col_lse[...] = merge(col_rx, n_dp, n_dp)
            for q in sources(e, n_el):
                arrived(row_rx.at[q], rs_r.at[q])
            merged = merge(row_rx, n_el, n_el)
            for r in range(n_el):
                row_lse[r * chunk : (r + 1) * chunk, :] = jnp.broadcast_to(
                    merged[r : r + 1, :], (LANES, chunk)).T

        def score_rows(r):
            base = row_lse[tile(r, pair), :]
            for step in steps:
                k = slot(step)
                value = scores[k, tile(r, pair), :]
                low = col_lse[pl.ds(shift(step), 1), :]
                both = jnp.exp2(value - base) + jnp.exp2(value - low)
                sgrad[tile(r, pair), k * half : (k + 1) * half] = both.astype(BF16)

            @pl.when(r == m)
            def _():
                line_at = tile(m * n_sec + s, half)
                value = scores[0, line_at, :]
                both = jnp.exp2(value - row_lse[line_at, :]) + jnp.exp2(
                    value - col_lse[pl.ds(d, 1), :])
                diagonal = lax.broadcasted_iota(jnp.int32, (half, half), 0) == (
                    lax.broadcasted_iota(jnp.int32, (half, half), 1))
                sgrad[line_at, 0:half] = (both - jnp.where(diagonal, 1.0, 0.0)).astype(BF16)

        def join(where):
            arrived(t_sr.at[where], ts_r.at[where])
            return t_keep[where] + t_sr[where].astype(F32)

        hops = (2, 3, 1, 0) if line == 4 else tuple(range(line - 1, -1, -1))

        def t_send(where, slot):
            return copy(t_tx.at[where], t_rx.at[spot], tc_s.at[slot], tc_r.at[spot],
                        at(where, core))

        with jax.named_scope("g_scorerows"):
            for i, hop in enumerate(hops):
                where = far(hop)
                score_rows(where)
                t_full[...] = dot_nn(sgrad[tile(where, pair), :], cols[...])
                t_sx[where] = t_full[tile(sib, chunk), :].astype(BF16)
                push(t_sx.at[where], t_sr.at[where], ts_s.at[i], ts_r.at[where], at(spot, sib))
                t_keep[where] = t_full[tile(core, chunk), :]
                if i > 0:
                    last = far(hops[i - 1])
                    t_tx[last] = join(last).astype(BF16)
                    push(t_tx.at[last], t_rx.at[spot], tc_s.at[i], tc_r.at[spot],
                         at(last, core))

        with jax.named_scope("g_relay"):
            for which in (0, 1):
                relay_weight(which, 1)
                relay_weight(which, line - 1)

        fold = half // 2

        with jax.named_scope("h_image"):
            for g in (2, 1, 3, 0):
                part = dot_tn(sgrad[:, g * RING * half : (g + 1) * RING * half], text_low[...])
                for k in range(RING):
                    low = part[k * half : k * half + fold, :]
                    high = part[k * half + fold : (k + 1) * half, :]
                    if g == 0:
                        i_own[0, k] = low
                    else:
                        i_tx[0, g, k] = low.astype(BF16)
                    if k == 0:
                        i_own[1, g] = high
                    else:
                        i_tx[1, k, g] = high.astype(BF16)
                if g > 0:
                    push(i_tx.at[0, g], i_rx.at[0, RING - g], im_s.at[0, g], im_r.at[0, RING - g],
                         along(1, g))
            for k in (2, 1, 3):
                push(i_tx.at[1, k], i_rx.at[1, RING - k], im_s.at[1, k], im_r.at[1, RING - k],
                     along(0, k))

        def image_second():
            for which in (0, 1):
                for k in (1, 3, 2):
                    arrived(i_rx.at[which, k], im_r.at[which, k])
                for g in (2, 1, 3, 0):
                    total = i_own[which, g]
                    for k in range(1, RING):
                        total = total + i_rx[which, k, g].astype(F32)
                    if g == 0:
                        i_own[which, 0] = total
                    else:
                        i_st[which, g] = total.astype(BF16)
                        push(i_st.at[which, g], i_end.at[which, RING - g],
                             im_s.at[which, RING + g], im_r.at[which, 2 * RING - g],
                             along(which, g))

        mine = tile(e, chunk)

        with jax.named_scope("h_cross"):
            cross_third(0)
            cross_third(1)

        def slopes(layer):
            for j in range(n_mp):
                pre = dot_nn(h_own[layer], wi_all[layer * n_mp + j])
                sigm = sigmoid(pre)
                slope_own[layer, j] = sigm + GELU * pre * sigm * (1.0 - sigm)

        with jax.named_scope("j_weights"):
            arrived(h_own.at[1 - s], h_r)
            for step in range(line):
                index = far(step) * CORES + sib
                for which in (0, 1):
                    arrived(ww[which][1].at[index], ww_r.at[which, index])
            for layer in range(n_sec):
                slopes(layer)

        with jax.named_scope("i_topgrad"):
            total = join(spot)
            for hop in hops[:-1]:
                where = far(hop)
                arrived(t_rx.at[where], tc_r.at[where])
                total = total + t_rx[where].astype(F32)
            unit, length = unit_rows(text[mine, :])
            g_st[n_sec - 1] = unit_backward(unit, length, mult * total).astype(BF16)

        def spread(layer):
            for c in range(chips):
                place = layer * chips + c

                @pl.when(spot != place)
                def _():
                    copy(g_st.at[layer], g_all.at[e], gs_s.at[layer, c], gs_r.at[e],
                         at(place, core)).start()

            @pl.when(s == layer)
            def _():
                g_all[e] = g_st[layer]
                copy(g_st.at[layer], g_all.at[e], gs_s.at[layer, chips], gs_r.at[e],
                     at(spot, sib)).start()

        def drain_spread(layer):
            for c in range(chips):
                place = layer * chips + c

                @pl.when(spot != place)
                def _():
                    copy(g_st.at[layer], g_all.at[e], gs_s.at[layer, c], gs_r.at[e],
                         at(place, core)).wait_send()

            @pl.when(s == layer)
            def _():
                copy(g_st.at[layer], g_all.at[e], gs_s.at[layer, chips], gs_r.at[e],
                     at(spot, sib)).wait_send()

        def feed_forward(layer):
            spread(layer)
            total = g_st[layer].astype(F32)
            for j in range(n_mp):
                index = layer * n_mp + j
                back = dot_nt(g_st[layer], wo_all[index])
                grad = (back * slope_own[layer, j]).astype(BF16)
                total = total + dot_nt(grad, wi_all[index])
            if layer > 0:
                g_st[layer - 1] = total.astype(BF16)
            else:
                for t in range(n_sec):
                    in_st[t] = total[:, t * width : (t + 1) * width].astype(BF16)

        def slab(k):
            return input_out.at[tile(k, chunk), :]

        with jax.named_scope("k_ffn"):
            for layer in range(n_sec - 1, -1, -1):
                feed_forward(layer)

        with jax.named_scope("l_inspread"):
            input_out[mine, :] = in_st[s]
            push(in_st.at[s], slab(e), in_s.at[0], in_r.at[e], at(spot, sib))
            for hop in hops[:-1]:
                where = far(hop)
                push(in_st.at[where // chips], slab(e), in_s.at[hop], in_r.at[e],
                     at(where, core))

        def weight_rows(k):
            back = dot_nt(g_all[k], w_out[...])
            pre_all[tile(k, chunk), :] = (back * slope_all[tile(k, chunk), :]).astype(BF16)

        with jax.named_scope("m_weightrows"):
            weight_rows(e)
            for hop in (1, 3, 2) if line == 4 else range(1, line):
                index = far(hop) * CORES + core
                arrived(g_all.at[index], gs_r.at[index])
                push(g_all.at[index], g_all.at[index], gr_s.at[hop], gs_r.at[index],
                     at(spot, sib))
                weight_rows(index)
            image_second()
            for hop in (0, 1, 3, 2) if line == 4 else range(line):
                index = far(hop) * CORES + sib
                arrived(g_all.at[index], gs_r.at[index])
                weight_rows(index)

        def send_weights(which):
            for k in (2, 1, 3):
                other = lax.rem(band[which] + k, RING)
                push(w_tx.at[which, tile(other, RING * share), :], w_rx.at[which, RING - k],
                     w_s.at[which, k], w_r.at[which, RING - k], along(1 - which, k))

        def weight_second(which):
            total = w_full[which, tile(band[which], RING * share), :]
            for k in (1, 3, 2):
                arrived(w_rx.at[which, k], w_r.at[which, k])
                total = total + w_rx[which, k].astype(F32)
            w_sum[which] = total
            w_st[which] = total.astype(BF16)
            for k in (2, 1, 3):
                other = lax.rem(band[1 - which] + k, RING)
                push(w_st.at[which, tile(other, share), :], w_end.at[which, RING - k],
                     w_s.at[which, RING + k], w_r.at[which, 2 * RING - k], along(which, k))

        def weight_last(which, out):
            total = w_sum[which, tile(band[1 - which], share), :]
            for k in (1, 3, 2):
                arrived(w_end.at[which, k], w_r.at[which, RING + k])
                total = total + w_end[which, k].astype(F32)
            out[...] = total

        with jax.named_scope("n_wgrad"):
            g_rows = g_all[...].reshape(rows, feats)
            grad = dot_tn(g_rows, act_all[...])
            for p in range(n_dp):
                q = (p % RING) * RING + p // RING
                w_full[1, q * share : (q + 1) * share, :] = grad[p * share : (p + 1) * share, :]
                w_tx[1, q * share : (q + 1) * share, :] = grad[
                    p * share : (p + 1) * share, :].astype(BF16)
            send_weights(1)
            grad = dot_tn(hidden[...], pre_all[...])
            w_full[0] = grad
            w_tx[0] = grad.astype(BF16)
            send_weights(0)

        with jax.named_scope("o_inrelay"):
            for hop in hops[:-1]:
                index = far(hop) * CORES + core
                arrived(slab(index), in_r.at[index])
                push(slab(index), slab(index), ir_s.at[hop], in_r.at[index], at(spot, sib))

        with jax.named_scope("q_image"):
            image_half = tile(s, half)
            unit, length = unit_rows(image[image_half, :])
            for which in (0, 1):
                total = i_own[which, 0]
                for k in (1, 3, 2):
                    arrived(i_end.at[which, k], im_r.at[which, RING + k])
                    total = total + i_end[which, k].astype(F32)
                part = slice(which * fold, (which + 1) * fold)
                image_out[tile(2 * s + which, fold), :] = unit_backward(
                    unit[part, :], length[part, :], mult * total).astype(BF16)
            push(image_out.at[image_half, :], image_out.at[image_half, :], io_s, io_r,
                 {"section": 1 - s})

        with jax.named_scope("p_wsecond"):
            weight_second(1)
            weight_second(0)

        with jax.named_scope("q_wsum"):
            weight_last(1, second_out)
            weight_last(0, first_out)

        with jax.named_scope("r_drain"):
            for step in range(line):
                index = far(step) * CORES + sib
                arrived(slab(index), in_r.at[index])
            arrived(image_out.at[tile(1 - s, half), :], io_r)
            for c in sent + passed:
                c.wait_send()
            for layer in range(n_sec):
                drain_spread(layer)

    return kernel


def solution(mesh):
    n_sec, n_dp, n_mp = mesh.shape["section"], mesh.shape["dp"], mesh.shape["mp"]

    def body(text, image, scale, hidden, w_in, w_out):
        rows, feats = text.shape
        own = image.shape[0]
        hid = w_in.shape[2]
        half, share = own // n_sec, feats // n_dp
        columns = half * n_dp
        line = n_sec * n_mp // CORES
        n_el = n_sec * n_mp
        chunk = rows // n_el
        dma = pltpu.SemaphoreType.DMA
        vmem = pl.BlockSpec(memory_space=pltpu.VMEM)
        out = pl.pallas_call(
            make_kernel(n_sec, n_dp, n_mp),
            out_shape=(
                jax.ShapeDtypeStruct((own, feats), BF16),
                jax.ShapeDtypeStruct((rows, feats // n_sec), BF16),
                jax.ShapeDtypeStruct((share, hid), F32),
                jax.ShapeDtypeStruct((share, hid), F32),
            ),
            in_specs=[vmem, vmem, pl.BlockSpec(memory_space=pltpu.SMEM), vmem, vmem, vmem],
            out_specs=(vmem,) * 4,
            scratch_shapes=[
                pltpu.VMEM((rows, feats), BF16),
                pltpu.VMEM((columns, feats), BF16),
                pltpu.VMEM((n_dp, rows, half), F32),
                pltpu.VMEM((rows, columns), BF16),
                pltpu.VMEM((rows, LANES), F32),
                pltpu.VMEM((rows, LANES), F32),
                pltpu.VMEM((rows, LANES), F32),
                pltpu.VMEM((n_dp, half), F32),
                pltpu.VMEM((2 * n_el, chunk), F32),
                pltpu.VMEM((n_el, 2 * n_el, chunk), F32),
                pltpu.VMEM((2 * n_dp, half), F32),
                pltpu.VMEM((n_dp, 2 * n_dp, half), F32),
                pltpu.VMEM((n_el, feats, hid), BF16),
                pltpu.VMEM((n_el, hid, feats), BF16),
                pltpu.VMEM((n_sec, chunk, feats), BF16),
                pltpu.VMEM((CORES * chunk, feats), F32),
                pltpu.VMEM((line, chunk, feats), F32),
                pltpu.VMEM((line, chunk, feats), BF16),
                pltpu.VMEM((line, chunk, feats), BF16),
                pltpu.VMEM((line, chunk, feats), BF16),
                pltpu.VMEM((line, chunk, feats), BF16),
                pltpu.VMEM((n_sec, chunk, feats), BF16),
                pltpu.VMEM((n_el, chunk, feats), BF16),
                pltpu.VMEM((n_sec, n_mp, chunk, hid), F32),
                pltpu.VMEM((n_sec, chunk, feats // n_sec), BF16),
                pltpu.VMEM((rows, hid), BF16),
                pltpu.VMEM((rows, hid), F32),
                pltpu.VMEM((rows, hid), BF16),
                pltpu.VMEM((2, feats, hid), F32),
                pltpu.VMEM((2, feats, hid), BF16),
                pltpu.VMEM((2, RING, RING * share, hid), BF16),
                pltpu.VMEM((2, RING * share, hid), F32),
                pltpu.VMEM((2, RING * share, hid), BF16),
                pltpu.VMEM((2, RING, share, hid), BF16),
                pltpu.VMEM((2, RING, RING, half // 2, feats), BF16),
                pltpu.VMEM((2, RING, RING, half // 2, feats), BF16),
                pltpu.VMEM((2, RING, half // 2, feats), F32),
                pltpu.VMEM((2, RING, half // 2, feats), BF16),
                pltpu.VMEM((2, RING, half // 2, feats), BF16),
                dma((44,)), dma((n_dp, 4)),
                dma((n_dp,)), dma((n_dp,)),
                dma((n_el,)), dma((n_el,)),
                dma((2, 8)), dma((2, n_el + 5)),
                dma, dma,
                dma((line,)), dma((line,)),
                dma((line,)), dma((line,)),
                dma((n_sec, line + 1)), dma((n_el,)),
                dma((line,)),
                dma((line,)), dma((n_el,)),
                dma((line,)),
                dma((2, 2 * RING)), dma((2, 2 * RING)),
                dma((2, 2 * RING)), dma((2, 2 * RING)),
                dma((2, 2 * RING)), dma((2, 2 * RING)),
                dma, dma,
            ],
            compiler_params=pltpu.CompilerParams(
                collective_id=0, has_side_effects=True, vmem_limit_bytes=52000000
            ),
        )(text, image, scale, hidden[0], w_in[0], w_out[0])
        image_grad, input_grad, first, second = out
        return (image_grad, input_grad, first[None], second[None])

    return jax.shard_map(
        body,
        mesh=mesh,
        in_specs=(
            P("dp", None),
            P(("dp", "mp"), None),
            P(),
            P("section", "dp", None),
            P("section", None, "mp"),
            P("section", "mp", None),
        ),
        out_specs=(
            P(("dp", "mp"), None),
            P("dp", "section"),
            P("section", "dp", "mp"),
            P("section", "dp", "mp"),
        ),
        check_vma=False,
    )
```

```python
import jax
import jax.numpy as jnp
from jax import lax
from jax.experimental import pallas as pl
from jax.experimental.pallas import tpu as pltpu
from jax.sharding import PartitionSpec as P

MESH = pl.DeviceIdType.MESH
F32 = jnp.float32
BF16 = jnp.bfloat16
GELU = 1.702
LOG2E = 1.4426950408889634
LANES = 128
CORES = 2
RING = 4


def unit_rows(values):
    wide = values.astype(F32)
    length = jnp.sqrt(jnp.sum(wide * wide, axis=1, keepdims=True) + 1.0)
    return (wide / length, length)


def unit_backward(unit, length, grad_unit):
    return (grad_unit - unit * jnp.sum(unit * grad_unit, axis=1, keepdims=True)) / length


def dot_nn(a, b):
    return lax.dot_general(a, b, (((1,), (0,)), ((), ())), preferred_element_type=F32)


def dot_nt(a, b):
    return lax.dot_general(a, b, (((1,), (1,)), ((), ())), preferred_element_type=F32)


def dot_tn(a, b):
    return lax.dot_general(a, b, (((0,), (0,)), ((), ())), preferred_element_type=F32)


def tile(index, size):
    return pl.ds(pl.multiple_of(index * size, size), size)


def leave(*refs):
    copies = [pltpu.make_async_copy(refs[k], refs[4 + k], refs[8].at[k]) for k in range(4)]
    for c in copies:
        c.start()
    for c in copies:
        c.wait()


def make_kernel(n_sec, n_dp, n_mp):
    chips = n_mp // CORES
    line = n_sec * chips
    n_el = n_sec * n_mp

    def kernel(
        text_hbm, image_hbm, scale_ref, hidden_hbm, w_in_hbm, w_out_hbm,
        image_out, input_out, first_out, second_out,
        text, image, hidden, text_low, cols, scores, sgrad, row_max, row_sum, row_lse, col_lse, row_st, row_rx, row_mix, col_st, col_rx,
        wi_all, wo_all, h_own, t_full, t_keep, t_sx, t_sr, t_tx, t_rx,
        g_st, g_all, slope_own, in_st, act_all, slope_all, pre_all,
        w_full, w_tx, w_rx, w_sum, w_st, w_end, i_tx, i_rx, i_own, i_st, i_end,
        gat_s, gat_r, cs_s, cs_r, rs_s, rs_r, ww_s, ww_r, h_s, h_r,
        ts_s, ts_r, tc_s, tc_r, gs_s, gs_r, gr_s, in_s, in_r, ir_s,
        ld_s, wc_s, wc_r, w_s, w_r, im_s, im_r, io_s, io_r,
    ):
        s = lax.axis_index("section")
        d = lax.axis_index("dp")
        m = lax.axis_index("mp")
        rows, feats = text.shape
        own = image.shape[0]
        half = own // n_sec
        chunk = rows // n_el
        pair = rows // line
        share = feats // n_dp
        width = feats // n_sec
        mult = scale_ref[0]
        mult2 = mult * LOG2E
        core = lax.rem(m, CORES)
        sib = 1 - core
        spot = s * chips + m // CORES
        e = s * n_mp + m

        def at(place, who):
            return {"section": place // chips, "mp": lax.rem(place, chips) * CORES + who}

        def far(step):
            return lax.rem(spot + step, line)

        def copy(src, dst, send, recv, where):
            return pltpu.make_async_remote_copy(
                src_ref=src, dst_ref=dst, send_sem=send, recv_sem=recv,
                device_id=where, device_id_type=MESH,
            )

        def arrived(ref, recv):
            copy(ref, ref, h_s, recv, at(spot, sib)).wait_recv()

        def shift(step):
            dz, dy = step[0] % RING, step[1] % RING
            z = lax.rem(d // RING + dz, RING)
            return z * RING + lax.rem(lax.rem(d, RING) + dy, RING)

        def slot(step):
            return (step[0] % RING) * RING + step[1] % RING

        steps = [(a, b) for a in range(RING) for b in range(RING)]

        def away(step):
            return (-step[0] % RING, -step[1] % RING)

        hops = (2, 3, 1, 0) if line == 4 else tuple(range(line - 1, -1, -1))

        def others(mine, count):
            return [lax.rem(mine + k, count) for k in range(1, count)]

        def sources(mine, count):
            return [lax.rem(mine + count - k, count) for k in range(1, count)]

        sent = []

        def push(*args):
            c = copy(*args)
            c.start()
            sent.append(c)

        with jax.named_scope("a_barrier"):
            loads = [
                pltpu.make_async_copy(src, dst, ld_s.at[k])
                for k, (src, dst) in enumerate((
                    (image_hbm, image), (text_hbm, text), (hidden_hbm, hidden),
                    (w_in_hbm, wi_all.at[e]), (w_out_hbm, wo_all.at[e]),
                ))
            ]
            for load in loads:
                load.start()
            barrier = pltpu.get_barrier_semaphore()
            for p in others(d, n_dp):
                pl.semaphore_signal(barrier, inc=1, device_id={"dp": p}, device_id_type=MESH)
            for q in others(e, n_el):
                pl.semaphore_signal(
                    barrier, inc=1, device_id={"section": q // n_mp, "mp": lax.rem(q, n_mp)},
                    device_id_type=MESH,
                )
            loads[0].wait()
            own_unit, _ = unit_rows(image[tile(s, half), :])
            cols[0:half, :] = own_unit.astype(BF16)
            pl.semaphore_wait(barrier, n_dp + n_el - 2)

        quarter = half // 4
        spans = {"A": (0, 2), "B": (2, 2), "A0": (0, 1), "A1": (1, 1), "B0": (2, 1), "B1": (3, 1)}
        ahead = {"Y-": (0, -1), "Y+": (0, 1), "Z-": (-1, 0), "Z+": (1, 0)}
        passed = []

        def piece_of(step, name):
            first, count = spans[name]
            base = slot(step) * half + first * quarter
            return cols.at[base : base + count * quarter, :]

        def forward(step, name, *directions):
            for way in directions:
                move = ahead[way]
                lands = (step[0] - move[0], step[1] - move[1])
                c = copy(piece_of(step, name), piece_of(lands, name), gat_s.at[len(passed)],
                         gat_r.at[slot(lands), spans[name][0]], {"dp": shift(move)})
                c.start()
                passed.append(c)

        def landed(step, name):
            arrived(piece_of(step, name), gat_r.at[slot(step), spans[name][0]])

        for way in ("Y-", "Y+"):
            forward((0, 0), "A", way)
        for way in ("Z-", "Z+"):
            forward((0, 0), "B", way)
        for way in ("Y-", "Y+"):
            forward((0, 0), "B", way)
        for way in ("Z-", "Z+"):
            forward((0, 0), "A", way)

        for load in loads[2:]:
            load.wait()
        h_own[s] = hidden[tile(e, chunk), :]
        mate = (1 - s) * n_mp + m
        push(hidden.at[tile(mate, chunk), :], h_own.at[s], h_s, h_r, {"section": 1 - s})
        w_in, w_out = wi_all.at[e], wo_all.at[e]
        ww = ((w_in, wi_all), (w_out, wo_all))
        z_at, y_at = d // RING, lax.rem(d, RING)
        cell = (z_at * RING + y_at, y_at * RING + z_at)
        band = (z_at, y_at)
        cross = far(2) * CORES + core
        bit = w_in.shape[0] // n_dp

        def along(which, step):
            return {"dp": shift((0, step) if which == 0 else (step, 0))}

        for which in (0, 1):
            part = tile(cell[which], bit)
            push(ww[which][0].at[part, :], ww[which][1].at[e, part, :], wc_s.at[which, 0],
                 wc_r.at[which, 0], at(far(2), core))
        top = pl.ds(0, w_in.shape[0] // 2)
        rest = pl.ds(w_in.shape[0] // 2, w_in.shape[0] // 2)

        def neighbour(which, toward, part, lane):
            push(ww[which][0].at[part, :], ww[which][1].at[e, part, :], ww_s.at[which, lane],
                 ww_r.at[which, n_el + lane], at(far(toward), core))

        def both_ways(which):
            for part, lane in ((top, 0), (rest, 2)):
                neighbour(which, line - 1, part, 1 + lane)
                neighbour(which, 1, part, 2 + lane)

        both_ways(0)

        for which in (0, 1):
            push(ww[which][0], ww[which][1].at[e], ww_s.at[which, 0], ww_r.at[which, e],
                 at(spot, sib))

        def cross_first(which):
            mine_bit = ww[which][1].at[cross, tile(cell[which], bit), :]
            arrived(mine_bit, wc_r.at[which, 0])
            for k in range(1, RING):
                push(mine_bit, mine_bit, wc_s.at[which, k], wc_r.at[which, RING - k],
                     along(which, k))

        def cross_second(which):
            for k in range(1, RING):
                other = band[which] * RING + lax.rem(band[1 - which] + k, RING)
                arrived(ww[which][1].at[cross, tile(other, bit), :], wc_r.at[which, k])
            group = ww[which][1].at[cross, tile(band[which], RING * bit), :]
            for k in range(1, RING):
                push(group, group, wc_s.at[which, RING + k], wc_r.at[which, 2 * RING - k],
                     along(1 - which, k))

        def cross_third(which):
            for k in range(1, RING):
                other = lax.rem(band[which] + k, RING)
                arrived(ww[which][1].at[cross, tile(other, RING * bit), :],
                        wc_r.at[which, RING + k])
            push(ww[which][1].at[cross], ww[which][1].at[cross], ww_s.at[which, 6],
                 ww_r.at[which, cross], at(spot, sib))

        def relay_weight(which, step):
            index = far(step) * CORES + core
            buf = ww[which][1].at[index]
            for part, lane in ((top, 0), (rest, 2)):
                arrived(ww[which][1].at[index, part, :],
                        ww_r.at[which, n_el + lane + (1 if step == 1 else 2)])
            push(buf, buf, ww_s.at[which, 5 if step == 1 else 7], ww_r.at[which, index],
                 at(spot, sib))

        def sigmoid(pre):
            return 1.0 / (1.0 + jnp.exp(-GELU * pre))

        with jax.named_scope("b_pre"):
            loads[1].wait()
            for i, hop in enumerate(hops):
                unit, _ = unit_rows(text[tile(far(hop), pair), :])
                text_low[i * pair : (i + 1) * pair, :] = unit.astype(BF16)

            @pl.loop(0, line)
            def _(r):
                pre = dot_nn(hidden[tile(r, pair), :], w_in[...])
                sigm = sigmoid(pre)
                act_all[tile(r, pair), :] = (pre * sigm).astype(BF16)
                slope_all[tile(r, pair), :] = sigm + GELU * pre * sigm * (1.0 - sigm)

        def group_scores(*group, fresh=False):
            piece = [cols[slot(k) * half : (slot(k) + 1) * half, :] for k in group]
            piece = piece[0] if len(piece) == 1 else jnp.concatenate(piece, axis=0)
            peak = total = None
            for r in range(line):
                part = pl.ds(r * pair, pair)
                value = mult2 * dot_nt(text_low[part, :], piece)
                blocks = [value[:, k * half : (k + 1) * half] for k in range(len(group))]
                for k, block in zip(group, blocks):
                    scores[slot(k), part, :] = block
                best = blocks[0]
                for block in blocks[1:]:
                    best = jnp.maximum(best, block)
                if not fresh:
                    best = jnp.maximum(best, row_max[part, :])
                    mass = row_sum[part, :] * jnp.exp2(row_max[part, :] - best)
                    for block in blocks:
                        mass = mass + jnp.exp2(block - best)
                    row_sum[part, :] = mass
                else:
                    row_sum[part, :] = jnp.ones(best.shape, F32)
                row_max[part, :] = best
                high = jnp.max(value, axis=0, keepdims=True)
                if peak is None:
                    peak = high
                    total = jnp.sum(jnp.exp2(value - peak), axis=0, keepdims=True)
                else:
                    high = jnp.maximum(peak, high)
                    total = total * jnp.exp2(peak - high) + jnp.sum(
                        jnp.exp2(value - high), axis=0, keepdims=True)
                    peak = high
            for k, step in enumerate(group):
                p = shift(step)
                col_st[pl.ds(p, 1), :] = peak[:, k * half : (k + 1) * half]
                col_st[pl.ds(n_dp + p, 1), :] = total[:, k * half : (k + 1) * half]

        with jax.named_scope("c_own"):
            group_scores((0, 0), fresh=True)

        with jax.named_scope("c_blocks"):
            landed((0, 1), "A")
            forward((0, 1), "A0", "Y-")
            forward((0, 1), "A", "Z-", "Z+")
            landed((1, 0), "B")
            forward((1, 0), "B0", "Z-")
            forward((1, 0), "B", "Y-", "Y+")
            landed((0, 3), "A")
            forward((0, 3), "A1", "Y+")
            forward((0, 3), "A", "Z-", "Z+")
            landed((3, 0), "B")
            forward((3, 0), "B1", "Z+")
            forward((3, 0), "B", "Y-", "Y+")
            landed((0, 1), "B")
            forward((0, 1), "B0", "Y-")
            landed((1, 0), "A")
            forward((1, 0), "A0", "Z-")
            landed((0, 3), "B")
            forward((0, 3), "B1", "Y+")
            landed((3, 0), "A")
            forward((3, 0), "A1", "Z+")
            group_scores((0, 1), (0, 3))
            group_scores((1, 0), (3, 0))
            for name in ("A0", "A1"):
                landed((0, 2), name)
                forward((0, 2), name, "Z-", "Z+")
            for name in ("B0", "B1"):
                landed((2, 0), name)
                forward((2, 0), name, "Y-", "Y+")
            for dy in (1, 3):
                landed((1, dy), "A")
                forward((1, dy), "A0", "Z-")
                landed((3, dy), "A")
                forward((3, dy), "A1", "Z+")
            for dz in (1, 3):
                landed((dz, 1), "B")
                forward((dz, 1), "B0", "Y-")
                landed((dz, 3), "B")
                forward((dz, 3), "B1", "Y+")
            cross_first(0)
            cross_first(1)
            group_scores((1, 1), (1, 3))
            for name in ("A0", "A1"):
                landed((1, 2), name)
                landed((3, 2), name)
            forward((1, 2), "A0", "Z-")
            forward((3, 2), "A1", "Z+")
            for name in ("B0", "B1"):
                landed((2, 1), name)
                landed((2, 3), name)
            forward((2, 1), "B0", "Y-")
            forward((2, 3), "B1", "Y+")
            group_scores((3, 1), (3, 3))
            for name in ("B0", "B1"):
                landed((0, 2), name)
            for name in ("A0", "A1"):
                landed((2, 0), name)
            group_scores((0, 2), (2, 0))
            for name in ("B0", "B1"):
                landed((1, 2), name)
                landed((3, 2), name)
            group_scores((1, 2), (3, 2))
            for name in ("A0", "A1"):
                landed((2, 1), name)
                landed((2, 3), name)
            group_scores((2, 1), (2, 3))
            for name in ("A0", "A1", "B0", "B1"):
                landed((2, 2), name)
            group_scores((2, 2))

        with jax.named_scope("d_colsend"):
            col_rx[d] = col_st[...]
            for p in others(d, n_dp):
                push(col_st, col_rx.at[d], cs_s.at[p], cs_r.at[d], {"dp": p})

        with jax.named_scope("e_rowstat"):
            for r in range(n_el):
                part = pl.ds(r * chunk, chunk)
                place = far(hops[r // CORES]) * CORES + r % CORES
                peak = jnp.max(row_max[part, :], axis=1, keepdims=True)
                acc = jnp.sum(row_sum[part, :] * jnp.exp2(row_max[part, :] - peak), axis=1,
                              keepdims=True)
                row_st[pl.ds(place, 1), :] = jnp.broadcast_to(peak, (chunk, LANES)).T[0:1, :]
                row_st[pl.ds(n_el + place, 1), :] = jnp.broadcast_to(acc, (chunk, LANES)).T[0:1, :]
            row_rx[e] = row_st[...]
            for q in others(e, n_el):
                push(row_st, row_rx.at[e], rs_s.at[q], rs_r.at[e],
                     {"section": q // n_mp, "mp": lax.rem(q, n_mp)})
            both_ways(1)

        def merge(rx, count, n):
            peak = rx[0, 0:n, :]
            for k in range(1, count):
                peak = jnp.maximum(peak, rx[k, 0:n, :])
            acc = jnp.zeros(peak.shape, F32)
            for k in range(count):
                acc = acc + rx[k, n : 2 * n, :] * jnp.exp2(rx[k, 0:n, :] - peak)
            return peak + (jnp.log(acc) * LOG2E + 1.0)

        def slopes(index):
            pre = dot_nn(h_own[index // n_mp], wi_all[index])
            sigm = sigmoid(pre)
            slope_own[index] = sigm + GELU * pre * sigm * (1.0 - sigm)

        with jax.named_scope("f_cross"):
            cross_second(0)
            cross_second(1)
            relay_weight(0, 1)
            relay_weight(0, line - 1)
            arrived(h_own.at[1 - s], h_r)
            for step in (0, 1, line - 1):
                slopes(far(step) * CORES + core)
            for step in (0, 1, line - 1):
                index = far(step) * CORES + sib
                arrived(wi_all.at[index], ww_r.at[0, index])
                slopes(index)

        with jax.named_scope("f_merge"):
            for p in sources(d, n_dp):
                arrived(col_rx.at[p], cs_r.at[p])
            col_lse[...] = merge(col_rx, n_dp, n_dp)
            for q in sources(e, n_el):
                arrived(row_rx.at[q], rs_r.at[q])
            row_mix[...] = merge(row_rx, n_el, n_el)
            for r in range(n_el):
                place = far(hops[r // CORES]) * CORES + r % CORES
                row_lse[r * chunk : (r + 1) * chunk, :] = jnp.broadcast_to(
                    row_mix[pl.ds(place, 1), :], (LANES, chunk)).T

        def score_rows(i):
            part = slice(i * pair, (i + 1) * pair)
            base = row_lse[part, :]
            offset = (m - far(hops[i])) * pair + s * half
            for step in steps:
                k = slot(step)
                value = scores[k, part, :]
                low = col_lse[pl.ds(shift(step), 1), :]
                both = jnp.exp2(value - base) + jnp.exp2(value - low)
                if k == 0:
                    diagonal = lax.broadcasted_iota(jnp.int32, (pair, half), 0) == (
                        lax.broadcasted_iota(jnp.int32, (pair, half), 1) + offset)
                    both = both - jnp.where(diagonal, 1.0, 0.0)
                sgrad[part, k * half : (k + 1) * half] = both.astype(BF16)

        def join(where):
            arrived(t_sr.at[where], ts_r.at[where])
            return t_keep[where] + t_sr[where].astype(F32)


        def t_send(where, slot):
            return copy(t_tx.at[where], t_rx.at[spot], tc_s.at[slot], tc_r.at[spot],
                        at(where, core))

        with jax.named_scope("g_scorerows"):
            score_rows(0)
            for i, hop in enumerate(hops):
                where = far(hop)
                t_full[...] = dot_nn(sgrad[i * pair : (i + 1) * pair, :], cols[...])
                if i + 1 < line:
                    score_rows(i + 1)
                t_sx[where] = t_full[tile(sib, chunk), :].astype(BF16)
                push(t_sx.at[where], t_sr.at[where], ts_s.at[i], ts_r.at[where], at(spot, sib))
                t_keep[where] = t_full[tile(core, chunk), :]
                if i > 0:
                    last = far(hops[i - 1])
                    t_tx[last] = join(last).astype(BF16)
                    push(t_tx.at[last], t_rx.at[spot], tc_s.at[i], tc_r.at[spot],
                         at(last, core))

        with jax.named_scope("g_relay"):
            relay_weight(1, 1)
            relay_weight(1, line - 1)

        fold = half // 2

        with jax.named_scope("h_image"):
            for g in (2, 1, 3, 0):
                part = dot_tn(sgrad[:, g * RING * half : (g + 1) * RING * half], text_low[...])
                for k in range(RING):
                    low = part[k * half : k * half + fold, :]
                    high = part[k * half + fold : (k + 1) * half, :]
                    if g == 0:
                        i_own[0, k] = low
                    else:
                        i_tx[0, g, k] = low.astype(BF16)
                    if k == 0:
                        i_own[1, g] = high
                    else:
                        i_tx[1, k, g] = high.astype(BF16)
                if g > 0:
                    push(i_tx.at[0, g], i_rx.at[0, RING - g], im_s.at[0, g], im_r.at[0, RING - g],
                         along(1, g))
            for k in (2, 1, 3):
                push(i_tx.at[1, k], i_rx.at[1, RING - k], im_s.at[1, k], im_r.at[1, RING - k],
                     along(0, k))

        def image_second():
            for which in (0, 1):
                for k in (1, 3, 2):
                    arrived(i_rx.at[which, k], im_r.at[which, k])
                for g in (2, 1, 3, 0):
                    total = i_own[which, g]
                    for k in range(1, RING):
                        total = total + i_rx[which, k, g].astype(F32)
                    if g == 0:
                        i_own[which, 0] = total
                    else:
                        i_st[which, g] = total.astype(BF16)
                        push(i_st.at[which, g], i_end.at[which, RING - g],
                             im_s.at[which, RING + g], im_r.at[which, 2 * RING - g],
                             along(which, g))

        mine = tile(e, chunk)

        with jax.named_scope("h_cross"):
            cross_third(0)
            cross_third(1)

        with jax.named_scope("j_weights"):
            slopes(cross)
            index = far(2) * CORES + sib
            arrived(wi_all.at[index], ww_r.at[0, index])
            slopes(index)
            for step in range(line):
                index = far(step) * CORES + sib
                arrived(wo_all.at[index], ww_r.at[1, index])

        with jax.named_scope("i_topgrad"):
            total = join(spot)
            for hop in hops[:-1]:
                where = far(hop)
                arrived(t_rx.at[where], tc_r.at[where])
                total = total + t_rx[where].astype(F32)
            unit, length = unit_rows(text[mine, :])
            g_st[n_sec - 1] = unit_backward(unit, length, mult * total).astype(BF16)

        def spread(layer):
            for c in range(chips):
                place = layer * chips + c

                @pl.when(spot != place)
                def _():
                    copy(g_st.at[layer], g_all.at[e], gs_s.at[layer, c], gs_r.at[e],
                         at(place, core)).start()

            @pl.when(s == layer)
            def _():
                g_all[e] = g_st[layer]
                copy(g_st.at[layer], g_all.at[e], gs_s.at[layer, chips], gs_r.at[e],
                     at(spot, sib)).start()

        def drain_spread(layer):
            for c in range(chips):
                place = layer * chips + c

                @pl.when(spot != place)
                def _():
                    copy(g_st.at[layer], g_all.at[e], gs_s.at[layer, c], gs_r.at[e],
                         at(place, core)).wait_send()

            @pl.when(s == layer)
            def _():
                copy(g_st.at[layer], g_all.at[e], gs_s.at[layer, chips], gs_r.at[e],
                     at(spot, sib)).wait_send()

        def feed_forward(layer):
            spread(layer)
            total = g_st[layer].astype(F32)
            for j in range(n_mp):
                index = layer * n_mp + j
                back = dot_nt(g_st[layer], wo_all[index])
                grad = (back * slope_own[index]).astype(BF16)
                total = total + dot_nt(grad, wi_all[index])
            if layer > 0:
                g_st[layer - 1] = total.astype(BF16)
            else:
                for t in range(n_sec):
                    in_st[t] = total[:, t * width : (t + 1) * width].astype(BF16)

        def slab(k):
            return input_out.at[tile(k, chunk), :]

        with jax.named_scope("k_ffn"):
            for layer in range(n_sec - 1, -1, -1):
                feed_forward(layer)

        with jax.named_scope("l_inspread"):
            input_out[mine, :] = in_st[s]
            push(in_st.at[s], slab(e), in_s.at[0], in_r.at[e], at(spot, sib))
            for hop in hops[:-1]:
                where = far(hop)
                push(in_st.at[where // chips], slab(e), in_s.at[hop], in_r.at[e],
                     at(where, core))

        def weight_rows(k):
            back = dot_nt(g_all[k], w_out[...])
            pre_all[tile(k, chunk), :] = (back * slope_all[tile(k, chunk), :]).astype(BF16)

        with jax.named_scope("m_weightrows"):
            weight_rows(e)
            for hop in (1, 3, 2) if line == 4 else range(1, line):
                index = far(hop) * CORES + core
                arrived(g_all.at[index], gs_r.at[index])
                push(g_all.at[index], g_all.at[index], gr_s.at[hop], gs_r.at[index],
                     at(spot, sib))
                weight_rows(index)
            for hop in (0, 1, 3, 2) if line == 4 else range(line):
                index = far(hop) * CORES + sib
                arrived(g_all.at[index], gs_r.at[index])
                weight_rows(index)

        def send_weights(which):
            for k in (2, 1, 3):
                other = lax.rem(band[which] + k, RING)
                push(w_tx.at[which, tile(other, RING * share), :], w_rx.at[which, RING - k],
                     w_s.at[which, k], w_r.at[which, RING - k], along(1 - which, k))

        def weight_second(which):
            total = w_full[which, tile(band[which], RING * share), :]
            for k in (1, 3, 2):
                arrived(w_rx.at[which, k], w_r.at[which, k])
                total = total + w_rx[which, k].astype(F32)
            w_sum[which] = total
            w_st[which] = total.astype(BF16)
            for k in (2, 1, 3):
                other = lax.rem(band[1 - which] + k, RING)
                push(w_st.at[which, tile(other, share), :], w_end.at[which, RING - k],
                     w_s.at[which, RING + k], w_r.at[which, 2 * RING - k], along(which, k))

        def weight_last(which, out):
            total = w_sum[which, tile(band[1 - which], share), :]
            for k in (1, 3, 2):
                arrived(w_end.at[which, k], w_r.at[which, RING + k])
                total = total + w_end[which, k].astype(F32)
            out[...] = total

        with jax.named_scope("n_wgrad"):
            g_rows = g_all[...].reshape(rows, feats)
            grad = dot_tn(g_rows, act_all[...])
            for p in range(n_dp):
                q = (p % RING) * RING + p // RING
                w_full[1, q * share : (q + 1) * share, :] = grad[p * share : (p + 1) * share, :]
                w_tx[1, q * share : (q + 1) * share, :] = grad[
                    p * share : (p + 1) * share, :].astype(BF16)
            send_weights(1)
            grad = dot_tn(hidden[...], pre_all[...])
            w_full[0] = grad
            w_tx[0] = grad.astype(BF16)
            send_weights(0)

        with jax.named_scope("o_inrelay"):
            for hop in hops[:-1]:
                index = far(hop) * CORES + core
                arrived(slab(index), in_r.at[index])
                push(slab(index), slab(index), ir_s.at[hop], in_r.at[index], at(spot, sib))

        with jax.named_scope("p_isecond"):
            image_second()

        with jax.named_scope("p_wsecond"):
            weight_second(1)
            weight_second(0)

        with jax.named_scope("q_image"):
            image_half = tile(s, half)
            unit, length = unit_rows(image[image_half, :])
            for which in (0, 1):
                total = i_own[which, 0]
                for k in (1, 3, 2):
                    arrived(i_end.at[which, k], im_r.at[which, RING + k])
                    total = total + i_end[which, k].astype(F32)
                part = slice(which * fold, (which + 1) * fold)
                image_out[tile(2 * s + which, fold), :] = unit_backward(
                    unit[part, :], length[part, :], mult * total).astype(BF16)
            push(image_out.at[image_half, :], image_out.at[image_half, :], io_s, io_r,
                 {"section": 1 - s})

        with jax.named_scope("q_wsum"):
            weight_last(1, second_out)
            weight_last(0, first_out)

        with jax.named_scope("r_drain"):
            for step in range(line):
                index = far(step) * CORES + sib
                arrived(slab(index), in_r.at[index])
            arrived(image_out.at[tile(1 - s, half), :], io_r)
            for c in sent + passed:
                c.wait_send()
            for layer in range(n_sec):
                drain_spread(layer)

    return kernel


def solution(mesh):
    n_sec, n_dp, n_mp = mesh.shape["section"], mesh.shape["dp"], mesh.shape["mp"]

    def body(text, image, scale, hidden, w_in, w_out):
        rows, feats = text.shape
        own = image.shape[0]
        hid = w_in.shape[2]
        half, share = own // n_sec, feats // n_dp
        columns = half * n_dp
        line = n_sec * n_mp // CORES
        n_el = n_sec * n_mp
        chunk = rows // n_el
        dma = pltpu.SemaphoreType.DMA
        vmem = pl.BlockSpec(memory_space=pltpu.VMEM)
        hbm = pl.BlockSpec(memory_space=pltpu.HBM)
        out = pl.pallas_call(
            make_kernel(n_sec, n_dp, n_mp),
            out_shape=(
                pltpu.VMEM((own, feats), BF16),
                pltpu.VMEM((rows, feats // n_sec), BF16),
                pltpu.VMEM((share, hid), F32),
                pltpu.VMEM((share, hid), F32),
            ),
            in_specs=[hbm, hbm, pl.BlockSpec(memory_space=pltpu.SMEM), hbm, hbm, hbm],
            out_specs=(vmem,) * 4,
            scratch_shapes=[
                pltpu.VMEM((rows, feats), BF16),
                pltpu.VMEM((own, feats), BF16),
                pltpu.VMEM((rows, feats), BF16),
                pltpu.VMEM((rows, feats), BF16),
                pltpu.VMEM((columns, feats), BF16),
                pltpu.VMEM((n_dp, rows, half), F32),
                pltpu.VMEM((rows, columns), BF16),
                pltpu.VMEM((rows, LANES), F32),
                pltpu.VMEM((rows, LANES), F32),
                pltpu.VMEM((rows, LANES), F32),
                pltpu.VMEM((n_dp, half), F32),
                pltpu.VMEM((2 * n_el, chunk), F32),
                pltpu.VMEM((n_el, 2 * n_el, chunk), F32),
                pltpu.VMEM((n_el, chunk), F32),
                pltpu.VMEM((2 * n_dp, half), F32),
                pltpu.VMEM((n_dp, 2 * n_dp, half), F32),
                pltpu.VMEM((n_el, feats, hid), BF16),
                pltpu.VMEM((n_el, hid, feats), BF16),
                pltpu.VMEM((n_sec, chunk, feats), BF16),
                pltpu.VMEM((CORES * chunk, feats), F32),
                pltpu.VMEM((line, chunk, feats), F32),
                pltpu.VMEM((line, chunk, feats), BF16),
                pltpu.VMEM((line, chunk, feats), BF16),
                pltpu.VMEM((line, chunk, feats), BF16),
                pltpu.VMEM((line, chunk, feats), BF16),
                pltpu.VMEM((n_sec, chunk, feats), BF16),
                pltpu.VMEM((n_el, chunk, feats), BF16),
                pltpu.VMEM((n_el, chunk, hid), F32),
                pltpu.VMEM((n_sec, chunk, feats // n_sec), BF16),
                pltpu.VMEM((rows, hid), BF16),
                pltpu.VMEM((rows, hid), F32),
                pltpu.VMEM((rows, hid), BF16),
                pltpu.VMEM((2, feats, hid), F32),
                pltpu.VMEM((2, feats, hid), BF16),
                pltpu.VMEM((2, RING, RING * share, hid), BF16),
                pltpu.VMEM((2, RING * share, hid), F32),
                pltpu.VMEM((2, RING * share, hid), BF16),
                pltpu.VMEM((2, RING, share, hid), BF16),
                pltpu.VMEM((2, RING, RING, half // 2, feats), BF16),
                pltpu.VMEM((2, RING, RING, half // 2, feats), BF16),
                pltpu.VMEM((2, RING, half // 2, feats), F32),
                pltpu.VMEM((2, RING, half // 2, feats), BF16),
                pltpu.VMEM((2, RING, half // 2, feats), BF16),
                dma((44,)), dma((n_dp, 4)),
                dma((n_dp,)), dma((n_dp,)),
                dma((n_el,)), dma((n_el,)),
                dma((2, 8)), dma((2, n_el + 5)),
                dma, dma,
                dma((line,)), dma((line,)),
                dma((line,)), dma((line,)),
                dma((n_sec, line + 1)), dma((n_el,)),
                dma((line,)),
                dma((line,)), dma((n_el,)),
                dma((line,)),
                dma((5,)),
                dma((2, 2 * RING)), dma((2, 2 * RING)),
                dma((2, 2 * RING)), dma((2, 2 * RING)),
                dma((2, 2 * RING)), dma((2, 2 * RING)),
                dma, dma,
            ],
            compiler_params=pltpu.CompilerParams(
                collective_id=0, has_side_effects=True, vmem_limit_bytes=57000000
            ),
        )(text, image, scale, hidden[0], w_in[0], w_out[0])
        image_grad, input_grad, first, second = pl.pallas_call(
            leave,
            out_shape=tuple(jax.ShapeDtypeStruct(x.shape, x.dtype) for x in out),
            in_specs=[vmem] * 4,
            out_specs=(hbm,) * 4,
            scratch_shapes=[dma((4,))],
            compiler_params=pltpu.CompilerParams(vmem_limit_bytes=4000000),
        )(*out)
        return (image_grad, input_grad, first[None], second[None])

    return jax.shard_map(
        body,
        mesh=mesh,
        in_specs=(
            P("dp", None),
            P(("dp", "mp"), None),
            P(),
            P("section", "dp", None),
            P("section", None, "mp"),
            P("section", "mp", None),
        ),
        out_specs=(
            P(("dp", "mp"), None),
            P("dp", "section"),
            P("section", "dp", "mp"),
            P("section", "dp", "mp"),
        ),
        check_vma=False,
    )
```

```python
import jax
import jax.numpy as jnp
from jax import lax
from jax.experimental import pallas as pl
from jax.experimental.pallas import tpu as pltpu
from jax.sharding import PartitionSpec as P

MESH = pl.DeviceIdType.MESH
F32 = jnp.float32
BF16 = jnp.bfloat16
GELU = 1.702
LOG2E = 1.4426950408889634
LANES = 128
CORES = 2
RING = 4


def unit_rows(values):
    wide = values.astype(F32)
    length = jnp.sqrt(jnp.sum(wide * wide, axis=1, keepdims=True) + 1.0)
    return (wide / length, length)


def unit_backward(unit, length, grad_unit):
    return (grad_unit - unit * jnp.sum(unit * grad_unit, axis=1, keepdims=True)) / length


def dot_nn(a, b):
    return lax.dot_general(a, b, (((1,), (0,)), ((), ())), preferred_element_type=F32)


def dot_nt(a, b):
    return lax.dot_general(a, b, (((1,), (1,)), ((), ())), preferred_element_type=F32)


def dot_tn(a, b):
    return lax.dot_general(a, b, (((0,), (0,)), ((), ())), preferred_element_type=F32)


def tile(index, size):
    return pl.ds(pl.multiple_of(index * size, size), size)


def leave(*refs):
    copies = [pltpu.make_async_copy(refs[k], refs[4 + k], refs[8].at[k]) for k in range(4)]
    for c in copies:
        c.start()
    for c in copies:
        c.wait()


def make_kernel(n_sec, n_dp, n_mp):
    chips = n_mp // CORES
    line = n_sec * chips
    n_el = n_sec * n_mp

    def kernel(
        text_hbm, image_hbm, scale_ref, hidden_hbm, w_in_hbm, w_out_hbm,
        image_out, input_out, first_out, second_out,
        text, image, hidden, text_low, cols, scores, sgrad, row_max, row_sum, row_lse, col_lse, row_st, row_rx, row_mix, col_st, col_rx,
        wi_all, wo_all, h_own, t_full, t_keep, t_sx, t_sr, t_tx, t_rx,
        g_st, g_all, slope_own, in_st, act_all, slope_all, pre_all,
        w_full, w_tx, w_rx, w_sum, w_st, w_end, i_tx, i_rx, i_own, i_st, i_end,
        gat_s, gat_r, cs_s, cs_r, rs_s, rs_r, ww_s, ww_r, h_s, h_r,
        ts_s, ts_r, tc_s, tc_r, gs_s, gs_r, gr_s, in_s, in_r, ir_s,
        ld_s, wc_s, wc_r, w_s, w_r, im_s, im_r, io_s, io_r,
    ):
        s = lax.axis_index("section")
        d = lax.axis_index("dp")
        m = lax.axis_index("mp")
        rows, feats = text.shape
        own = image.shape[0]
        half = own // n_sec
        chunk = rows // n_el
        pair = rows // line
        share = feats // n_dp
        width = feats // n_sec
        mult = scale_ref[0]
        mult2 = mult * LOG2E
        core = lax.rem(m, CORES)
        sib = 1 - core
        spot = s * chips + m // CORES
        e = s * n_mp + m

        def at(place, who):
            return {"section": place // chips, "mp": lax.rem(place, chips) * CORES + who}

        def far(step):
            return lax.rem(spot + step, line)

        def copy(src, dst, send, recv, where):
            return pltpu.make_async_remote_copy(
                src_ref=src, dst_ref=dst, send_sem=send, recv_sem=recv,
                device_id=where, device_id_type=MESH,
            )

        def arrived(ref, recv):
            copy(ref, ref, h_s, recv, at(spot, sib)).wait_recv()

        def shift(step):
            dz, dy = step[0] % RING, step[1] % RING
            z = lax.rem(d // RING + dz, RING)
            return z * RING + lax.rem(lax.rem(d, RING) + dy, RING)

        def slot(step):
            return (step[0] % RING) * RING + step[1] % RING

        steps = [(a, b) for a in range(RING) for b in range(RING)]

        def away(step):
            return (-step[0] % RING, -step[1] % RING)

        hops = (2, 3, 1, 0) if line == 4 else tuple(range(line - 1, -1, -1))

        def others(mine, count):
            return [lax.rem(mine + k, count) for k in range(1, count)]

        def sources(mine, count):
            return [lax.rem(mine + count - k, count) for k in range(1, count)]

        sent = []

        def push(*args):
            c = copy(*args)
            c.start()
            sent.append(c)

        with jax.named_scope("a_barrier"):
            loads = [
                pltpu.make_async_copy(src, dst, ld_s.at[k])
                for k, (src, dst) in enumerate((
                    (image_hbm, image), (text_hbm, text), (hidden_hbm, hidden),
                    (w_in_hbm, wi_all.at[e]), (w_out_hbm, wo_all.at[e]),
                ))
            ]
            for load in loads:
                load.start()
            barrier = pltpu.get_barrier_semaphore()
            for p in others(d, n_dp):
                pl.semaphore_signal(barrier, inc=1, device_id={"dp": p}, device_id_type=MESH)
            for q in others(e, n_el):
                pl.semaphore_signal(
                    barrier, inc=1, device_id={"section": q // n_mp, "mp": lax.rem(q, n_mp)},
                    device_id_type=MESH,
                )
            loads[0].wait()
            own_unit, _ = unit_rows(image[tile(s, half), :])
            cols[0:half, :] = own_unit.astype(BF16)
            pl.semaphore_wait(barrier, n_dp + n_el - 2)

        quarter = half // 4
        spans = {"A": (0, 2), "B": (2, 2), "A0": (0, 1), "A1": (1, 1), "B0": (2, 1), "B1": (3, 1)}
        ahead = {"Y-": (0, -1), "Y+": (0, 1), "Z-": (-1, 0), "Z+": (1, 0)}
        passed = []

        def piece_of(step, name):
            first, count = spans[name]
            base = slot(step) * half + first * quarter
            return cols.at[base : base + count * quarter, :]

        def forward(step, name, *directions):
            for way in directions:
                move = ahead[way]
                lands = (step[0] - move[0], step[1] - move[1])
                c = copy(piece_of(step, name), piece_of(lands, name), gat_s.at[len(passed)],
                         gat_r.at[slot(lands), spans[name][0]], {"dp": shift(move)})
                c.start()
                passed.append(c)

        def landed(step, name):
            arrived(piece_of(step, name), gat_r.at[slot(step), spans[name][0]])

        for way in ("Y-", "Y+"):
            forward((0, 0), "A", way)
        for way in ("Z-", "Z+"):
            forward((0, 0), "B", way)
        for way in ("Y-", "Y+"):
            forward((0, 0), "B", way)
        for way in ("Z-", "Z+"):
            forward((0, 0), "A", way)

        for load in loads[2:]:
            load.wait()
        h_own[s] = hidden[tile(e, chunk), :]
        mate = (1 - s) * n_mp + m
        push(hidden.at[tile(mate, chunk), :], h_own.at[s], h_s, h_r, {"section": 1 - s})
        w_in, w_out = wi_all.at[e], wo_all.at[e]
        ww = ((w_in, wi_all), (w_out, wo_all))
        z_at, y_at = d // RING, lax.rem(d, RING)
        cell = (z_at * RING + y_at, y_at * RING + z_at)
        band = (z_at, y_at)
        cross = far(2) * CORES + core
        bit = w_in.shape[0] // n_dp

        def along(which, step):
            return {"dp": shift((0, step) if which == 0 else (step, 0))}

        for which in (0, 1):
            part = tile(cell[which], bit)
            push(ww[which][0].at[part, :], ww[which][1].at[e, part, :], wc_s.at[which, 0],
                 wc_r.at[which, 0], at(far(2), core))
        top = pl.ds(0, w_in.shape[0] // 2)
        rest = pl.ds(w_in.shape[0] // 2, w_in.shape[0] // 2)

        def neighbour(which, toward, part, lane):
            push(ww[which][0].at[part, :], ww[which][1].at[e, part, :], ww_s.at[which, lane],
                 ww_r.at[which, n_el + lane], at(far(toward), core))

        def both_ways(which, *parts):
            for part, lane in parts:
                neighbour(which, line - 1, part, 1 + lane)
                neighbour(which, 1, part, 2 + lane)

        both_ways(0, (top, 0), (rest, 2))
        both_ways(1, (top, 0))

        for which in (0, 1):
            push(ww[which][0], ww[which][1].at[e], ww_s.at[which, 0], ww_r.at[which, e],
                 at(spot, sib))

        def cross_first(which):
            mine_bit = ww[which][1].at[cross, tile(cell[which], bit), :]
            arrived(mine_bit, wc_r.at[which, 0])
            for k in range(1, RING):
                push(mine_bit, mine_bit, wc_s.at[which, k], wc_r.at[which, RING - k],
                     along(which, k))

        def cross_second(which):
            for k in range(1, RING):
                other = band[which] * RING + lax.rem(band[1 - which] + k, RING)
                arrived(ww[which][1].at[cross, tile(other, bit), :], wc_r.at[which, k])
            group = ww[which][1].at[cross, tile(band[which], RING * bit), :]
            for k in range(1, RING):
                push(group, group, wc_s.at[which, RING + k], wc_r.at[which, 2 * RING - k],
                     along(1 - which, k))

        def cross_third(which):
            for k in range(1, RING):
                other = lax.rem(band[which] + k, RING)
                arrived(ww[which][1].at[cross, tile(other, RING * bit), :],
                        wc_r.at[which, RING + k])
            push(ww[which][1].at[cross], ww[which][1].at[cross], ww_s.at[which, 6],
                 ww_r.at[which, cross], at(spot, sib))

        def relay_weight(which, step):
            index = far(step) * CORES + core
            buf = ww[which][1].at[index]
            for part, lane in ((top, 0), (rest, 2)):
                arrived(ww[which][1].at[index, part, :],
                        ww_r.at[which, n_el + lane + (1 if step == 1 else 2)])
            push(buf, buf, ww_s.at[which, 5 if step == 1 else 7], ww_r.at[which, index],
                 at(spot, sib))

        def sigmoid(pre):
            return 1.0 / (1.0 + jnp.exp(-GELU * pre))

        with jax.named_scope("b_pre"):
            loads[1].wait()
            for i, hop in enumerate(hops):
                unit, _ = unit_rows(text[tile(far(hop), pair), :])
                text_low[i * pair : (i + 1) * pair, :] = unit.astype(BF16)

            @pl.loop(0, line)
            def _(r):
                pre = dot_nn(hidden[tile(r, pair), :], w_in[...])
                sigm = sigmoid(pre)
                act_all[tile(r, pair), :] = (pre * sigm).astype(BF16)
                slope_all[tile(r, pair), :] = sigm + GELU * pre * sigm * (1.0 - sigm)

        def group_scores(*group, fresh=False):
            piece = [cols[slot(k) * half : (slot(k) + 1) * half, :] for k in group]
            piece = piece[0] if len(piece) == 1 else jnp.concatenate(piece, axis=0)
            peak = total = None
            for r in range(line):
                part = pl.ds(r * pair, pair)
                value = mult2 * dot_nt(text_low[part, :], piece)
                blocks = [value[:, k * half : (k + 1) * half] for k in range(len(group))]
                for k, block in zip(group, blocks):
                    scores[slot(k), part, :] = block
                best = blocks[0]
                for block in blocks[1:]:
                    best = jnp.maximum(best, block)
                if not fresh:
                    best = jnp.maximum(best, row_max[part, :])
                    mass = row_sum[part, :] * jnp.exp2(row_max[part, :] - best)
                    for block in blocks:
                        mass = mass + jnp.exp2(block - best)
                    row_sum[part, :] = mass
                else:
                    row_sum[part, :] = jnp.ones(best.shape, F32)
                row_max[part, :] = best
                high = jnp.max(value, axis=0, keepdims=True)
                if peak is None:
                    peak = high
                    total = jnp.sum(jnp.exp2(value - peak), axis=0, keepdims=True)
                else:
                    high = jnp.maximum(peak, high)
                    total = total * jnp.exp2(peak - high) + jnp.sum(
                        jnp.exp2(value - high), axis=0, keepdims=True)
                    peak = high
            level = peak + jnp.log(total) * LOG2E
            for k, step in enumerate(group):
                p = shift(step)
                col_st[pl.ds(p, 1), :] = level[:, k * half : (k + 1) * half]

        with jax.named_scope("c_own"):
            group_scores((0, 0), fresh=True)

        with jax.named_scope("c_blocks"):
            landed((0, 1), "A")
            forward((0, 1), "A0", "Y-")
            forward((0, 1), "A", "Z-", "Z+")
            landed((1, 0), "B")
            forward((1, 0), "B0", "Z-")
            forward((1, 0), "B", "Y-", "Y+")
            landed((0, 3), "A")
            forward((0, 3), "A1", "Y+")
            forward((0, 3), "A", "Z-", "Z+")
            landed((3, 0), "B")
            forward((3, 0), "B1", "Z+")
            forward((3, 0), "B", "Y-", "Y+")
            landed((0, 1), "B")
            forward((0, 1), "B0", "Y-")
            landed((1, 0), "A")
            forward((1, 0), "A0", "Z-")
            landed((0, 3), "B")
            forward((0, 3), "B1", "Y+")
            landed((3, 0), "A")
            forward((3, 0), "A1", "Z+")
            group_scores((0, 1), (0, 3))
            group_scores((1, 0), (3, 0))
            for name in ("A0", "A1"):
                landed((0, 2), name)
                forward((0, 2), name, "Z-", "Z+")
            for name in ("B0", "B1"):
                landed((2, 0), name)
                forward((2, 0), name, "Y-", "Y+")
            for dy in (1, 3):
                landed((1, dy), "A")
                forward((1, dy), "A0", "Z-")
                landed((3, dy), "A")
                forward((3, dy), "A1", "Z+")
            for dz in (1, 3):
                landed((dz, 1), "B")
                forward((dz, 1), "B0", "Y-")
                landed((dz, 3), "B")
                forward((dz, 3), "B1", "Y+")
            cross_first(0)
            cross_first(1)
            group_scores((1, 1), (1, 3))
            group_scores((3, 1), (3, 3))
            for name in ("B0", "B1"):
                landed((0, 2), name)
            for name in ("A0", "A1"):
                landed((2, 0), name)
            group_scores((0, 2), (2, 0))
            for name in ("A0", "A1"):
                landed((1, 2), name)
                landed((3, 2), name)
            forward((1, 2), "A0", "Z-")
            forward((3, 2), "A1", "Z+")
            for name in ("B0", "B1"):
                landed((2, 1), name)
                landed((2, 3), name)
            forward((2, 1), "B0", "Y-")
            forward((2, 3), "B1", "Y+")
            for name in ("B0", "B1"):
                landed((1, 2), name)
                landed((3, 2), name)
            group_scores((1, 2), (3, 2))
            for name in ("A0", "A1"):
                landed((2, 1), name)
                landed((2, 3), name)
            group_scores((2, 1), (2, 3))
            for name in ("A0", "A1", "B0", "B1"):
                landed((2, 2), name)
            group_scores((2, 2))

        with jax.named_scope("d_colsend"):
            col_rx[d] = col_st[...]
            for p in others(d, n_dp):
                push(col_st, col_rx.at[d], cs_s.at[p], cs_r.at[d], {"dp": p})

        with jax.named_scope("e_rowstat"):
            for r in range(n_el):
                part = pl.ds(r * chunk, chunk)
                place = far(hops[r // CORES]) * CORES + r % CORES
                peak = jnp.max(row_max[part, :], axis=1, keepdims=True)
                acc = jnp.sum(row_sum[part, :] * jnp.exp2(row_max[part, :] - peak), axis=1,
                              keepdims=True)
                level = peak + jnp.log(acc) * LOG2E
                row_st[pl.ds(place, 1), :] = jnp.broadcast_to(level, (chunk, LANES)).T[0:1, :]
            row_rx[e] = row_st[...]
            for q in others(e, n_el):
                push(row_st, row_rx.at[e], rs_s.at[q], rs_r.at[e],
                     {"section": q // n_mp, "mp": lax.rem(q, n_mp)})
            both_ways(1, (rest, 2))

        def merge(rx, count):
            peak = rx[0]
            for k in range(1, count):
                peak = jnp.maximum(peak, rx[k])
            acc = jnp.zeros(peak.shape, F32)
            for k in range(count):
                acc = acc + jnp.exp2(rx[k] - peak)
            return peak + (jnp.log(acc) * LOG2E + 1.0)

        def slopes(index):
            pre = dot_nn(h_own[index // n_mp], wi_all[index])
            sigm = sigmoid(pre)
            slope_own[index] = sigm + GELU * pre * sigm * (1.0 - sigm)

        with jax.named_scope("f_cross"):
            cross_second(0)
            cross_second(1)
            relay_weight(0, 1)
            relay_weight(0, line - 1)
            arrived(h_own.at[1 - s], h_r)
            for step in (0, 1, line - 1):
                slopes(far(step) * CORES + core)
            for step in (0, 1, line - 1):
                index = far(step) * CORES + sib
                arrived(wi_all.at[index], ww_r.at[0, index])
                slopes(index)

        with jax.named_scope("f_merge"):
            for p in sources(d, n_dp):
                arrived(col_rx.at[p], cs_r.at[p])
            col_lse[...] = merge(col_rx, n_dp)
            for q in sources(e, n_el):
                arrived(row_rx.at[q], rs_r.at[q])
            row_mix[...] = merge(row_rx, n_el)
            for r in range(n_el):
                place = far(hops[r // CORES]) * CORES + r % CORES
                row_lse[r * chunk : (r + 1) * chunk, :] = jnp.broadcast_to(
                    row_mix[pl.ds(place, 1), :], (LANES, chunk)).T

        def score_rows(i):
            part = slice(i * pair, (i + 1) * pair)
            base = row_lse[part, :]
            offset = (m - far(hops[i])) * pair + s * half
            for step in steps:
                k = slot(step)
                value = scores[k, part, :]
                low = col_lse[pl.ds(shift(step), 1), :]
                both = jnp.exp2(value - base) + jnp.exp2(value - low)
                if k == 0:
                    diagonal = lax.broadcasted_iota(jnp.int32, (pair, half), 0) == (
                        lax.broadcasted_iota(jnp.int32, (pair, half), 1) + offset)
                    both = both - jnp.where(diagonal, 1.0, 0.0)
                sgrad[part, k * half : (k + 1) * half] = both.astype(BF16)

        def join(where):
            arrived(t_sr.at[where], ts_r.at[where])
            return t_keep[where] + t_sr[where].astype(F32)


        def t_send(where, slot):
            return copy(t_tx.at[where], t_rx.at[spot], tc_s.at[slot], tc_r.at[spot],
                        at(where, core))

        with jax.named_scope("g_scorerows"):
            score_rows(0)
            for i, hop in enumerate(hops):
                where = far(hop)
                t_full[...] = dot_nn(sgrad[i * pair : (i + 1) * pair, :], cols[...])
                if i + 1 < line:
                    score_rows(i + 1)
                t_sx[where] = t_full[tile(sib, chunk), :].astype(BF16)
                push(t_sx.at[where], t_sr.at[where], ts_s.at[i], ts_r.at[where], at(spot, sib))
                t_keep[where] = t_full[tile(core, chunk), :]
                if i > 0:
                    last = far(hops[i - 1])
                    t_tx[last] = join(last).astype(BF16)
                    push(t_tx.at[last], t_rx.at[spot], tc_s.at[i], tc_r.at[spot],
                         at(last, core))

        with jax.named_scope("g_relay"):
            cross_third(0)
            cross_third(1)
            relay_weight(1, 1)
            relay_weight(1, line - 1)

        fold = half // 2

        with jax.named_scope("h_image"):
            for g in (2, 1, 3, 0):
                part = dot_tn(sgrad[:, g * RING * half : (g + 1) * RING * half], text_low[...])
                for k in range(RING):
                    low = part[k * half : k * half + fold, :]
                    high = part[k * half + fold : (k + 1) * half, :]
                    if g == 0:
                        i_own[0, k] = low
                    else:
                        i_tx[0, g, k] = low.astype(BF16)
                    if k == 0:
                        i_own[1, g] = high
                    else:
                        i_tx[1, k, g] = high.astype(BF16)
                if g > 0:
                    push(i_tx.at[0, g], i_rx.at[0, RING - g], im_s.at[0, g], im_r.at[0, RING - g],
                         along(1, g))
            for k in (2, 1, 3):
                push(i_tx.at[1, k], i_rx.at[1, RING - k], im_s.at[1, k], im_r.at[1, RING - k],
                     along(0, k))

        def image_second():
            for which in (0, 1):
                for k in (1, 3, 2):
                    arrived(i_rx.at[which, k], im_r.at[which, k])
                for g in (2, 1, 3, 0):
                    total = i_own[which, g]
                    for k in range(1, RING):
                        total = total + i_rx[which, k, g].astype(F32)
                    if g == 0:
                        i_own[which, 0] = total
                    else:
                        i_st[which, g] = total.astype(BF16)
                        push(i_st.at[which, g], i_end.at[which, RING - g],
                             im_s.at[which, RING + g], im_r.at[which, 2 * RING - g],
                             along(which, g))

        mine = tile(e, chunk)

        with jax.named_scope("j_weights"):
            slopes(cross)
            index = far(2) * CORES + sib
            arrived(wi_all.at[index], ww_r.at[0, index])
            slopes(index)
            for step in range(line):
                index = far(step) * CORES + sib
                arrived(wo_all.at[index], ww_r.at[1, index])

        with jax.named_scope("i_topgrad"):
            total = join(spot)
            for hop in hops[:-1]:
                where = far(hop)
                arrived(t_rx.at[where], tc_r.at[where])
                total = total + t_rx[where].astype(F32)
            unit, length = unit_rows(text[mine, :])
            g_st[n_sec - 1] = unit_backward(unit, length, mult * total).astype(BF16)

        def spread(layer):
            for c in range(chips):
                place = layer * chips + c

                @pl.when(spot != place)
                def _():
                    copy(g_st.at[layer], g_all.at[e], gs_s.at[layer, c], gs_r.at[e],
                         at(place, core)).start()

            @pl.when(s == layer)
            def _():
                g_all[e] = g_st[layer]
                copy(g_st.at[layer], g_all.at[e], gs_s.at[layer, chips], gs_r.at[e],
                     at(spot, sib)).start()

        def drain_spread(layer):
            for c in range(chips):
                place = layer * chips + c

                @pl.when(spot != place)
                def _():
                    copy(g_st.at[layer], g_all.at[e], gs_s.at[layer, c], gs_r.at[e],
                         at(place, core)).wait_send()

            @pl.when(s == layer)
            def _():
                copy(g_st.at[layer], g_all.at[e], gs_s.at[layer, chips], gs_r.at[e],
                     at(spot, sib)).wait_send()

        def feed_forward(layer):
            spread(layer)
            total = g_st[layer].astype(F32)
            for j in range(n_mp):
                index = layer * n_mp + j
                back = dot_nt(g_st[layer], wo_all[index])
                grad = (back * slope_own[index]).astype(BF16)
                total = total + dot_nt(grad, wi_all[index])
            if layer > 0:
                g_st[layer - 1] = total.astype(BF16)
            else:
                for t in range(n_sec):
                    in_st[t] = total[:, t * width : (t + 1) * width].astype(BF16)

        def slab(k):
            return input_out.at[tile(k, chunk), :]

        with jax.named_scope("k_ffn"):
            for layer in range(n_sec - 1, -1, -1):
                feed_forward(layer)

        def weight_rows(k):
            back = dot_nt(g_all[k], w_out[...])
            pre_all[tile(k, chunk), :] = (back * slope_all[tile(k, chunk), :]).astype(BF16)

        with jax.named_scope("m_weightrows"):
            weight_rows(e)
            for hop in (1, 3, 2) if line == 4 else range(1, line):
                index = far(hop) * CORES + core
                arrived(g_all.at[index], gs_r.at[index])
                push(g_all.at[index], g_all.at[index], gr_s.at[hop], gs_r.at[index],
                     at(spot, sib))
                weight_rows(index)
            input_out[mine, :] = in_st[s]
            push(in_st.at[s], slab(e), in_s.at[0], in_r.at[e], at(spot, sib))
            for hop in hops[:-1]:
                where = far(hop)
                push(in_st.at[where // chips], slab(e), in_s.at[hop], in_r.at[e],
                     at(where, core))
            image_second()
            for hop in (0, 1, 3, 2) if line == 4 else range(line):
                index = far(hop) * CORES + sib
                arrived(g_all.at[index], gs_r.at[index])
                weight_rows(index)

        def send_weights(which):
            for k in (2, 1, 3):
                other = lax.rem(band[which] + k, RING)
                push(w_tx.at[which, tile(other, RING * share), :], w_rx.at[which, RING - k],
                     w_s.at[which, k], w_r.at[which, RING - k], along(1 - which, k))

        def weight_second(which):
            total = w_full[which, tile(band[which], RING * share), :]
            for k in (1, 3, 2):
                arrived(w_rx.at[which, k], w_r.at[which, k])
                total = total + w_rx[which, k].astype(F32)
            w_sum[which] = total
            w_st[which] = total.astype(BF16)
            for k in (2, 1, 3):
                other = lax.rem(band[1 - which] + k, RING)
                push(w_st.at[which, tile(other, share), :], w_end.at[which, RING - k],
                     w_s.at[which, RING + k], w_r.at[which, 2 * RING - k], along(which, k))

        def weight_last(which, out):
            total = w_sum[which, tile(band[1 - which], share), :]
            for k in (1, 3, 2):
                arrived(w_end.at[which, k], w_r.at[which, RING + k])
                total = total + w_end[which, k].astype(F32)
            out[...] = total

        with jax.named_scope("n_wgrad"):
            g_rows = g_all[...].reshape(rows, feats)
            grad = dot_tn(g_rows, act_all[...])
            for p in range(n_dp):
                q = (p % RING) * RING + p // RING
                w_full[1, q * share : (q + 1) * share, :] = grad[p * share : (p + 1) * share, :]
                w_tx[1, q * share : (q + 1) * share, :] = grad[
                    p * share : (p + 1) * share, :].astype(BF16)
            send_weights(1)
            grad = dot_tn(hidden[...], pre_all[...])
            w_full[0] = grad
            w_tx[0] = grad.astype(BF16)
            send_weights(0)

        with jax.named_scope("q_image"):
            image_half = tile(s, half)
            unit, length = unit_rows(image[image_half, :])
            for which in (0, 1):
                total = i_own[which, 0]
                for k in (1, 3, 2):
                    arrived(i_end.at[which, k], im_r.at[which, RING + k])
                    total = total + i_end[which, k].astype(F32)
                part = slice(which * fold, (which + 1) * fold)
                image_out[tile(2 * s + which, fold), :] = unit_backward(
                    unit[part, :], length[part, :], mult * total).astype(BF16)
            push(image_out.at[image_half, :], image_out.at[image_half, :], io_s, io_r,
                 {"section": 1 - s})

        with jax.named_scope("o_inrelay"):
            for hop in hops[:-1]:
                index = far(hop) * CORES + core
                arrived(slab(index), in_r.at[index])
                push(slab(index), slab(index), ir_s.at[hop], in_r.at[index], at(spot, sib))

        with jax.named_scope("p_wsecond"):
            weight_second(1)
            weight_second(0)

        with jax.named_scope("q_wsum"):
            weight_last(1, second_out)
            weight_last(0, first_out)

        with jax.named_scope("r_drain"):
            for step in range(line):
                index = far(step) * CORES + sib
                arrived(slab(index), in_r.at[index])
            arrived(image_out.at[tile(1 - s, half), :], io_r)
            for c in sent + passed:
                c.wait_send()
            for layer in range(n_sec):
                drain_spread(layer)

    return kernel


def solution(mesh):
    n_sec, n_dp, n_mp = mesh.shape["section"], mesh.shape["dp"], mesh.shape["mp"]

    def body(text, image, scale, hidden, w_in, w_out):
        rows, feats = text.shape
        own = image.shape[0]
        hid = w_in.shape[2]
        half, share = own // n_sec, feats // n_dp
        columns = half * n_dp
        line = n_sec * n_mp // CORES
        n_el = n_sec * n_mp
        chunk = rows // n_el
        dma = pltpu.SemaphoreType.DMA
        vmem = pl.BlockSpec(memory_space=pltpu.VMEM)
        hbm = pl.BlockSpec(memory_space=pltpu.HBM)
        out = pl.pallas_call(
            make_kernel(n_sec, n_dp, n_mp),
            out_shape=(
                pltpu.VMEM((own, feats), BF16),
                pltpu.VMEM((rows, feats // n_sec), BF16),
                pltpu.VMEM((share, hid), F32),
                pltpu.VMEM((share, hid), F32),
            ),
            in_specs=[hbm, hbm, pl.BlockSpec(memory_space=pltpu.SMEM), hbm, hbm, hbm],
            out_specs=(vmem,) * 4,
            scratch_shapes=[
                pltpu.VMEM((rows, feats), BF16),
                pltpu.VMEM((own, feats), BF16),
                pltpu.VMEM((rows, feats), BF16),
                pltpu.VMEM((rows, feats), BF16),
                pltpu.VMEM((columns, feats), BF16),
                pltpu.VMEM((n_dp, rows, half), F32),
                pltpu.VMEM((rows, columns), BF16),
                pltpu.VMEM((rows, LANES), F32),
                pltpu.VMEM((rows, LANES), F32),
                pltpu.VMEM((rows, LANES), F32),
                pltpu.VMEM((n_dp, half), F32),
                pltpu.VMEM((n_el, chunk), F32),
                pltpu.VMEM((n_el, n_el, chunk), F32),
                pltpu.VMEM((n_el, chunk), F32),
                pltpu.VMEM((n_dp, half), F32),
                pltpu.VMEM((n_dp, n_dp, half), F32),
                pltpu.VMEM((n_el, feats, hid), BF16),
                pltpu.VMEM((n_el, hid, feats), BF16),
                pltpu.VMEM((n_sec, chunk, feats), BF16),
                pltpu.VMEM((CORES * chunk, feats), F32),
                pltpu.VMEM((line, chunk, feats), F32),
                pltpu.VMEM((line, chunk, feats), BF16),
                pltpu.VMEM((line, chunk, feats), BF16),
                pltpu.VMEM((line, chunk, feats), BF16),
                pltpu.VMEM((line, chunk, feats), BF16),
                pltpu.VMEM((n_sec, chunk, feats), BF16),
                pltpu.VMEM((n_el, chunk, feats), BF16),
                pltpu.VMEM((n_el, chunk, hid), F32),
                pltpu.VMEM((n_sec, chunk, feats // n_sec), BF16),
                pltpu.VMEM((rows, hid), BF16),
                pltpu.VMEM((rows, hid), F32),
                pltpu.VMEM((rows, hid), BF16),
                pltpu.VMEM((2, feats, hid), F32),
                pltpu.VMEM((2, feats, hid), BF16),
                pltpu.VMEM((2, RING, RING * share, hid), BF16),
                pltpu.VMEM((2, RING * share, hid), F32),
                pltpu.VMEM((2, RING * share, hid), BF16),
                pltpu.VMEM((2, RING, share, hid), BF16),
                pltpu.VMEM((2, RING, RING, half // 2, feats), BF16),
                pltpu.VMEM((2, RING, RING, half // 2, feats), BF16),
                pltpu.VMEM((2, RING, half // 2, feats), F32),
                pltpu.VMEM((2, RING, half // 2, feats), BF16),
                pltpu.VMEM((2, RING, half // 2, feats), BF16),
                dma((44,)), dma((n_dp, 4)),
                dma((n_dp,)), dma((n_dp,)),
                dma((n_el,)), dma((n_el,)),
                dma((2, 8)), dma((2, n_el + 5)),
                dma, dma,
                dma((line,)), dma((line,)),
                dma((line,)), dma((line,)),
                dma((n_sec, line + 1)), dma((n_el,)),
                dma((line,)),
                dma((line,)), dma((n_el,)),
                dma((line,)),
                dma((5,)),
                dma((2, 2 * RING)), dma((2, 2 * RING)),
                dma((2, 2 * RING)), dma((2, 2 * RING)),
                dma((2, 2 * RING)), dma((2, 2 * RING)),
                dma, dma,
            ],
            compiler_params=pltpu.CompilerParams(
                collective_id=0, has_side_effects=True, vmem_limit_bytes=57000000
            ),
        )(text, image, scale, hidden[0], w_in[0], w_out[0])
        image_grad, input_grad, first, second = pl.pallas_call(
            leave,
            out_shape=tuple(jax.ShapeDtypeStruct(x.shape, x.dtype) for x in out),
            in_specs=[vmem] * 4,
            out_specs=(hbm,) * 4,
            scratch_shapes=[dma((4,))],
            compiler_params=pltpu.CompilerParams(vmem_limit_bytes=4000000),
        )(*out)
        return (image_grad, input_grad, first[None], second[None])

    return jax.shard_map(
        body,
        mesh=mesh,
        in_specs=(
            P("dp", None),
            P(("dp", "mp"), None),
            P(),
            P("section", "dp", None),
            P("section", None, "mp"),
            P("section", "mp", None),
        ),
        out_specs=(
            P(("dp", "mp"), None),
            P("dp", "section"),
            P("section", "dp", "mp"),
            P("section", "dp", "mp"),
        ),
        check_vma=False,
    )
```

```python
import jax
import jax.numpy as jnp
from jax import lax
from jax.experimental import pallas as pl
from jax.experimental.pallas import tpu as pltpu
from jax.sharding import PartitionSpec as P

MESH = pl.DeviceIdType.MESH
F32 = jnp.float32
BF16 = jnp.bfloat16
GELU = 1.702
LOG2E = 1.4426950408889634
LANES = 128
CORES = 2
RING = 4


def unit_rows(values):
    wide = values.astype(F32)
    length = jnp.sqrt(jnp.sum(wide * wide, axis=1, keepdims=True) + 1.0)
    return (wide / length, length)


def unit_backward(unit, length, grad_unit):
    return (grad_unit - unit * jnp.sum(unit * grad_unit, axis=1, keepdims=True)) / length


def dot_nn(a, b):
    return lax.dot_general(a, b, (((1,), (0,)), ((), ())), preferred_element_type=F32)


def dot_nt(a, b):
    return lax.dot_general(a, b, (((1,), (1,)), ((), ())), preferred_element_type=F32)


def dot_tn(a, b):
    return lax.dot_general(a, b, (((0,), (0,)), ((), ())), preferred_element_type=F32)


def tile(index, size):
    return pl.ds(pl.multiple_of(index * size, size), size)


def leave(*refs):
    copies = [pltpu.make_async_copy(refs[k], refs[4 + k], refs[8].at[k]) for k in range(4)]
    for c in copies:
        c.start()
    for c in copies:
        c.wait()


def make_kernel(n_sec, n_dp, n_mp):
    chips = n_mp // CORES
    line = n_sec * chips
    n_el = n_sec * n_mp

    def kernel(
        text_hbm, image_hbm, scale_ref, hidden_hbm, w_in_hbm, w_out_hbm,
        image_out, input_out, first_out, second_out,
        text, image, hidden, text_low, cols, scores, sgrad, row_max, row_sum, row_lse, col_lse, row_st, row_rx, row_mix, col_st, col_rx,
        wi_all, wo_all, h_own, t_full, t_keep, t_sx, t_sr, t_tx, t_rx,
        g_st, g_all, slope_own, in_st, act_all, slope_all, pre_all,
        w_full, w_tx, w_rx, w_sum, w_st, w_end, i_tx, i_rx, i_own, i_st, i_end,
        gat_s, gat_r, cs_s, cs_r, rs_s, rs_r, ww_s, ww_r, h_s, h_r,
        ts_s, ts_r, tc_s, tc_r, gs_s, gs_r, in_s, in_r,
        ld_s, wc_s, wc_r, w_s, w_r, im_s, im_r, io_s, io_r,
    ):
        s = lax.axis_index("section")
        d = lax.axis_index("dp")
        m = lax.axis_index("mp")
        rows, feats = text.shape
        own = image.shape[0]
        half = own // n_sec
        chunk = rows // n_el
        pair = rows // line
        share = feats // n_dp
        width = feats // n_sec
        mult = scale_ref[0]
        mult2 = mult * LOG2E
        core = lax.rem(m, CORES)
        sib = 1 - core
        spot = s * chips + m // CORES
        e = s * n_mp + m

        def at(place, who):
            return {"section": place // chips, "mp": lax.rem(place, chips) * CORES + who}

        def far(step):
            return lax.rem(spot + step, line)

        def copy(src, dst, send, recv, where):
            return pltpu.make_async_remote_copy(
                src_ref=src, dst_ref=dst, send_sem=send, recv_sem=recv,
                device_id=where, device_id_type=MESH,
            )

        def arrived(ref, recv):
            copy(ref, ref, h_s, recv, at(spot, sib)).wait_recv()

        def shift(step):
            dz, dy = step[0] % RING, step[1] % RING
            z = lax.rem(d // RING + dz, RING)
            return z * RING + lax.rem(lax.rem(d, RING) + dy, RING)

        def slot(step):
            return (step[0] % RING) * RING + step[1] % RING

        steps = [(a, b) for a in range(RING) for b in range(RING)]

        def away(step):
            return (-step[0] % RING, -step[1] % RING)

        hops = (2, 3, 1, 0) if line == 4 else tuple(range(line - 1, -1, -1))

        def others(mine, count):
            return [lax.rem(mine + k, count) for k in range(1, count)]

        def sources(mine, count):
            return [lax.rem(mine + count - k, count) for k in range(1, count)]

        def push(*args):
            copy(*args).start()

        def left(ref, send):
            copy(ref, ref, send, h_r, at(spot, sib)).wait_send()

        with jax.named_scope("a_barrier"):
            loads = [
                pltpu.make_async_copy(src, dst, ld_s.at[k])
                for k, (src, dst) in enumerate((
                    (image_hbm, image), (text_hbm, text), (hidden_hbm, hidden),
                    (w_in_hbm, wi_all.at[e]), (w_out_hbm, wo_all.at[e]),
                ))
            ]
            for load in loads:
                load.start()
            barrier = pltpu.get_barrier_semaphore()
            for near in ((0, 1), (0, -1), (1, 0), (-1, 0)):
                pl.semaphore_signal(
                    barrier, inc=1, device_id={"dp": shift(near)}, device_id_type=MESH)
            for q in others(e, n_el):
                pl.semaphore_signal(
                    barrier, inc=1, device_id={"section": q // n_mp, "mp": lax.rem(q, n_mp)},
                    device_id_type=MESH,
                )
            loads[0].wait()
            own_unit, _ = unit_rows(image[tile(s, half), :])
            cols[0:half, :] = own_unit.astype(BF16)
            pl.semaphore_wait(barrier, n_el + 3)

        quarter = half // 4
        spans = {"A": (0, 2), "B": (2, 2), "A0": (0, 1), "A1": (1, 1), "B0": (2, 1), "B1": (3, 1)}
        ahead = {"Y-": (0, -1), "Y+": (0, 1), "Z-": (-1, 0), "Z+": (1, 0)}
        quads = {
            "a": [((0, 2), "B0"), ((0, 2), "B1"), ((2, 0), "A0"), ((2, 0), "A1")],
            "b": [(k, name) for k in ((1, 2), (3, 2)) for name in ("A0", "A1")]
            + [(k, name) for k in ((2, 1), (2, 3)) for name in ("B0", "B1")],
            "c": [(k, name) for k in ((1, 2), (3, 2)) for name in ("B0", "B1")],
            "d": [(k, name) for k in ((2, 1), (2, 3)) for name in ("A0", "A1")],
            "e": [((2, 2), name) for name in ("A0", "A1", "B0", "B1")],
        }
        ports = {}

        def port(step, name):
            key = (slot(step), name)
            for group, members in quads.items():
                if any(key == (slot(k), other) for k, other in members):
                    key = group
            return ports.setdefault(key, len(ports))

        def landed_all(group):
            count = len(quads[group])
            k, name = quads[group][0]
            arrived(cols.at[0 : count * quarter, :], gat_r.at[port(k, name)])

        def piece_of(step, name):
            first, count = spans[name]
            base = slot(step) * half + first * quarter
            return cols.at[base : base + count * quarter, :]

        def forward(step, name, *directions):
            for way in directions:
                move = ahead[way]
                lands = (step[0] - move[0], step[1] - move[1])
                push(piece_of(step, name), piece_of(lands, name), gat_s,
                     gat_r.at[port(lands, name)], {"dp": shift(move)})

        def landed(step, name):
            arrived(piece_of(step, name), gat_r.at[port(step, name)])

        for way in ("Y-", "Y+"):
            forward((0, 0), "A", way)
        for way in ("Z-", "Z+"):
            forward((0, 0), "B", way)
        for way in ("Y-", "Y+"):
            forward((0, 0), "B", way)
        for way in ("Z-", "Z+"):
            forward((0, 0), "A", way)

        for load in loads[2:]:
            load.wait()
        h_own[s] = hidden[tile(e, chunk), :]
        mate = (1 - s) * n_mp + m
        push(hidden.at[tile(mate, chunk), :], h_own.at[s], h_s, h_r, {"section": 1 - s})
        w_in, w_out = wi_all.at[e], wo_all.at[e]
        ww = ((w_in, wi_all), (w_out, wo_all))
        z_at, y_at = d // RING, lax.rem(d, RING)
        cell = (z_at * RING + y_at, y_at * RING + z_at)
        band = (z_at, y_at)
        cross = far(2) * CORES + core
        bit = w_in.shape[0] // n_dp

        def along(which, step):
            return {"dp": shift((0, step) if which == 0 else (step, 0))}

        for which in (0, 1):
            part = tile(cell[which], bit)
            push(ww[which][0].at[part, :], ww[which][1].at[e, part, :], wc_s.at[which],
                 wc_r.at[which, 0], at(far(2), core))
        top = pl.ds(0, w_in.shape[0] // 2)
        rest = pl.ds(w_in.shape[0] // 2, w_in.shape[0] // 2)

        def neighbour(which, toward, part):
            push(ww[which][0].at[part, :], ww[which][1].at[e, part, :], ww_s.at[which],
                 ww_r.at[which, 1 if toward == 1 else 0], at(far(toward), core))

        def both_ways(which):
            for part in (top, rest):
                neighbour(which, line - 1, part)
                neighbour(which, 1, part)

        both_ways(0)

        for which in (0, 1):
            push(ww[which][0], ww[which][1].at[e], ww_s.at[which], ww_r.at[which, 2],
                 at(spot, sib))

        def cross_first(which):
            mine_bit = ww[which][1].at[cross, tile(cell[which], bit), :]
            arrived(mine_bit, wc_r.at[which, 0])
            for k in range(1, RING):
                push(mine_bit, mine_bit, wc_s.at[which], wc_r.at[which, 1],
                     along(which, k))

        def cross_second(which):
            arrived(ww[which][1].at[cross, 0 : (RING - 1) * bit, :], wc_r.at[which, 1])
            group = ww[which][1].at[cross, tile(band[which], RING * bit), :]
            for k in range(1, RING):
                push(group, group, wc_s.at[which], wc_r.at[which, 2],
                     along(1 - which, k))

        def cross_third(which):
            arrived(ww[which][1].at[cross, 0 : (RING - 1) * RING * bit, :], wc_r.at[which, 2])
            push(ww[which][1].at[cross], ww[which][1].at[cross], ww_s.at[which],
                 ww_r.at[which, 2 if which else 3], at(spot, sib))

        def relay_weight(which, step):
            index = far(step) * CORES + core
            buf = ww[which][1].at[index]
            arrived(buf, ww_r.at[which, 0 if step == 1 else 1])
            push(buf, buf, ww_s.at[which], ww_r.at[which, 2], at(spot, sib))

        def sigmoid(pre):
            return 1.0 / (1.0 + jnp.exp(-GELU * pre))

        with jax.named_scope("b_pre"):
            loads[1].wait()
            for i, hop in enumerate(hops):
                unit, _ = unit_rows(text[tile(far(hop), pair), :])
                text_low[i * pair : (i + 1) * pair, :] = unit.astype(BF16)

            @pl.loop(0, line)
            def _(r):
                pre = dot_nn(hidden[tile(r, pair), :], w_in[...])
                sigm = sigmoid(pre)
                act_all[tile(r, pair), :] = (pre * sigm).astype(BF16)
                slope_all[tile(r, pair), :] = sigm + GELU * pre * sigm * (1.0 - sigm)

        def group_scores(*group, fresh=False):
            piece = [cols[slot(k) * half : (slot(k) + 1) * half, :] for k in group]
            piece = piece[0] if len(piece) == 1 else jnp.concatenate(piece, axis=0)
            peak = total = None
            for r in range(line):
                part = pl.ds(r * pair, pair)
                value = mult2 * dot_nt(text_low[part, :], piece)
                blocks = [value[:, k * half : (k + 1) * half] for k in range(len(group))]
                for k, block in zip(group, blocks):
                    scores[slot(k), part, :] = block
                best = blocks[0]
                for block in blocks[1:]:
                    best = jnp.maximum(best, block)
                if not fresh:
                    best = jnp.maximum(best, row_max[part, :])
                    mass = row_sum[part, :] * jnp.exp2(row_max[part, :] - best)
                    for block in blocks:
                        mass = mass + jnp.exp2(block - best)
                    row_sum[part, :] = mass
                else:
                    row_sum[part, :] = jnp.ones(best.shape, F32)
                row_max[part, :] = best
                high = jnp.max(value, axis=0, keepdims=True)
                if peak is None:
                    peak = high
                    total = jnp.sum(jnp.exp2(value - peak), axis=0, keepdims=True)
                else:
                    high = jnp.maximum(peak, high)
                    total = total * jnp.exp2(peak - high) + jnp.sum(
                        jnp.exp2(value - high), axis=0, keepdims=True)
                    peak = high
            level = peak + jnp.log(total) * LOG2E
            for k, step in enumerate(group):
                p = shift(step)
                col_st[pl.ds(p, 1), :] = level[:, k * half : (k + 1) * half]

        with jax.named_scope("c_own"):
            group_scores((0, 0), fresh=True)

        with jax.named_scope("c_blocks"):
            landed((0, 1), "A")
            forward((0, 1), "A0", "Y-")
            forward((0, 1), "A", "Z-", "Z+")
            landed((1, 0), "B")
            forward((1, 0), "B0", "Z-")
            forward((1, 0), "B", "Y-", "Y+")
            landed((0, 3), "A")
            forward((0, 3), "A1", "Y+")
            forward((0, 3), "A", "Z-", "Z+")
            landed((3, 0), "B")
            forward((3, 0), "B1", "Z+")
            forward((3, 0), "B", "Y-", "Y+")
            landed((0, 1), "B")
            forward((0, 1), "B0", "Y-")
            landed((1, 0), "A")
            forward((1, 0), "A0", "Z-")
            landed((0, 3), "B")
            forward((0, 3), "B1", "Y+")
            landed((3, 0), "A")
            forward((3, 0), "A1", "Z+")
            group_scores((0, 1), (0, 3))
            group_scores((1, 0), (3, 0))
            for name in ("A0", "A1"):
                landed((0, 2), name)
                forward((0, 2), name, "Z-", "Z+")
            for name in ("B0", "B1"):
                landed((2, 0), name)
                forward((2, 0), name, "Y-", "Y+")
            for dy in (1, 3):
                landed((1, dy), "A")
                forward((1, dy), "A0", "Z-")
                landed((3, dy), "A")
                forward((3, dy), "A1", "Z+")
            for dz in (1, 3):
                landed((dz, 1), "B")
                forward((dz, 1), "B0", "Y-")
                landed((dz, 3), "B")
                forward((dz, 3), "B1", "Y+")
            cross_first(0)
            cross_first(1)
            group_scores((1, 1), (1, 3))
            group_scores((3, 1), (3, 3))
            landed_all("a")
            group_scores((0, 2), (2, 0))
            landed_all("b")
            forward((1, 2), "A0", "Z-")
            forward((3, 2), "A1", "Z+")
            forward((2, 1), "B0", "Y-")
            forward((2, 3), "B1", "Y+")
            landed_all("c")
            group_scores((1, 2), (3, 2))
            landed_all("d")
            group_scores((2, 1), (2, 3))
            landed_all("e")
            group_scores((2, 2))

        with jax.named_scope("d_colsend"):
            col_rx[d] = col_st[...]
            for p in others(d, n_dp):
                push(col_st, col_rx.at[d], cs_s, cs_r, {"dp": p})

        with jax.named_scope("e_rowstat"):
            for r in range(n_el):
                part = pl.ds(r * chunk, chunk)
                place = far(hops[r // CORES]) * CORES + r % CORES
                peak = jnp.max(row_max[part, :], axis=1, keepdims=True)
                acc = jnp.sum(row_sum[part, :] * jnp.exp2(row_max[part, :] - peak), axis=1,
                              keepdims=True)
                level = peak + jnp.log(acc) * LOG2E
                row_st[pl.ds(place, 1), :] = jnp.broadcast_to(level, (chunk, LANES)).T[0:1, :]
            row_rx[e] = row_st[...]
            for q in others(e, n_el):
                push(row_st, row_rx.at[e], rs_s, rs_r,
                     {"section": q // n_mp, "mp": lax.rem(q, n_mp)})
            both_ways(1)

        def merge(rx, count):
            peak = rx[0]
            for k in range(1, count):
                peak = jnp.maximum(peak, rx[k])
            acc = jnp.zeros(peak.shape, F32)
            for k in range(count):
                acc = acc + jnp.exp2(rx[k] - peak)
            return peak + (jnp.log(acc) * LOG2E + 1.0)

        def slopes(index):
            pre = dot_nn(h_own[index // n_mp], wi_all[index])
            sigm = sigmoid(pre)
            slope_own[index] = sigm + GELU * pre * sigm * (1.0 - sigm)

        with jax.named_scope("f_cross"):
            cross_second(0)
            cross_second(1)
            relay_weight(0, 1)
            relay_weight(0, line - 1)
            arrived(h_own.at[1 - s], h_r)
            for step in (0, 1, line - 1):
                slopes(far(step) * CORES + core)
            arrived(wi_all.at[0:3], ww_r.at[0, 2])
            for step in (0, 1, line - 1):
                slopes(far(step) * CORES + sib)

        with jax.named_scope("f_merge"):
            arrived(col_rx.at[0 : n_dp - 1], cs_r)
            col_lse[...] = merge(col_rx, n_dp)
            arrived(row_rx.at[0 : n_el - 1], rs_r)
            row_mix[...] = merge(row_rx, n_el)
            for r in range(n_el):
                place = far(hops[r // CORES]) * CORES + r % CORES
                row_lse[r * chunk : (r + 1) * chunk, :] = jnp.broadcast_to(
                    row_mix[pl.ds(place, 1), :], (LANES, chunk)).T

        def score_rows(i):
            part = slice(i * pair, (i + 1) * pair)
            base = row_lse[part, :]
            offset = (m - far(hops[i])) * pair + s * half
            for step in steps:
                k = slot(step)
                value = scores[k, part, :]
                low = col_lse[pl.ds(shift(step), 1), :]
                both = jnp.exp2(value - base) + jnp.exp2(value - low)
                if k == 0:
                    diagonal = lax.broadcasted_iota(jnp.int32, (pair, half), 0) == (
                        lax.broadcasted_iota(jnp.int32, (pair, half), 1) + offset)
                    both = both - jnp.where(diagonal, 1.0, 0.0)
                sgrad[part, k * half : (k + 1) * half] = both.astype(BF16)

        def join(where):
            arrived(t_sr.at[where], ts_r.at[where])
            return t_keep[where] + t_sr[where].astype(F32)


        with jax.named_scope("g_scorerows"):
            score_rows(0)
            for i, hop in enumerate(hops):
                where = far(hop)
                t_full[...] = dot_nn(sgrad[i * pair : (i + 1) * pair, :], cols[...])
                if i + 1 < line:
                    score_rows(i + 1)
                t_sx[where] = t_full[tile(sib, chunk), :].astype(BF16)
                push(t_sx.at[where], t_sr.at[where], ts_s, ts_r.at[where], at(spot, sib))
                t_keep[where] = t_full[tile(core, chunk), :]
                if i > 0:
                    last = far(hops[i - 1])
                    t_tx[last] = join(last).astype(BF16)
                    push(t_tx.at[last], t_rx.at[spot - (spot > last).astype(jnp.int32)], tc_s, tc_r,
                         at(last, core))

        with jax.named_scope("g_relay"):
            cross_third(0)
            cross_third(1)

        fold = feats // 2

        with jax.named_scope("h_image"):
            for g in (2, 1, 3, 0):
                for which in (0, 1):
                    ends = [(g, k) if which == 0 else (k, g) for k in range(RING)]
                    block = jnp.concatenate(
                        [sgrad[:, slot(k) * half : (slot(k) + 1) * half] for k in ends], axis=1)
                    part = dot_tn(block, text_low[:, which * fold : (which + 1) * fold])
                    for k in range(RING):
                        if g == 0:
                            i_own[which, k] = part[k * half : (k + 1) * half, :]
                        else:
                            i_tx[which, g, k] = part[k * half : (k + 1) * half, :].astype(BF16)
                    if g > 0:
                        push(i_tx.at[which, g], i_rx.at[which, RING - g], im_s, im_r.at[which, 0],
                             along(1 - which, g))

        def image_second():
            for which in (0, 1):
                arrived(i_rx.at[which, 1:RING], im_r.at[which, 0])
                for g in (2, 1, 3, 0):
                    total = i_own[which, g]
                    for k in range(1, RING):
                        total = total + i_rx[which, k, g].astype(F32)
                    if g == 0:
                        i_own[which, 0] = total
                    else:
                        i_st[which, g] = total.astype(BF16)
                        push(i_st.at[which, g], i_end.at[which, RING - g],
                             im_s, im_r.at[which, 1], along(which, g))

        mine = tile(e, chunk)

        with jax.named_scope("j_weights"):
            relay_weight(1, 1)
            relay_weight(1, line - 1)
            slopes(cross)
            arrived(wi_all.at[0], ww_r.at[0, 3])
            slopes(far(2) * CORES + sib)
            arrived(wo_all.at[0:line], ww_r.at[1, 2])

        with jax.named_scope("i_topgrad"):
            total = join(spot)
            arrived(t_rx.at[0 : line - 1], tc_r)
            for k in range(line - 1):
                total = total + t_rx[k].astype(F32)
            unit, length = unit_rows(text[mine, :])
            g_st[n_sec - 1] = unit_backward(unit, length, mult * total).astype(BF16)

        def spread(layer):
            for c in range(chips):
                place = layer * chips + c

                @pl.when(spot != place)
                def _():
                    copy(g_st.at[layer], g_all.at[e], gs_s, gs_r.at[e],
                         at(place, core)).start()

            @pl.when(s == layer)
            def _():
                g_all[e] = g_st[layer]
                copy(g_st.at[layer], g_all.at[e], gs_s, gs_r.at[e],
                     at(spot, sib)).start()

        def feed_forward(layer):
            spread(layer)
            total = g_st[layer].astype(F32)
            for j in range(n_mp):
                index = layer * n_mp + j
                back = dot_nt(g_st[layer], wo_all[index])
                grad = (back * slope_own[index]).astype(BF16)
                total = total + dot_nt(grad, wi_all[index])
            if layer > 0:
                g_st[layer - 1] = total.astype(BF16)
            else:
                for t in range(n_sec):
                    in_st[t] = total[:, t * width : (t + 1) * width].astype(BF16)

        def slab(k):
            return input_out.at[tile(k, chunk), :]

        with jax.named_scope("k_ffn"):
            for layer in range(n_sec - 1, -1, -1):
                feed_forward(layer)

        def weight_rows(k):
            back = dot_nt(g_all[k], w_out[...])
            pre_all[tile(k, chunk), :] = (back * slope_all[tile(k, chunk), :]).astype(BF16)

        with jax.named_scope("m_weightrows"):
            weight_rows(e)
            for hop in (1, 3, 2) if line == 4 else range(1, line):
                index = far(hop) * CORES + core
                arrived(g_all.at[index], gs_r.at[index])
                push(g_all.at[index], g_all.at[index], gs_s, gs_r.at[index],
                     at(spot, sib))
                weight_rows(index)
            input_out[mine, :] = in_st[s]
            push(in_st.at[s], slab(e), in_s, in_r.at[0], at(spot, sib))
            for hop in hops[:-1]:
                where = far(hop)
                push(in_st.at[where // chips], slab(e), in_s, in_r.at[line - hop],
                     at(where, core))
            image_second()
            for hop in (0, 1, 3, 2) if line == 4 else range(line):
                index = far(hop) * CORES + sib
                arrived(g_all.at[index], gs_r.at[index])
                weight_rows(index)

        def send_weights(which):
            for k in (2, 1, 3):
                other = lax.rem(band[which] + k, RING)
                push(w_tx.at[which, tile(other, RING * share), :], w_rx.at[which, RING - k],
                     w_s, w_r.at[which, 0], along(1 - which, k))

        def weight_second(which):
            total = w_full[which, tile(band[which], RING * share), :]
            arrived(w_rx.at[which, 1:RING], w_r.at[which, 0])
            for k in (1, 3, 2):
                total = total + w_rx[which, k].astype(F32)
            w_sum[which] = total
            w_st[which] = total.astype(BF16)
            for k in (2, 1, 3):
                other = lax.rem(band[1 - which] + k, RING)
                push(w_st.at[which, tile(other, share), :], w_end.at[which, RING - k],
                     w_s, w_r.at[which, 1], along(which, k))

        def weight_last(which, out):
            total = w_sum[which, tile(band[1 - which], share), :]
            arrived(w_end.at[which, 1:RING], w_r.at[which, 1])
            for k in (1, 3, 2):
                total = total + w_end[which, k].astype(F32)
            out[...] = total

        with jax.named_scope("n_wgrad"):
            g_rows = g_all[...].reshape(rows, feats)
            grad = dot_tn(g_rows, act_all[...])
            for p in range(n_dp):
                q = (p % RING) * RING + p // RING
                w_full[1, q * share : (q + 1) * share, :] = grad[p * share : (p + 1) * share, :]
                w_tx[1, q * share : (q + 1) * share, :] = grad[
                    p * share : (p + 1) * share, :].astype(BF16)
            send_weights(1)
            grad = dot_tn(hidden[...], pre_all[...])
            w_full[0] = grad
            w_tx[0] = grad.astype(BF16)
            send_weights(0)

        with jax.named_scope("q_image"):
            image_half = tile(s, half)
            unit, length = unit_rows(image[image_half, :])
            sides = []
            for which in (0, 1):
                total = i_own[which, 0]
                arrived(i_end.at[which, 1:RING], im_r.at[which, 1])
                for k in (1, 3, 2):
                    total = total + i_end[which, k].astype(F32)
                sides.append(total)
            image_out[image_half, :] = unit_backward(
                unit, length, mult * jnp.concatenate(sides, axis=1)).astype(BF16)
            push(image_out.at[image_half, :], image_out.at[image_half, :], io_s, io_r,
                 {"section": 1 - s})

        with jax.named_scope("o_inrelay"):
            for hop in hops[:-1]:
                index = far(hop) * CORES + core
                arrived(slab(index), in_r.at[hop])
                push(slab(index), slab(index), in_s, in_r.at[0], at(spot, sib))

        with jax.named_scope("p_wsecond"):
            weight_second(1)
            weight_second(0)

        with jax.named_scope("q_wsum"):
            weight_last(1, second_out)
            weight_last(0, first_out)

        with jax.named_scope("r_drain"):
            arrived(input_out.at[0 : line * chunk, :], in_r.at[0])
            arrived(image_out.at[tile(1 - s, half), :], io_r)
            left(hidden.at[0:chunk, :], h_s)
            left(cols.at[0 : 15 * half, :], gat_s)
            left(col_rx.at[0 : n_dp - 1], cs_s)
            left(row_rx.at[0 : n_el - 1], rs_s)
            for which in (0, 1):
                left(ww[which][1].at[0:6], ww_s.at[which])
                left(ww[which][1].at[0], wc_s.at[which])
            left(t_sx, ts_s)
            left(t_tx.at[0 : line - 1], tc_s)
            left(g_all.at[0 : 2 * n_sec + line - 1], gs_s)
            left(input_out.at[0 : (2 * line - 1) * chunk, :], in_s)
            left(text.at[0 : 2 * (RING - 1) * (RING + 1) * share, :], w_s)
            left(cols.at[0 : 15 * half, :], im_s)
            left(image_out.at[0:half, :], io_s)

    return kernel


def solution(mesh):
    n_sec, n_dp, n_mp = mesh.shape["section"], mesh.shape["dp"], mesh.shape["mp"]

    def body(text, image, scale, hidden, w_in, w_out):
        rows, feats = text.shape
        own = image.shape[0]
        hid = w_in.shape[2]
        half, share = own // n_sec, feats // n_dp
        columns = half * n_dp
        line = n_sec * n_mp // CORES
        n_el = n_sec * n_mp
        chunk = rows // n_el
        dma = pltpu.SemaphoreType.DMA
        vmem = pl.BlockSpec(memory_space=pltpu.VMEM)
        hbm = pl.BlockSpec(memory_space=pltpu.HBM)
        out = pl.pallas_call(
            make_kernel(n_sec, n_dp, n_mp),
            out_shape=(
                pltpu.VMEM((own, feats), BF16),
                pltpu.VMEM((rows, feats // n_sec), BF16),
                pltpu.VMEM((share, hid), F32),
                pltpu.VMEM((share, hid), F32),
            ),
            in_specs=[hbm, hbm, pl.BlockSpec(memory_space=pltpu.SMEM), hbm, hbm, hbm],
            out_specs=(vmem,) * 4,
            scratch_shapes=[
                pltpu.VMEM((rows, feats), BF16),
                pltpu.VMEM((own, feats), BF16),
                pltpu.VMEM((rows, feats), BF16),
                pltpu.VMEM((rows, feats), BF16),
                pltpu.VMEM((columns, feats), BF16),
                pltpu.VMEM((n_dp, rows, half), F32),
                pltpu.VMEM((rows, columns), BF16),
                pltpu.VMEM((rows, LANES), F32),
                pltpu.VMEM((rows, LANES), F32),
                pltpu.VMEM((rows, LANES), F32),
                pltpu.VMEM((n_dp, half), F32),
                pltpu.VMEM((n_el, chunk), F32),
                pltpu.VMEM((n_el, n_el, chunk), F32),
                pltpu.VMEM((n_el, chunk), F32),
                pltpu.VMEM((n_dp, half), F32),
                pltpu.VMEM((n_dp, n_dp, half), F32),
                pltpu.VMEM((n_el, feats, hid), BF16),
                pltpu.VMEM((n_el, hid, feats), BF16),
                pltpu.VMEM((n_sec, chunk, feats), BF16),
                pltpu.VMEM((CORES * chunk, feats), F32),
                pltpu.VMEM((line, chunk, feats), F32),
                pltpu.VMEM((line, chunk, feats), BF16),
                pltpu.VMEM((line, chunk, feats), BF16),
                pltpu.VMEM((line, chunk, feats), BF16),
                pltpu.VMEM((line, chunk, feats), BF16),
                pltpu.VMEM((n_sec, chunk, feats), BF16),
                pltpu.VMEM((n_el, chunk, feats), BF16),
                pltpu.VMEM((n_el, chunk, hid), F32),
                pltpu.VMEM((n_sec, chunk, feats // n_sec), BF16),
                pltpu.VMEM((rows, hid), BF16),
                pltpu.VMEM((rows, hid), F32),
                pltpu.VMEM((rows, hid), BF16),
                pltpu.VMEM((2, feats, hid), F32),
                pltpu.VMEM((2, feats, hid), BF16),
                pltpu.VMEM((2, RING, RING * share, hid), BF16),
                pltpu.VMEM((2, RING * share, hid), F32),
                pltpu.VMEM((2, RING * share, hid), BF16),
                pltpu.VMEM((2, RING, share, hid), BF16),
                pltpu.VMEM((2, RING, RING, half, feats // 2), BF16),
                pltpu.VMEM((2, RING, RING, half, feats // 2), BF16),
                pltpu.VMEM((2, RING, half, feats // 2), F32),
                pltpu.VMEM((2, RING, half, feats // 2), BF16),
                pltpu.VMEM((2, RING, half, feats // 2), BF16),
                dma, dma((25,)), dma, dma, dma, dma, dma((2,)), dma((2, 4)), dma, dma,
                dma, dma((line,)), dma, dma, dma, dma((n_el,)), dma, dma((line,)),
                dma((5,)), dma((2,)), dma((2, 3)), dma, dma((2, 2)), dma, dma((2, 2)), dma, dma,
            ],
            compiler_params=pltpu.CompilerParams(
                collective_id=0, has_side_effects=True, vmem_limit_bytes=57000000
            ),
        )(text, image, scale, hidden[0], w_in[0], w_out[0])
        image_grad, input_grad, first, second = pl.pallas_call(
            leave,
            out_shape=tuple(jax.ShapeDtypeStruct(x.shape, x.dtype) for x in out),
            in_specs=[vmem] * 4,
            out_specs=(hbm,) * 4,
            scratch_shapes=[dma((4,))],
            compiler_params=pltpu.CompilerParams(vmem_limit_bytes=4000000),
        )(*out)
        return (image_grad, input_grad, first[None], second[None])

    return jax.shard_map(
        body,
        mesh=mesh,
        in_specs=(
            P("dp", None),
            P(("dp", "mp"), None),
            P(),
            P("section", "dp", None),
            P("section", None, "mp"),
            P("section", "mp", None),
        ),
        out_specs=(
            P(("dp", "mp"), None),
            P("dp", "section"),
            P("section", "dp", "mp"),
            P("section", "dp", "mp"),
        ),
        check_vma=False,
    )
```

```python
import jax
import jax.numpy as jnp
from jax import lax
from jax.experimental import pallas as pl
from jax.experimental.pallas import tpu as pltpu
from jax.sharding import PartitionSpec as P

MESH = pl.DeviceIdType.MESH
F32 = jnp.float32
BF16 = jnp.bfloat16
GELU = 1.702
LOG2E = 1.4426950408889634
LANES = 128
CORES = 2
RING = 4


def unit_rows(values):
    wide = values.astype(F32)
    length = jnp.sqrt(jnp.sum(wide * wide, axis=1, keepdims=True) + 1.0)
    return (wide / length, length)


def unit_backward(unit, length, grad_unit):
    return (grad_unit - unit * jnp.sum(unit * grad_unit, axis=1, keepdims=True)) / length


def dot_nn(a, b):
    return lax.dot_general(a, b, (((1,), (0,)), ((), ())), preferred_element_type=F32)


def dot_nt(a, b):
    return lax.dot_general(a, b, (((1,), (1,)), ((), ())), preferred_element_type=F32)


def dot_tn(a, b):
    return lax.dot_general(a, b, (((0,), (0,)), ((), ())), preferred_element_type=F32)


def tile(index, size):
    return pl.ds(pl.multiple_of(index * size, size), size)


def leave(*refs):
    copies = [pltpu.make_async_copy(refs[k], refs[4 + k], refs[8].at[k]) for k in range(4)]
    for c in copies:
        c.start()
    for c in copies:
        c.wait()


def make_kernel(n_sec, n_dp, n_mp):
    chips = n_mp // CORES
    line = n_sec * chips
    n_el = n_sec * n_mp

    def kernel(
        text_hbm, image_hbm, scale_ref, hidden_hbm, w_in_hbm, w_out_hbm,
        image_out, input_out, first_out, second_out,
        text, image, hidden, text_low, cols, scores, sgrad, row_max, row_sum, row_part, col_lse, row_st, row_rx, row_mix, col_st, col_rx,
        wi_all, wo_all, h_own, t_full, t_keep, t_sx, t_sr, t_tx, t_rx,
        g_st, g_all, slope_own, in_st, act_all, slope_all, pre_all,
        w_full, w_tx, w_rx, w_sum, w_st, w_end, i_tx, i_rx, i_own, i_st, i_end,
        gat_s, gat_r, cs_s, cs_r, rs_s, rs_r, ww_s, ww_r, h_s, h_r,
        ts_s, ts_r, tc_s, tc_r, gs_s, gs_r, in_s, in_r,
        ld_s, wc_s, wc_r, w_s, w_r, im_s, im_r, io_s, io_r,
    ):
        s = lax.axis_index("section")
        d = lax.axis_index("dp")
        m = lax.axis_index("mp")
        rows, feats = text.shape
        own = image.shape[0]
        half = own // n_sec
        chunk = rows // n_el
        pair = rows // line
        share = feats // n_dp
        width = feats // n_sec
        mult = scale_ref[0]
        mult2 = mult * LOG2E
        core = lax.rem(m, CORES)
        sib = 1 - core
        spot = s * chips + m // CORES
        e = s * n_mp + m

        def at(place, who):
            return {"section": place // chips, "mp": lax.rem(place, chips) * CORES + who}

        def far(step):
            return lax.rem(spot + step, line)

        def copy(src, dst, send, recv, where):
            return pltpu.make_async_remote_copy(
                src_ref=src, dst_ref=dst, send_sem=send, recv_sem=recv,
                device_id=where, device_id_type=MESH,
            )

        def arrived(ref, recv):
            copy(ref, ref, h_s, recv, at(spot, sib)).wait_recv()

        def shift(step):
            dz, dy = step[0] % RING, step[1] % RING
            z = lax.rem(d // RING + dz, RING)
            return z * RING + lax.rem(lax.rem(d, RING) + dy, RING)

        def slot(step):
            return (step[0] % RING) * RING + step[1] % RING

        steps = [(a, b) for a in range(RING) for b in range(RING)]

        def away(step):
            return (-step[0] % RING, -step[1] % RING)

        hops = (2, 3, 1, 0) if line == 4 else tuple(range(line - 1, -1, -1))

        def others(mine, count):
            return [lax.rem(mine + k, count) for k in range(1, count)]

        def sources(mine, count):
            return [lax.rem(mine + count - k, count) for k in range(1, count)]

        def push(*args):
            copy(*args).start()

        def left(ref, send):
            copy(ref, ref, send, h_r, at(spot, sib)).wait_send()

        with jax.named_scope("a_barrier"):
            loads = [
                pltpu.make_async_copy(src, dst, ld_s.at[k])
                for k, (src, dst) in enumerate((
                    (image_hbm, image), (text_hbm, text), (hidden_hbm, hidden),
                    (w_in_hbm, wi_all.at[e]), (w_out_hbm, wo_all.at[e]),
                ))
            ]
            for load in loads:
                load.start()
            barrier = pltpu.get_barrier_semaphore()
            for near in ((0, 1), (0, -1), (1, 0), (-1, 0)):
                pl.semaphore_signal(
                    barrier, inc=1, device_id={"dp": shift(near)}, device_id_type=MESH)
            for q in others(e, n_el):
                pl.semaphore_signal(
                    barrier, inc=1, device_id={"section": q // n_mp, "mp": lax.rem(q, n_mp)},
                    device_id_type=MESH,
                )
            loads[0].wait()
            own_unit, _ = unit_rows(image[tile(s, half), :])
            cols[0:half, :] = own_unit.astype(BF16)
            pl.semaphore_wait(barrier, n_el + 3)

        quarter = half // 4
        spans = {"A": (0, 2), "B": (2, 2), "A0": (0, 1), "A1": (1, 1), "B0": (2, 1), "B1": (3, 1)}
        ahead = {"Y-": (0, -1), "Y+": (0, 1), "Z-": (-1, 0), "Z+": (1, 0)}
        quads = {
            "a": [((0, 2), "B0"), ((0, 2), "B1"), ((2, 0), "A0"), ((2, 0), "A1")],
            "b": [(k, name) for k in ((1, 2), (3, 2)) for name in ("A0", "A1")]
            + [(k, name) for k in ((2, 1), (2, 3)) for name in ("B0", "B1")],
            "c": [(k, name) for k in ((1, 2), (3, 2)) for name in ("B0", "B1")],
            "d": [(k, name) for k in ((2, 1), (2, 3)) for name in ("A0", "A1")],
            "e": [((2, 2), name) for name in ("A0", "A1", "B0", "B1")],
        }
        ports = {}

        def port(step, name):
            key = (slot(step), name)
            for group, members in quads.items():
                if any(key == (slot(k), other) for k, other in members):
                    key = group
            return ports.setdefault(key, len(ports))

        def landed_all(group):
            count = len(quads[group])
            k, name = quads[group][0]
            arrived(cols.at[0 : count * quarter, :], gat_r.at[port(k, name)])

        def piece_of(step, name):
            first, count = spans[name]
            base = slot(step) * half + first * quarter
            return cols.at[base : base + count * quarter, :]

        def forward(step, name, *directions):
            for way in directions:
                move = ahead[way]
                lands = (step[0] - move[0], step[1] - move[1])
                push(piece_of(step, name), piece_of(lands, name), gat_s,
                     gat_r.at[port(lands, name)], {"dp": shift(move)})

        def landed(step, name):
            arrived(piece_of(step, name), gat_r.at[port(step, name)])

        for way in ("Y-", "Y+"):
            forward((0, 0), "A", way)
        for way in ("Z-", "Z+"):
            forward((0, 0), "B", way)
        for way in ("Y-", "Y+"):
            forward((0, 0), "B", way)
        for way in ("Z-", "Z+"):
            forward((0, 0), "A", way)

        for load in loads[2:]:
            load.wait()
        h_own[s] = hidden[tile(e, chunk), :]
        mate = (1 - s) * n_mp + m
        push(hidden.at[tile(mate, chunk), :], h_own.at[s], h_s, h_r, {"section": 1 - s})
        w_in, w_out = wi_all.at[e], wo_all.at[e]
        ww = ((w_in, wi_all), (w_out, wo_all))
        z_at, y_at = d // RING, lax.rem(d, RING)
        cell = (z_at * RING + y_at, y_at * RING + z_at)
        band = (z_at, y_at)
        cross = far(2) * CORES + core
        bit = w_in.shape[0] // n_dp

        def along(which, step):
            return {"dp": shift((0, step) if which == 0 else (step, 0))}

        for which in (0, 1):
            part = tile(cell[which], bit)
            push(ww[which][0].at[part, :], ww[which][1].at[e, part, :], wc_s.at[which],
                 wc_r.at[which, 0], at(far(2), core))
        top = pl.ds(0, w_in.shape[0] // 2)
        rest = pl.ds(w_in.shape[0] // 2, w_in.shape[0] // 2)

        def neighbour(which, toward, part):
            push(ww[which][0].at[part, :], ww[which][1].at[e, part, :], ww_s.at[which],
                 ww_r.at[which, 1 if toward == 1 else 0], at(far(toward), core))

        def both_ways(which):
            for part in (top, rest):
                neighbour(which, line - 1, part)
                neighbour(which, 1, part)

        both_ways(0)

        for which in (0, 1):
            push(ww[which][0], ww[which][1].at[e], ww_s.at[which], ww_r.at[which, 2],
                 at(spot, sib))

        def cross_first(which):
            mine_bit = ww[which][1].at[cross, tile(cell[which], bit), :]
            arrived(mine_bit, wc_r.at[which, 0])
            for k in range(1, RING):
                push(mine_bit, mine_bit, wc_s.at[which], wc_r.at[which, 1],
                     along(which, k))

        def cross_second(which):
            arrived(ww[which][1].at[cross, 0 : (RING - 1) * bit, :], wc_r.at[which, 1])
            group = ww[which][1].at[cross, tile(band[which], RING * bit), :]
            for k in range(1, RING):
                push(group, group, wc_s.at[which], wc_r.at[which, 2],
                     along(1 - which, k))

        def cross_third(which):
            arrived(ww[which][1].at[cross, 0 : (RING - 1) * RING * bit, :], wc_r.at[which, 2])
            push(ww[which][1].at[cross], ww[which][1].at[cross], ww_s.at[which],
                 ww_r.at[which, 2 if which else 3], at(spot, sib))

        def relay_weight(which, step):
            index = far(step) * CORES + core
            buf = ww[which][1].at[index]
            arrived(buf, ww_r.at[which, 0 if step == 1 else 1])
            push(buf, buf, ww_s.at[which], ww_r.at[which, 2], at(spot, sib))

        def sigmoid(pre):
            return 1.0 / (1.0 + jnp.exp(-GELU * pre))

        with jax.named_scope("b_pre"):
            loads[1].wait()
            for i, hop in enumerate(hops):
                unit, _ = unit_rows(text[tile(far(hop), pair), :])
                text_low[i * pair : (i + 1) * pair, :] = unit.astype(BF16)

            @pl.loop(0, line)
            def _(r):
                pre = dot_nn(hidden[tile(r, pair), :], w_in[...])
                sigm = sigmoid(pre)
                act_all[tile(r, pair), :] = (pre * sigm).astype(BF16)
                slope_all[tile(r, pair), :] = sigm + GELU * pre * sigm * (1.0 - sigm)

        def group_scores(*group, fresh=False):
            piece = [cols[slot(k) * half : (slot(k) + 1) * half, :] for k in group]
            piece = piece[0] if len(piece) == 1 else jnp.concatenate(piece, axis=0)
            peak = total = None
            for r in range(line):
                part = pl.ds(r * pair, pair)
                value = mult2 * dot_nt(text_low[part, :], piece)
                blocks = [value[:, k * half : (k + 1) * half] for k in range(len(group))]
                for k, block in zip(group, blocks):
                    scores[slot(k), part, :] = block
                best = blocks[0]
                for block in blocks[1:]:
                    best = jnp.maximum(best, block)
                if not fresh:
                    best = jnp.maximum(best, row_max[part, :])
                    mass = row_sum[part, :] * jnp.exp2(row_max[part, :] - best)
                    for block in blocks:
                        mass = mass + jnp.exp2(block - best)
                    row_sum[part, :] = mass
                else:
                    row_sum[part, :] = jnp.ones(best.shape, F32)
                row_max[part, :] = best
                high = jnp.max(value, axis=0, keepdims=True)
                if peak is None:
                    peak = high
                    total = jnp.sum(jnp.exp2(value - peak), axis=0, keepdims=True)
                else:
                    high = jnp.maximum(peak, high)
                    total = total * jnp.exp2(peak - high) + jnp.sum(
                        jnp.exp2(value - high), axis=0, keepdims=True)
                    peak = high
            level = peak + jnp.log(total) * LOG2E
            for k, step in enumerate(group):
                p = shift(step)
                col_st[pl.ds(p, 1), :] = level[:, k * half : (k + 1) * half]

        with jax.named_scope("c_own"):
            group_scores((0, 0), fresh=True)

        with jax.named_scope("c_blocks"):
            landed((0, 1), "A")
            forward((0, 1), "A0", "Y-")
            forward((0, 1), "A", "Z-", "Z+")
            landed((1, 0), "B")
            forward((1, 0), "B0", "Z-")
            forward((1, 0), "B", "Y-", "Y+")
            landed((0, 3), "A")
            forward((0, 3), "A1", "Y+")
            forward((0, 3), "A", "Z-", "Z+")
            landed((3, 0), "B")
            forward((3, 0), "B1", "Z+")
            forward((3, 0), "B", "Y-", "Y+")
            landed((0, 1), "B")
            forward((0, 1), "B0", "Y-")
            landed((1, 0), "A")
            forward((1, 0), "A0", "Z-")
            landed((0, 3), "B")
            forward((0, 3), "B1", "Y+")
            landed((3, 0), "A")
            forward((3, 0), "A1", "Z+")
            group_scores((0, 1), (0, 3))
            group_scores((1, 0), (3, 0))
            for name in ("A0", "A1"):
                landed((0, 2), name)
                forward((0, 2), name, "Z-", "Z+")
            for name in ("B0", "B1"):
                landed((2, 0), name)
                forward((2, 0), name, "Y-", "Y+")
            for dy in (1, 3):
                landed((1, dy), "A")
                forward((1, dy), "A0", "Z-")
                landed((3, dy), "A")
                forward((3, dy), "A1", "Z+")
            for dz in (1, 3):
                landed((dz, 1), "B")
                forward((dz, 1), "B0", "Y-")
                landed((dz, 3), "B")
                forward((dz, 3), "B1", "Y+")
            cross_first(0)
            cross_first(1)
            group_scores((1, 1), (1, 3))
            group_scores((3, 1), (3, 3))
            landed_all("a")
            group_scores((0, 2), (2, 0))
            landed_all("b")
            forward((1, 2), "A0", "Z-")
            forward((3, 2), "A1", "Z+")
            forward((2, 1), "B0", "Y-")
            forward((2, 3), "B1", "Y+")
            landed_all("c")
            group_scores((1, 2), (3, 2))
            landed_all("d")
            group_scores((2, 1), (2, 3))
            landed_all("e")
            group_scores((2, 2))

        with jax.named_scope("d_colsend"):
            col_rx[d] = col_st[...]
            for p in others(d, n_dp):
                push(col_st, col_rx.at[d], cs_s, cs_r, {"dp": p})

        with jax.named_scope("e_rowstat"):
            for r in range(n_el):
                part = pl.ds(r * chunk, chunk)
                place = far(hops[r // CORES]) * CORES + r % CORES
                peak = jnp.max(row_max[part, :], axis=1, keepdims=True)
                acc = jnp.sum(row_sum[part, :] * jnp.exp2(row_max[part, :] - peak), axis=1,
                              keepdims=True)
                level = peak + jnp.log(acc) * LOG2E
                row_st[pl.ds(place, 1), :] = jnp.broadcast_to(level, (chunk, LANES)).T[0:1, :]
            row_rx[e] = row_st[...]
            for q in others(e, n_el):
                push(row_st, row_rx.at[e], rs_s, rs_r,
                     {"section": q // n_mp, "mp": lax.rem(q, n_mp)})
            both_ways(1)

        def merge(rx, count):
            peak = rx[0]
            for k in range(1, count):
                peak = jnp.maximum(peak, rx[k])
            acc = jnp.zeros(peak.shape, F32)
            for k in range(count):
                acc = acc + jnp.exp2(rx[k] - peak)
            return peak + (jnp.log(acc) * LOG2E + 1.0)

        def slopes(index):
            pre = dot_nn(h_own[index // n_mp], wi_all[index])
            sigm = sigmoid(pre)
            slope_own[index] = sigm + GELU * pre * sigm * (1.0 - sigm)

        with jax.named_scope("f_cross"):
            cross_second(0)
            cross_second(1)
            relay_weight(0, 1)
            relay_weight(0, line - 1)
            arrived(h_own.at[1 - s], h_r)
            for step in (0, 1, line - 1):
                slopes(far(step) * CORES + core)

        with jax.named_scope("f_rows"):
            arrived(row_rx.at[0 : n_el - 1], rs_r)
            row_mix[...] = merge(row_rx, n_el)
            for r in range(n_el):
                part = slice(r * chunk, (r + 1) * chunk)
                place = far(hops[r // CORES]) * CORES + r % CORES
                base = jnp.broadcast_to(row_mix[pl.ds(place, 1), :], (LANES, chunk)).T
                for k in range(n_dp):
                    row_part[k, part, :] = jnp.exp2(scores[k, part, :] - base)

        with jax.named_scope("f_merge"):
            arrived(col_rx.at[0 : n_dp - 1], cs_r)
            col_lse[...] = merge(col_rx, n_dp)

        def score_rows(i):
            part = slice(i * pair, (i + 1) * pair)
            offset = (m - far(hops[i])) * pair + s * half
            for step in steps:
                k = slot(step)
                value = scores[k, part, :]
                low = col_lse[pl.ds(shift(step), 1), :]
                both = row_part[k, part, :] + jnp.exp2(value - low)
                if k == 0:
                    diagonal = lax.broadcasted_iota(jnp.int32, (pair, half), 0) == (
                        lax.broadcasted_iota(jnp.int32, (pair, half), 1) + offset)
                    both = both - jnp.where(diagonal, 1.0, 0.0)
                sgrad[part, k * half : (k + 1) * half] = both.astype(BF16)

        def join(where):
            arrived(t_sr.at[where], ts_r.at[where])
            return t_keep[where] + t_sr[where].astype(F32)


        with jax.named_scope("g_scorerows"):
            score_rows(0)
            for i, hop in enumerate(hops):
                where = far(hop)
                t_full[...] = dot_nn(sgrad[i * pair : (i + 1) * pair, :], cols[...])
                if i + 1 < line:
                    score_rows(i + 1)
                t_sx[where] = t_full[tile(sib, chunk), :].astype(BF16)
                push(t_sx.at[where], t_sr.at[where], ts_s, ts_r.at[where], at(spot, sib))
                t_keep[where] = t_full[tile(core, chunk), :]
                if i > 0:
                    last = far(hops[i - 1])
                    t_tx[last] = join(last).astype(BF16)
                    push(t_tx.at[last], t_rx.at[spot - (spot > last).astype(jnp.int32)], tc_s, tc_r,
                         at(last, core))

        with jax.named_scope("g_relay"):
            cross_third(0)
            cross_third(1)

        fold = half // 2

        with jax.named_scope("h_image"):
            for g in (2, 1, 3, 0):
                part = dot_tn(sgrad[:, g * RING * half : (g + 1) * RING * half], text_low[...])
                for k in range(RING):
                    low = part[k * half : k * half + fold, :]
                    high = part[k * half + fold : (k + 1) * half, :]
                    if g == 0:
                        i_own[0, k] = low
                    else:
                        i_tx[0, g, k] = low.astype(BF16)
                    if k == 0:
                        i_own[1, g] = high
                    else:
                        i_tx[1, k, g] = high.astype(BF16)
                if g > 0:
                    push(i_tx.at[0, g], i_rx.at[0, RING - g], im_s, im_r.at[0, 0], along(1, g))
                if g == 1:
                    relay_weight(1, 1)
                    relay_weight(1, line - 1)
            for k in (2, 1, 3):
                push(i_tx.at[1, k], i_rx.at[1, RING - k], im_s, im_r.at[1, 0], along(0, k))

        def image_second():
            for which in (0, 1):
                arrived(i_rx.at[which, 1:RING], im_r.at[which, 0])
                for g in (2, 1, 3, 0):
                    total = i_own[which, g]
                    for k in range(1, RING):
                        total = total + i_rx[which, k, g].astype(F32)
                    if g == 0:
                        i_own[which, 0] = total
                    else:
                        i_st[which, g] = total.astype(BF16)
                        push(i_st.at[which, g], i_end.at[which, RING - g],
                             im_s, im_r.at[which, 1], along(which, g))

        mine = tile(e, chunk)

        with jax.named_scope("j_weights"):
            arrived(wi_all.at[0:3], ww_r.at[0, 2])
            for step in (0, 1, line - 1):
                slopes(far(step) * CORES + sib)
            slopes(cross)
            arrived(wi_all.at[0], ww_r.at[0, 3])
            slopes(far(2) * CORES + sib)
            arrived(wo_all.at[0:line], ww_r.at[1, 2])

        with jax.named_scope("i_topgrad"):
            total = join(spot)
            arrived(t_rx.at[0 : line - 1], tc_r)
            for k in range(line - 1):
                total = total + t_rx[k].astype(F32)
            unit, length = unit_rows(text[mine, :])
            g_st[n_sec - 1] = unit_backward(unit, length, mult * total).astype(BF16)

        def spread(layer):
            for step in (2, 1, 3) if line == 4 else range(1, line):
                place = far(step)

                @pl.when(place // chips == layer)
                def _():
                    copy(g_st.at[layer], g_all.at[e], gs_s, gs_r.at[e], at(place, core)).start()

            @pl.when(s == layer)
            def _():
                g_all[e] = g_st[layer]
                copy(g_st.at[layer], g_all.at[e], gs_s, gs_r.at[e],
                     at(spot, sib)).start()

        def feed_forward(layer):
            spread(layer)
            first = layer * n_mp
            total = g_st[layer].astype(F32)
            grads = []
            for j in range(n_mp):
                back = dot_nt(g_st[layer], wo_all[first + j])
                grads.append((back * slope_own[first + j]).astype(BF16))
            for j in range(n_mp):
                total = total + dot_nt(grads[j], wi_all[first + j])
            if layer > 0:
                g_st[layer - 1] = total.astype(BF16)
            else:
                for t in range(n_sec):
                    in_st[t] = total[:, t * width : (t + 1) * width].astype(BF16)

        def slab(k):
            return input_out.at[tile(k, chunk), :]

        with jax.named_scope("k_ffn"):
            for layer in range(n_sec - 1, -1, -1):
                feed_forward(layer)

        def weight_rows(k):
            back = dot_nt(g_all[k], w_out[...])
            pre_all[tile(k, chunk), :] = (back * slope_all[tile(k, chunk), :]).astype(BF16)

        with jax.named_scope("m_weightrows"):
            weight_rows(e)
            for hop in (1, 3, 2) if line == 4 else range(1, line):
                index = far(hop) * CORES + core
                arrived(g_all.at[index], gs_r.at[index])
                push(g_all.at[index], g_all.at[index], gs_s, gs_r.at[index],
                     at(spot, sib))
                weight_rows(index)
            input_out[mine, :] = in_st[s]
            push(in_st.at[s], slab(e), in_s, in_r.at[0], at(spot, sib))
            for hop in hops[:-1]:
                where = far(hop)
                push(in_st.at[where // chips], slab(e), in_s, in_r.at[line - hop],
                     at(where, core))
            image_second()
            for hop in (0, 1, 3, 2) if line == 4 else range(line):
                index = far(hop) * CORES + sib
                arrived(g_all.at[index], gs_r.at[index])
                weight_rows(index)

        def send_weights(which):
            for k in (2, 1, 3):
                other = lax.rem(band[which] + k, RING)
                push(w_tx.at[which, tile(other, RING * share), :], w_rx.at[which, RING - k],
                     w_s, w_r.at[which, 0], along(1 - which, k))

        def weight_second(which):
            total = w_full[which, tile(band[which], RING * share), :]
            arrived(w_rx.at[which, 1:RING], w_r.at[which, 0])
            for k in (1, 3, 2):
                total = total + w_rx[which, k].astype(F32)
            w_sum[which] = total
            w_st[which] = total.astype(BF16)
            for k in (2, 1, 3):
                other = lax.rem(band[1 - which] + k, RING)
                push(w_st.at[which, tile(other, share), :], w_end.at[which, RING - k],
                     w_s, w_r.at[which, 1], along(which, k))

        def weight_last(which, out):
            total = w_sum[which, tile(band[1 - which], share), :]
            arrived(w_end.at[which, 1:RING], w_r.at[which, 1])
            for k in (1, 3, 2):
                total = total + w_end[which, k].astype(F32)
            out[...] = total

        with jax.named_scope("n_wgrad"):
            g_rows = g_all[...].reshape(rows, feats)
            grad = dot_tn(g_rows, act_all[...])
            for p in range(n_dp):
                q = (p % RING) * RING + p // RING
                w_full[1, q * share : (q + 1) * share, :] = grad[p * share : (p + 1) * share, :]
                w_tx[1, q * share : (q + 1) * share, :] = grad[
                    p * share : (p + 1) * share, :].astype(BF16)
            send_weights(1)
            grad = dot_tn(hidden[...], pre_all[...])
            w_full[0] = grad
            w_tx[0] = grad.astype(BF16)
            send_weights(0)

        with jax.named_scope("q_image"):
            image_half = tile(s, half)
            unit, length = unit_rows(image[image_half, :])
            for which in (0, 1):
                total = i_own[which, 0]
                arrived(i_end.at[which, 1:RING], im_r.at[which, 1])
                for k in (1, 3, 2):
                    total = total + i_end[which, k].astype(F32)
                part = slice(which * fold, (which + 1) * fold)
                image_out[tile(2 * s + which, fold), :] = unit_backward(
                    unit[part, :], length[part, :], mult * total).astype(BF16)
            push(image_out.at[image_half, :], image_out.at[image_half, :], io_s, io_r,
                 {"section": 1 - s})

        with jax.named_scope("o_inrelay"):
            for hop in hops[:-1]:
                index = far(hop) * CORES + core
                arrived(slab(index), in_r.at[hop])
                push(slab(index), slab(index), in_s, in_r.at[0], at(spot, sib))

        with jax.named_scope("p_wsecond"):
            weight_second(1)
            weight_second(0)

        with jax.named_scope("q_wsum"):
            weight_last(1, second_out)
            weight_last(0, first_out)

        with jax.named_scope("r_drain"):
            arrived(input_out.at[0 : line * chunk, :], in_r.at[0])
            arrived(image_out.at[tile(1 - s, half), :], io_r)
            left(hidden.at[0:chunk, :], h_s)
            left(cols.at[0 : 15 * half, :], gat_s)
            left(col_rx.at[0 : n_dp - 1], cs_s)
            left(row_rx.at[0 : n_el - 1], rs_s)
            for which in (0, 1):
                left(ww[which][1].at[0:6], ww_s.at[which])
                left(ww[which][1].at[0], wc_s.at[which])
            left(t_sx, ts_s)
            left(t_tx.at[0 : line - 1], tc_s)
            left(g_all.at[0 : 2 * n_sec + line - 1], gs_s)
            left(input_out.at[0 : (2 * line - 1) * chunk, :], in_s)
            left(text.at[0 : 2 * (RING - 1) * (RING + 1) * share, :], w_s)
            left(cols.at[0 : 15 * half, :], im_s)
            left(image_out.at[0:half, :], io_s)

    return kernel


def solution(mesh):
    n_sec, n_dp, n_mp = mesh.shape["section"], mesh.shape["dp"], mesh.shape["mp"]

    def body(text, image, scale, hidden, w_in, w_out):
        rows, feats = text.shape
        own = image.shape[0]
        hid = w_in.shape[2]
        half, share = own // n_sec, feats // n_dp
        columns = half * n_dp
        line = n_sec * n_mp // CORES
        n_el = n_sec * n_mp
        chunk = rows // n_el
        dma = pltpu.SemaphoreType.DMA
        vmem = pl.BlockSpec(memory_space=pltpu.VMEM)
        hbm = pl.BlockSpec(memory_space=pltpu.HBM)
        out = pl.pallas_call(
            make_kernel(n_sec, n_dp, n_mp),
            out_shape=(
                pltpu.VMEM((own, feats), BF16),
                pltpu.VMEM((rows, feats // n_sec), BF16),
                pltpu.VMEM((share, hid), F32),
                pltpu.VMEM((share, hid), F32),
            ),
            in_specs=[hbm, hbm, pl.BlockSpec(memory_space=pltpu.SMEM), hbm, hbm, hbm],
            out_specs=(vmem,) * 4,
            scratch_shapes=[
                pltpu.VMEM((rows, feats), BF16),
                pltpu.VMEM((own, feats), BF16),
                pltpu.VMEM((rows, feats), BF16),
                pltpu.VMEM((rows, feats), BF16),
                pltpu.VMEM((columns, feats), BF16),
                pltpu.VMEM((n_dp, rows, half), F32),
                pltpu.VMEM((rows, columns), BF16),
                pltpu.VMEM((rows, LANES), F32),
                pltpu.VMEM((rows, LANES), F32),
                pltpu.VMEM((n_dp, rows, half), F32),
                pltpu.VMEM((n_dp, half), F32),
                pltpu.VMEM((n_el, chunk), F32),
                pltpu.VMEM((n_el, n_el, chunk), F32),
                pltpu.VMEM((n_el, chunk), F32),
                pltpu.VMEM((n_dp, half), F32),
                pltpu.VMEM((n_dp, n_dp, half), F32),
                pltpu.VMEM((n_el, feats, hid), BF16),
                pltpu.VMEM((n_el, hid, feats), BF16),
                pltpu.VMEM((n_sec, chunk, feats), BF16),
                pltpu.VMEM((CORES * chunk, feats), F32),
                pltpu.VMEM((line, chunk, feats), F32),
                pltpu.VMEM((line, chunk, feats), BF16),
                pltpu.VMEM((line, chunk, feats), BF16),
                pltpu.VMEM((line, chunk, feats), BF16),
                pltpu.VMEM((line, chunk, feats), BF16),
                pltpu.VMEM((n_sec, chunk, feats), BF16),
                pltpu.VMEM((n_el, chunk, feats), BF16),
                pltpu.VMEM((n_el, chunk, hid), F32),
                pltpu.VMEM((n_sec, chunk, feats // n_sec), BF16),
                pltpu.VMEM((rows, hid), BF16),
                pltpu.VMEM((rows, hid), F32),
                pltpu.VMEM((rows, hid), BF16),
                pltpu.VMEM((2, feats, hid), F32),
                pltpu.VMEM((2, feats, hid), BF16),
                pltpu.VMEM((2, RING, RING * share, hid), BF16),
                pltpu.VMEM((2, RING * share, hid), F32),
                pltpu.VMEM((2, RING * share, hid), BF16),
                pltpu.VMEM((2, RING, share, hid), BF16),
                pltpu.VMEM((2, RING, RING, half // 2, feats), BF16),
                pltpu.VMEM((2, RING, RING, half // 2, feats), BF16),
                pltpu.VMEM((2, RING, half // 2, feats), F32),
                pltpu.VMEM((2, RING, half // 2, feats), BF16),
                pltpu.VMEM((2, RING, half // 2, feats), BF16),
                dma, dma((25,)), dma, dma, dma, dma, dma((2,)), dma((2, 4)), dma, dma,
                dma, dma((line,)), dma, dma, dma, dma((n_el,)), dma, dma((line,)),
                dma((5,)), dma((2,)), dma((2, 3)), dma, dma((2, 2)), dma, dma((2, 2)), dma, dma,
            ],
            compiler_params=pltpu.CompilerParams(
                collective_id=0, has_side_effects=True, vmem_limit_bytes=62000000
            ),
        )(text, image, scale, hidden[0], w_in[0], w_out[0])
        image_grad, input_grad, first, second = pl.pallas_call(
            leave,
            out_shape=tuple(jax.ShapeDtypeStruct(x.shape, x.dtype) for x in out),
            in_specs=[vmem] * 4,
            out_specs=(hbm,) * 4,
            scratch_shapes=[dma((4,))],
            compiler_params=pltpu.CompilerParams(vmem_limit_bytes=4000000),
        )(*out)
        return (image_grad, input_grad, first[None], second[None])

    return jax.shard_map(
        body,
        mesh=mesh,
        in_specs=(
            P("dp", None),
            P(("dp", "mp"), None),
            P(),
            P("section", "dp", None),
            P("section", None, "mp"),
            P("section", "mp", None),
        ),
        out_specs=(
            P(("dp", "mp"), None),
            P("dp", "section"),
            P("section", "dp", "mp"),
            P("section", "dp", "mp"),
        ),
        check_vma=False,
    )
```

```python
import jax
import jax.numpy as jnp
from jax import lax
from jax.experimental import pallas as pl
from jax.experimental.pallas import tpu as pltpu
from jax.sharding import PartitionSpec as P

MESH = pl.DeviceIdType.MESH
F32 = jnp.float32
BF16 = jnp.bfloat16
GELU = 1.702
LOG2E = 1.4426950408889634
LANES = 128
CORES = 2
RING = 4


def unit_rows(values):
    wide = values.astype(F32)
    length = jnp.sqrt(jnp.sum(wide * wide, axis=1, keepdims=True) + 1.0)
    return (wide / length, length)


def unit_backward(unit, length, grad_unit):
    return (grad_unit - unit * jnp.sum(unit * grad_unit, axis=1, keepdims=True)) / length


def dot_nn(a, b):
    return lax.dot_general(a, b, (((1,), (0,)), ((), ())), preferred_element_type=F32)


def dot_nt(a, b):
    return lax.dot_general(a, b, (((1,), (1,)), ((), ())), preferred_element_type=F32)


def dot_tn(a, b):
    return lax.dot_general(a, b, (((0,), (0,)), ((), ())), preferred_element_type=F32)


def tile(index, size):
    return pl.ds(pl.multiple_of(index * size, size), size)


def leave(*refs):
    copies = [pltpu.make_async_copy(refs[k], refs[4 + k], refs[8].at[k]) for k in range(4)]
    for c in copies:
        c.start()
    for c in copies:
        c.wait()


def make_kernel(n_sec, n_dp, n_mp):
    chips = n_mp // CORES
    line = n_sec * chips
    n_el = n_sec * n_mp

    def kernel(
        text_hbm, image_hbm, scale_ref, hidden_hbm, w_in_hbm, w_out_hbm,
        image_out, input_out, first_out, second_out,
        text, image, hidden, text_low, cols, scores, sgrad, row_max, row_sum, row_part, col_lse, row_st, row_rx, row_mix, col_st, col_rx,
        wi_all, wo_all, h_own, t_full, t_keep, t_sx, t_sr, t_tx, t_rx,
        g_st, g_all, slope_own, in_st, act_all, slope_all, pre_all,
        w_full, w_tx, w_rx, w_sum, w_st, w_end, i_tx, i_rx, i_own, i_st, i_end,
        gat_s, gat_r, cs_s, cs_r, rs_s, rs_r, ww_s, ww_r, h_s, h_r,
        ts_s, ts_r, tc_s, tc_r, gs_s, gs_r, in_s, in_r,
        ld_s, wc_s, wc_r, w_s, w_r, im_s, im_r, io_s, io_r,
    ):
        s = lax.axis_index("section")
        d = lax.axis_index("dp")
        m = lax.axis_index("mp")
        rows, feats = text.shape
        own = image.shape[0]
        half = own // n_sec
        chunk = rows // n_el
        pair = rows // line
        share = feats // n_dp
        width = feats // n_sec
        mult = scale_ref[0]
        mult2 = mult * LOG2E
        core = lax.rem(m, CORES)
        sib = 1 - core
        spot = s * chips + m // CORES
        e = s * n_mp + m

        def at(place, who):
            return {"section": place // chips, "mp": lax.rem(place, chips) * CORES + who}

        def far(step):
            return lax.rem(spot + step, line)

        def copy(src, dst, send, recv, where):
            return pltpu.make_async_remote_copy(
                src_ref=src, dst_ref=dst, send_sem=send, recv_sem=recv,
                device_id=where, device_id_type=MESH,
            )

        def arrived(ref, recv):
            copy(ref, ref, h_s, recv, at(spot, sib)).wait_recv()

        def shift(step):
            dz, dy = step[0] % RING, step[1] % RING
            z = lax.rem(d // RING + dz, RING)
            return z * RING + lax.rem(lax.rem(d, RING) + dy, RING)

        def slot(step):
            return (step[0] % RING) * RING + step[1] % RING

        steps = [(a, b) for a in range(RING) for b in range(RING)]

        def away(step):
            return (-step[0] % RING, -step[1] % RING)

        hops = (2, 3, 1, 0) if line == 4 else tuple(range(line - 1, -1, -1))

        def others(mine, count):
            return [lax.rem(mine + k, count) for k in range(1, count)]

        def sources(mine, count):
            return [lax.rem(mine + count - k, count) for k in range(1, count)]

        def push(*args):
            copy(*args).start()

        def left(ref, send):
            copy(ref, ref, send, h_r, at(spot, sib)).wait_send()

        with jax.named_scope("a_barrier"):
            loads = [
                pltpu.make_async_copy(src, dst, ld_s.at[k])
                for k, (src, dst) in enumerate((
                    (image_hbm, image), (text_hbm, text), (hidden_hbm, hidden),
                    (w_in_hbm, wi_all.at[e]), (w_out_hbm, wo_all.at[e]),
                ))
            ]
            for load in loads:
                load.start()
            barrier = pltpu.get_barrier_semaphore()
            for near in ((0, 1), (0, -1), (1, 0), (-1, 0)):
                pl.semaphore_signal(
                    barrier, inc=1, device_id={"dp": shift(near)}, device_id_type=MESH)
            for q in others(e, n_el):
                pl.semaphore_signal(
                    barrier, inc=1, device_id={"section": q // n_mp, "mp": lax.rem(q, n_mp)},
                    device_id_type=MESH,
                )
            loads[0].wait()
            own_unit, _ = unit_rows(image[tile(s, half), :])
            cols[0:half, :] = own_unit.astype(BF16)
            pl.semaphore_wait(barrier, n_el + 3)

        quarter = half // 4
        spans = {"A": (0, 2), "B": (2, 2), "A0": (0, 1), "A1": (1, 1), "B0": (2, 1), "B1": (3, 1)}
        ahead = {"Y-": (0, -1), "Y+": (0, 1), "Z-": (-1, 0), "Z+": (1, 0)}
        quads = {
            "a": [((0, 2), "B0"), ((0, 2), "B1"), ((2, 0), "A0"), ((2, 0), "A1")],
            "b": [(k, name) for k in ((1, 2), (3, 2)) for name in ("A0", "A1")]
            + [(k, name) for k in ((2, 1), (2, 3)) for name in ("B0", "B1")],
            "c": [(k, name) for k in ((1, 2), (3, 2)) for name in ("B0", "B1")],
            "d": [(k, name) for k in ((2, 1), (2, 3)) for name in ("A0", "A1")],
            "e": [((2, 2), name) for name in ("A0", "A1", "B0", "B1")],
        }
        ports = {}

        def port(step, name):
            key = (slot(step), name)
            for group, members in quads.items():
                if any(key == (slot(k), other) for k, other in members):
                    key = group
            return ports.setdefault(key, len(ports))

        def landed_all(group):
            count = len(quads[group])
            k, name = quads[group][0]
            arrived(cols.at[0 : count * quarter, :], gat_r.at[port(k, name)])

        def piece_of(step, name):
            first, count = spans[name]
            base = slot(step) * half + first * quarter
            return cols.at[base : base + count * quarter, :]

        def forward(step, name, *directions):
            for way in directions:
                move = ahead[way]
                lands = (step[0] - move[0], step[1] - move[1])
                push(piece_of(step, name), piece_of(lands, name), gat_s,
                     gat_r.at[port(lands, name)], {"dp": shift(move)})

        def landed(step, name):
            arrived(piece_of(step, name), gat_r.at[port(step, name)])

        for way in ("Y-", "Y+"):
            forward((0, 0), "A", way)
        for way in ("Z-", "Z+"):
            forward((0, 0), "B", way)
        for way in ("Y-", "Y+"):
            forward((0, 0), "B", way)
        for way in ("Z-", "Z+"):
            forward((0, 0), "A", way)

        for load in loads[2:]:
            load.wait()
        h_own[s] = hidden[tile(e, chunk), :]
        mate = (1 - s) * n_mp + m
        push(hidden.at[tile(mate, chunk), :], h_own.at[s], h_s, h_r, {"section": 1 - s})
        w_in, w_out = wi_all.at[e], wo_all.at[e]
        ww = ((w_in, wi_all), (w_out, wo_all))
        z_at, y_at = d // RING, lax.rem(d, RING)
        cell = (z_at * RING + y_at, y_at * RING + z_at)
        band = (z_at, y_at)
        cross = far(2) * CORES + core
        bit = w_in.shape[0] // n_dp

        def along(which, step):
            return {"dp": shift((0, step) if which == 0 else (step, 0))}

        for which in (0, 1):
            part = tile(cell[which], bit)
            push(ww[which][0].at[part, :], ww[which][1].at[e, part, :], wc_s.at[which],
                 wc_r.at[which, 0], at(far(2), core))
        depth = w_in.shape[0]
        whole = (pl.ds(0, depth // 2), pl.ds(depth // 2, depth // 2))
        early = (pl.ds(0, depth // 4),)
        later = (pl.ds(depth // 4, depth // 4), pl.ds(depth // 2, depth // 2))

        def neighbour(which, toward, part):
            push(ww[which][0].at[part, :], ww[which][1].at[e, part, :], ww_s.at[which],
                 ww_r.at[which, 1 if toward == 1 else 0], at(far(toward), core))

        def both_ways(which, parts):
            for part in parts:
                neighbour(which, line - 1, part)
                neighbour(which, 1, part)

        both_ways(0, whole)
        both_ways(1, early)

        for which in (0, 1):
            push(ww[which][0], ww[which][1].at[e], ww_s.at[which], ww_r.at[which, 2],
                 at(spot, sib))

        def cross_first(which):
            mine_bit = ww[which][1].at[cross, tile(cell[which], bit), :]
            arrived(mine_bit, wc_r.at[which, 0])
            for k in range(1, RING):
                push(mine_bit, mine_bit, wc_s.at[which], wc_r.at[which, 1],
                     along(which, k))

        def cross_second(which):
            arrived(ww[which][1].at[cross, 0 : (RING - 1) * bit, :], wc_r.at[which, 1])
            group = ww[which][1].at[cross, tile(band[which], RING * bit), :]
            for k in range(1, RING):
                push(group, group, wc_s.at[which], wc_r.at[which, 2],
                     along(1 - which, k))

        def cross_third(which):
            arrived(ww[which][1].at[cross, 0 : (RING - 1) * RING * bit, :], wc_r.at[which, 2])
            push(ww[which][1].at[cross], ww[which][1].at[cross], ww_s.at[which],
                 ww_r.at[which, 2 if which else 3], at(spot, sib))

        def relay_weight(which, step):
            index = far(step) * CORES + core
            buf = ww[which][1].at[index]
            arrived(buf, ww_r.at[which, 0 if step == 1 else 1])
            push(buf, buf, ww_s.at[which], ww_r.at[which, 2], at(spot, sib))

        def sigmoid(pre):
            return 1.0 / (1.0 + jnp.exp(-GELU * pre))

        with jax.named_scope("b_pre"):
            loads[1].wait()
            for i, hop in enumerate(hops):
                unit, _ = unit_rows(text[tile(far(hop), pair), :])
                text_low[i * pair : (i + 1) * pair, :] = unit.astype(BF16)

            @pl.loop(0, line)
            def _(r):
                pre = dot_nn(hidden[tile(r, pair), :], w_in[...])
                sigm = sigmoid(pre)
                act_all[tile(r, pair), :] = (pre * sigm).astype(BF16)
                slope_all[tile(r, pair), :] = sigm + GELU * pre * sigm * (1.0 - sigm)

        def group_scores(*group, fresh=False):
            piece = [cols[slot(k) * half : (slot(k) + 1) * half, :] for k in group]
            piece = piece[0] if len(piece) == 1 else jnp.concatenate(piece, axis=0)
            peak = total = None
            for r in range(line):
                part = pl.ds(r * pair, pair)
                value = mult2 * dot_nt(text_low[part, :], piece)
                blocks = [value[:, k * half : (k + 1) * half] for k in range(len(group))]
                for k, block in zip(group, blocks):
                    scores[slot(k), part, :] = block
                best = blocks[0]
                for block in blocks[1:]:
                    best = jnp.maximum(best, block)
                if not fresh:
                    best = jnp.maximum(best, row_max[part, :])
                    mass = row_sum[part, :] * jnp.exp2(row_max[part, :] - best)
                    for block in blocks:
                        mass = mass + jnp.exp2(block - best)
                    row_sum[part, :] = mass
                else:
                    row_sum[part, :] = jnp.ones(best.shape, F32)
                row_max[part, :] = best
                high = jnp.max(value, axis=0, keepdims=True)
                if peak is None:
                    peak = high
                    total = jnp.sum(jnp.exp2(value - peak), axis=0, keepdims=True)
                else:
                    high = jnp.maximum(peak, high)
                    total = total * jnp.exp2(peak - high) + jnp.sum(
                        jnp.exp2(value - high), axis=0, keepdims=True)
                    peak = high
            level = peak + jnp.log(total) * LOG2E
            for k, step in enumerate(group):
                p = shift(step)
                col_st[pl.ds(p, 1), :] = level[:, k * half : (k + 1) * half]

        with jax.named_scope("c_own"):
            group_scores((0, 0), fresh=True)

        with jax.named_scope("c_blocks"):
            landed((0, 1), "A")
            forward((0, 1), "A0", "Y-")
            landed((1, 0), "B")
            forward((1, 0), "B0", "Z-")
            landed((0, 3), "A")
            forward((0, 3), "A1", "Y+")
            landed((3, 0), "B")
            forward((3, 0), "B1", "Z+")
            for dy in (1, 3):
                forward((0, dy), "A", "Z-", "Z+")
            for dz in (1, 3):
                forward((dz, 0), "B", "Y-", "Y+")
            landed((0, 1), "B")
            forward((0, 1), "B0", "Y-")
            landed((1, 0), "A")
            forward((1, 0), "A0", "Z-")
            landed((0, 3), "B")
            forward((0, 3), "B1", "Y+")
            landed((3, 0), "A")
            forward((3, 0), "A1", "Z+")
            group_scores((0, 1), (0, 3))
            group_scores((1, 0), (3, 0))
            for name in ("A0", "A1"):
                landed((0, 2), name)
                forward((0, 2), name, "Z-", "Z+")
            for name in ("B0", "B1"):
                landed((2, 0), name)
                forward((2, 0), name, "Y-", "Y+")
            for dy in (1, 3):
                landed((1, dy), "A")
                forward((1, dy), "A0", "Z-")
                landed((3, dy), "A")
                forward((3, dy), "A1", "Z+")
            for dz in (1, 3):
                landed((dz, 1), "B")
                forward((dz, 1), "B0", "Y-")
                landed((dz, 3), "B")
                forward((dz, 3), "B1", "Y+")
            cross_first(0)
            cross_first(1)
            group_scores((1, 1), (1, 3))
            group_scores((3, 1), (3, 3))
            landed_all("a")
            group_scores((0, 2), (2, 0))
            landed_all("b")
            forward((1, 2), "A0", "Z-")
            forward((3, 2), "A1", "Z+")
            forward((2, 1), "B0", "Y-")
            forward((2, 3), "B1", "Y+")
            landed_all("c")
            group_scores((1, 2), (3, 2))
            landed_all("d")
            group_scores((2, 1), (2, 3))
            landed_all("e")
            group_scores((2, 2))

        with jax.named_scope("d_colsend"):
            col_rx[d] = col_st[...]
            for p in others(d, n_dp):
                push(col_st, col_rx.at[d], cs_s, cs_r, {"dp": p})

        with jax.named_scope("e_rowstat"):
            for r in range(n_el):
                part = pl.ds(r * chunk, chunk)
                place = far(hops[r // CORES]) * CORES + r % CORES
                peak = jnp.max(row_max[part, :], axis=1, keepdims=True)
                acc = jnp.sum(row_sum[part, :] * jnp.exp2(row_max[part, :] - peak), axis=1,
                              keepdims=True)
                level = peak + jnp.log(acc) * LOG2E
                row_st[pl.ds(place, 1), :] = jnp.broadcast_to(level, (chunk, LANES)).T[0:1, :]
            row_rx[e] = row_st[...]
            for q in others(e, n_el):
                push(row_st, row_rx.at[e], rs_s, rs_r,
                     {"section": q // n_mp, "mp": lax.rem(q, n_mp)})
            both_ways(1, later)

        def merge(rx, count):
            peak = rx[0]
            for k in range(1, count):
                peak = jnp.maximum(peak, rx[k])
            acc = jnp.zeros(peak.shape, F32)
            for k in range(count):
                acc = acc + jnp.exp2(rx[k] - peak)
            return peak + (jnp.log(acc) * LOG2E + 1.0)

        def slopes(index):
            pre = dot_nn(h_own[index // n_mp], wi_all[index])
            sigm = sigmoid(pre)
            slope_own[index] = sigm + GELU * pre * sigm * (1.0 - sigm)

        with jax.named_scope("f_cross"):
            cross_second(0)
            cross_second(1)
            relay_weight(0, 1)
            relay_weight(0, line - 1)
            arrived(h_own.at[1 - s], h_r)
            for step in (0, 1, line - 1):
                slopes(far(step) * CORES + core)

        with jax.named_scope("f_rows"):
            arrived(row_rx.at[0 : n_el - 1], rs_r)
            row_mix[...] = merge(row_rx, n_el)
            for r in range(n_el):
                part = slice(r * chunk, (r + 1) * chunk)
                place = far(hops[r // CORES]) * CORES + r % CORES
                base = jnp.broadcast_to(row_mix[pl.ds(place, 1), :], (LANES, chunk)).T
                for k in range(n_dp):
                    row_part[k, part, :] = jnp.exp2(scores[k, part, :] - base)

        with jax.named_scope("f_merge"):
            arrived(col_rx.at[0 : n_dp - 1], cs_r)
            col_lse[...] = merge(col_rx, n_dp)

        def score_rows(i):
            part = slice(i * pair, (i + 1) * pair)
            offset = (m - far(hops[i])) * pair + s * half
            for step in steps:
                k = slot(step)
                value = scores[k, part, :]
                low = col_lse[pl.ds(shift(step), 1), :]
                both = row_part[k, part, :] + jnp.exp2(value - low)
                if k == 0:
                    diagonal = lax.broadcasted_iota(jnp.int32, (pair, half), 0) == (
                        lax.broadcasted_iota(jnp.int32, (pair, half), 1) + offset)
                    both = both - jnp.where(diagonal, 1.0, 0.0)
                sgrad[part, k * half : (k + 1) * half] = both.astype(BF16)

        def join(where):
            arrived(t_sr.at[where], ts_r.at[where])
            return t_keep[where] + t_sr[where].astype(F32)


        with jax.named_scope("g_scorerows"):
            score_rows(0)
            for i, hop in enumerate(hops):
                where = far(hop)
                t_full[...] = dot_nn(sgrad[i * pair : (i + 1) * pair, :], cols[...])
                if i + 1 < line:
                    score_rows(i + 1)
                t_sx[where] = t_full[tile(sib, chunk), :].astype(BF16)
                push(t_sx.at[where], t_sr.at[where], ts_s, ts_r.at[where], at(spot, sib))
                t_keep[where] = t_full[tile(core, chunk), :]
                if i > 0:
                    last = far(hops[i - 1])
                    t_tx[last] = join(last).astype(BF16)
                    push(t_tx.at[last], t_rx.at[spot - (spot > last).astype(jnp.int32)], tc_s, tc_r,
                         at(last, core))

        with jax.named_scope("g_relay"):
            cross_third(0)
            cross_third(1)

        fold = half // 2

        with jax.named_scope("h_image"):
            for g in (2, 1, 3, 0):
                part = dot_tn(sgrad[:, g * RING * half : (g + 1) * RING * half], text_low[...])
                for k in range(RING):
                    low = part[k * half : k * half + fold, :]
                    high = part[k * half + fold : (k + 1) * half, :]
                    if g == 0:
                        i_own[0, k] = low
                    else:
                        i_tx[0, g, k] = low.astype(BF16)
                    if k == 0:
                        i_own[1, g] = high
                    else:
                        i_tx[1, k, g] = high.astype(BF16)
                if g > 0:
                    push(i_tx.at[0, g], i_rx.at[0, RING - g], im_s, im_r.at[0, 0], along(1, g))
                for k in (2, 1, 3):
                    push(i_tx.at[1, k, g], i_rx.at[1, RING - k, g], im_s, im_r.at[1, 0],
                         along(0, k))
                if g == 1:
                    relay_weight(1, 1)
                    relay_weight(1, line - 1)

        def image_second():
            for which in (0, 1):
                arrived(i_rx.at[which, 1:RING], im_r.at[which, 0])
                for g in (2, 1, 3, 0):
                    total = i_own[which, g]
                    for k in range(1, RING):
                        total = total + i_rx[which, k, g].astype(F32)
                    if g == 0:
                        i_own[which, 0] = total
                    else:
                        i_st[which, g] = total.astype(BF16)
                        push(i_st.at[which, g], i_end.at[which, RING - g],
                             im_s, im_r.at[which, 1], along(which, g))

        mine = tile(e, chunk)

        with jax.named_scope("j_weights"):
            arrived(wi_all.at[0:3], ww_r.at[0, 2])
            for step in (0, 1, line - 1):
                slopes(far(step) * CORES + sib)
            slopes(cross)
            arrived(wi_all.at[0], ww_r.at[0, 3])
            slopes(far(2) * CORES + sib)
            arrived(wo_all.at[0:line], ww_r.at[1, 2])

        with jax.named_scope("i_topgrad"):
            total = join(spot)
            arrived(t_rx.at[0 : line - 1], tc_r)
            for k in range(line - 1):
                total = total + t_rx[k].astype(F32)
            unit, length = unit_rows(text[mine, :])
            g_st[n_sec - 1] = unit_backward(unit, length, mult * total).astype(BF16)

        def spread(layer):
            for step in (2, 1, 3) if line == 4 else range(1, line):
                place = far(step)

                @pl.when(place // chips == layer)
                def _():
                    copy(g_st.at[layer], g_all.at[e], gs_s, gs_r.at[e], at(place, core)).start()

            @pl.when(s == layer)
            def _():
                g_all[e] = g_st[layer]
                copy(g_st.at[layer], g_all.at[e], gs_s, gs_r.at[e],
                     at(spot, sib)).start()

        def feed_forward(layer):
            spread(layer)
            first = layer * n_mp
            total = g_st[layer].astype(F32)
            grads = []
            for j in range(n_mp):
                back = dot_nt(g_st[layer], wo_all[first + j])
                grads.append((back * slope_own[first + j]).astype(BF16))
            for j in range(n_mp):
                total = total + dot_nt(grads[j], wi_all[first + j])
            if layer > 0:
                g_st[layer - 1] = total.astype(BF16)
            else:
                for t in range(n_sec):
                    in_st[t] = total[:, t * width : (t + 1) * width].astype(BF16)

        def slab(k):
            return input_out.at[tile(k, chunk), :]

        with jax.named_scope("k_ffn"):
            for layer in range(n_sec - 1, -1, -1):
                feed_forward(layer)

        def weight_rows(k):
            back = dot_nt(g_all[k], w_out[...])
            pre_all[tile(k, chunk), :] = (back * slope_all[tile(k, chunk), :]).astype(BF16)

        with jax.named_scope("m_weightrows"):
            weight_rows(e)
            for hop in (1, 3, 2) if line == 4 else range(1, line):
                index = far(hop) * CORES + core
                arrived(g_all.at[index], gs_r.at[index])
                push(g_all.at[index], g_all.at[index], gs_s, gs_r.at[index],
                     at(spot, sib))
                weight_rows(index)
            input_out[mine, :] = in_st[s]
            push(in_st.at[s], slab(e), in_s, in_r.at[0], at(spot, sib))
            for hop in hops[:-1]:
                where = far(hop)
                push(in_st.at[where // chips], slab(e), in_s, in_r.at[line - hop],
                     at(where, core))
            image_second()
            for hop in (0, 1, 3, 2) if line == 4 else range(line):
                index = far(hop) * CORES + sib
                arrived(g_all.at[index], gs_r.at[index])
                weight_rows(index)

        def send_weights(which):
            for k in (2, 1, 3):
                other = lax.rem(band[which] + k, RING)
                push(w_tx.at[which, tile(other, RING * share), :], w_rx.at[which, RING - k],
                     w_s, w_r.at[which, 0], along(1 - which, k))

        def weight_second(which):
            total = w_full[which, tile(band[which], RING * share), :]
            arrived(w_rx.at[which, 1:RING], w_r.at[which, 0])
            for k in (1, 3, 2):
                total = total + w_rx[which, k].astype(F32)
            w_sum[which] = total
            w_st[which] = total.astype(BF16)
            for k in (2, 1, 3):
                other = lax.rem(band[1 - which] + k, RING)
                push(w_st.at[which, tile(other, share), :], w_end.at[which, RING - k],
                     w_s, w_r.at[which, 1], along(which, k))

        def weight_last(which, out):
            total = w_sum[which, tile(band[1 - which], share), :]
            arrived(w_end.at[which, 1:RING], w_r.at[which, 1])
            for k in (1, 3, 2):
                total = total + w_end[which, k].astype(F32)
            out[...] = total

        with jax.named_scope("n_wgrad"):
            g_rows = g_all[...].reshape(rows, feats)
            grad = dot_tn(g_rows, act_all[...])
            for p in range(n_dp):
                q = (p % RING) * RING + p // RING
                w_full[1, q * share : (q + 1) * share, :] = grad[p * share : (p + 1) * share, :]
                w_tx[1, q * share : (q + 1) * share, :] = grad[
                    p * share : (p + 1) * share, :].astype(BF16)
            send_weights(1)
            grad = dot_tn(hidden[...], pre_all[...])
            w_full[0] = grad
            w_tx[0] = grad.astype(BF16)
            send_weights(0)

        with jax.named_scope("q_image"):
            image_half = tile(s, half)
            unit, length = unit_rows(image[image_half, :])
            for which in (0, 1):
                total = i_own[which, 0]
                arrived(i_end.at[which, 1:RING], im_r.at[which, 1])
                for k in (1, 3, 2):
                    total = total + i_end[which, k].astype(F32)
                part = slice(which * fold, (which + 1) * fold)
                image_out[tile(2 * s + which, fold), :] = unit_backward(
                    unit[part, :], length[part, :], mult * total).astype(BF16)
            push(image_out.at[image_half, :], image_out.at[image_half, :], io_s, io_r,
                 {"section": 1 - s})

        with jax.named_scope("o_inrelay"):
            for hop in hops[:-1]:
                index = far(hop) * CORES + core
                arrived(slab(index), in_r.at[hop])
                push(slab(index), slab(index), in_s, in_r.at[0], at(spot, sib))

        with jax.named_scope("p_wsecond"):
            weight_second(1)
            weight_second(0)

        with jax.named_scope("q_wsum"):
            weight_last(1, second_out)
            weight_last(0, first_out)

        with jax.named_scope("r_drain"):
            arrived(input_out.at[0 : line * chunk, :], in_r.at[0])
            arrived(image_out.at[tile(1 - s, half), :], io_r)
            left(hidden.at[0:chunk, :], h_s)
            left(cols.at[0 : 15 * half, :], gat_s)
            left(col_rx.at[0 : n_dp - 1], cs_s)
            left(row_rx.at[0 : n_el - 1], rs_s)
            for which in (0, 1):
                left(ww[which][1].at[0:6], ww_s.at[which])
                left(ww[which][1].at[0], wc_s.at[which])
            left(t_sx, ts_s)
            left(t_tx.at[0 : line - 1], tc_s)
            left(g_all.at[0 : 2 * n_sec + line - 1], gs_s)
            left(input_out.at[0 : (2 * line - 1) * chunk, :], in_s)
            left(text.at[0 : 2 * (RING - 1) * (RING + 1) * share, :], w_s)
            left(cols.at[0 : 15 * half, :], im_s)
            left(image_out.at[0:half, :], io_s)

    return kernel


def solution(mesh):
    n_sec, n_dp, n_mp = mesh.shape["section"], mesh.shape["dp"], mesh.shape["mp"]

    def body(text, image, scale, hidden, w_in, w_out):
        rows, feats = text.shape
        own = image.shape[0]
        hid = w_in.shape[2]
        half, share = own // n_sec, feats // n_dp
        columns = half * n_dp
        line = n_sec * n_mp // CORES
        n_el = n_sec * n_mp
        chunk = rows // n_el
        dma = pltpu.SemaphoreType.DMA
        vmem = pl.BlockSpec(memory_space=pltpu.VMEM)
        hbm = pl.BlockSpec(memory_space=pltpu.HBM)
        out = pl.pallas_call(
            make_kernel(n_sec, n_dp, n_mp),
            out_shape=(
                pltpu.VMEM((own, feats), BF16),
                pltpu.VMEM((rows, feats // n_sec), BF16),
                pltpu.VMEM((share, hid), F32),
                pltpu.VMEM((share, hid), F32),
            ),
            in_specs=[hbm, hbm, pl.BlockSpec(memory_space=pltpu.SMEM), hbm, hbm, hbm],
            out_specs=(vmem,) * 4,
            scratch_shapes=[
                pltpu.VMEM((rows, feats), BF16),
                pltpu.VMEM((own, feats), BF16),
                pltpu.VMEM((rows, feats), BF16),
                pltpu.VMEM((rows, feats), BF16),
                pltpu.VMEM((columns, feats), BF16),
                pltpu.VMEM((n_dp, rows, half), F32),
                pltpu.VMEM((rows, columns), BF16),
                pltpu.VMEM((rows, LANES), F32),
                pltpu.VMEM((rows, LANES), F32),
                pltpu.VMEM((n_dp, rows, half), F32),
                pltpu.VMEM((n_dp, half), F32),
                pltpu.VMEM((n_el, chunk), F32),
                pltpu.VMEM((n_el, n_el, chunk), F32),
                pltpu.VMEM((n_el, chunk), F32),
                pltpu.VMEM((n_dp, half), F32),
                pltpu.VMEM((n_dp, n_dp, half), F32),
                pltpu.VMEM((n_el, feats, hid), BF16),
                pltpu.VMEM((n_el, hid, feats), BF16),
                pltpu.VMEM((n_sec, chunk, feats), BF16),
                pltpu.VMEM((CORES * chunk, feats), F32),
                pltpu.VMEM((line, chunk, feats), F32),
                pltpu.VMEM((line, chunk, feats), BF16),
                pltpu.VMEM((line, chunk, feats), BF16),
                pltpu.VMEM((line, chunk, feats), BF16),
                pltpu.VMEM((line, chunk, feats), BF16),
                pltpu.VMEM((n_sec, chunk, feats), BF16),
                pltpu.VMEM((n_el, chunk, feats), BF16),
                pltpu.VMEM((n_el, chunk, hid), F32),
                pltpu.VMEM((n_sec, chunk, feats // n_sec), BF16),
                pltpu.VMEM((rows, hid), BF16),
                pltpu.VMEM((rows, hid), F32),
                pltpu.VMEM((rows, hid), BF16),
                pltpu.VMEM((2, feats, hid), F32),
                pltpu.VMEM((2, feats, hid), BF16),
                pltpu.VMEM((2, RING, RING * share, hid), BF16),
                pltpu.VMEM((2, RING * share, hid), F32),
                pltpu.VMEM((2, RING * share, hid), BF16),
                pltpu.VMEM((2, RING, share, hid), BF16),
                pltpu.VMEM((2, RING, RING, half // 2, feats), BF16),
                pltpu.VMEM((2, RING, RING, half // 2, feats), BF16),
                pltpu.VMEM((2, RING, half // 2, feats), F32),
                pltpu.VMEM((2, RING, half // 2, feats), BF16),
                pltpu.VMEM((2, RING, half // 2, feats), BF16),
                dma, dma((25,)), dma, dma, dma, dma, dma((2,)), dma((2, 4)), dma, dma,
                dma, dma((line,)), dma, dma, dma, dma((n_el,)), dma, dma((line,)),
                dma((5,)), dma((2,)), dma((2, 3)), dma, dma((2, 2)), dma, dma((2, 2)), dma, dma,
            ],
            compiler_params=pltpu.CompilerParams(
                collective_id=0, has_side_effects=True, vmem_limit_bytes=62000000
            ),
        )(text, image, scale, hidden[0], w_in[0], w_out[0])
        image_grad, input_grad, first, second = pl.pallas_call(
            leave,
            out_shape=tuple(jax.ShapeDtypeStruct(x.shape, x.dtype) for x in out),
            in_specs=[vmem] * 4,
            out_specs=(hbm,) * 4,
            scratch_shapes=[dma((4,))],
            compiler_params=pltpu.CompilerParams(vmem_limit_bytes=4000000),
        )(*out)
        return (image_grad, input_grad, first[None], second[None])

    return jax.shard_map(
        body,
        mesh=mesh,
        in_specs=(
            P("dp", None),
            P(("dp", "mp"), None),
            P(),
            P("section", "dp", None),
            P("section", None, "mp"),
            P("section", "mp", None),
        ),
        out_specs=(
            P(("dp", "mp"), None),
            P("dp", "section"),
            P("section", "dp", "mp"),
            P("section", "dp", "mp"),
        ),
        check_vma=False,
    )
```

```python
import jax
import jax.numpy as jnp
from jax import lax
from jax.experimental import pallas as pl
from jax.experimental.pallas import tpu as pltpu
from jax.sharding import PartitionSpec as P

MESH = pl.DeviceIdType.MESH
F32 = jnp.float32
BF16 = jnp.bfloat16
GELU = 1.702
LOG2E = 1.4426950408889634
LANES = 128
CORES = 2
RING = 4


def unit_rows(values):
    wide = values.astype(F32)
    length = jnp.sqrt(jnp.sum(wide * wide, axis=1, keepdims=True) + 1.0)
    return (wide / length, length)


def unit_backward(unit, length, grad_unit):
    return (grad_unit - unit * jnp.sum(unit * grad_unit, axis=1, keepdims=True)) / length


def dot_nn(a, b):
    return lax.dot_general(a, b, (((1,), (0,)), ((), ())), preferred_element_type=F32)


def dot_nt(a, b):
    return lax.dot_general(a, b, (((1,), (1,)), ((), ())), preferred_element_type=F32)


def dot_tn(a, b):
    return lax.dot_general(a, b, (((0,), (0,)), ((), ())), preferred_element_type=F32)


def tile(index, size):
    return pl.ds(pl.multiple_of(index * size, size), size)


def leave(*refs):
    copies = [pltpu.make_async_copy(refs[k], refs[4 + k], refs[8].at[k]) for k in range(4)]
    for c in copies:
        c.start()
    for c in copies:
        c.wait()


def make_kernel(n_sec, n_dp, n_mp):
    chips = n_mp // CORES
    line = n_sec * chips
    n_el = n_sec * n_mp

    def kernel(
        text_hbm, image_hbm, scale_hbm, hidden_hbm, w_in_hbm, w_out_hbm,
        image_out, input_out, first_out, second_out,
        scale_ref, text, image, hidden, text_low, cols, scores, sgrad, row_max, row_sum, row_part, col_lse, row_st, row_rx, row_mix, col_st, col_rx,
        wi_all, wo_all, h_own, t_full, t_keep, t_sx, t_sr, t_tx, t_rx,
        g_st, g_all, slope_own, in_st, act_all, slope_all, pre_all,
        w_full, w_tx, w_rx, w_sum, w_st, w_end, i_tx, i_rx, i_own, i_st, i_end,
        gat_s, gat_r, cs_s, cs_r, rs_s, rs_r, ww_s, ww_r, h_s, h_r,
        ts_s, ts_r, tc_s, tc_r, gs_s, gs_r, in_s, in_r,
        ld_s, wc_s, wc_r, w_s, w_r, im_s, im_r, io_s, io_r,
    ):
        s = lax.axis_index("section")
        d = lax.axis_index("dp")
        m = lax.axis_index("mp")
        rows, feats = text.shape
        own = image_hbm.shape[0]
        half = own // n_sec
        chunk = rows // n_el
        pair = rows // line
        share = feats // n_dp
        width = feats // n_sec
        core = lax.rem(m, CORES)
        sib = 1 - core
        spot = s * chips + m // CORES
        e = s * n_mp + m

        def at(place, who):
            return {"section": place // chips, "mp": lax.rem(place, chips) * CORES + who}

        def far(step):
            return lax.rem(spot + step, line)

        def copy(src, dst, send, recv, where):
            return pltpu.make_async_remote_copy(
                src_ref=src, dst_ref=dst, send_sem=send, recv_sem=recv,
                device_id=where, device_id_type=MESH,
            )

        def arrived(ref, recv):
            copy(ref, ref, h_s, recv, at(spot, sib)).wait_recv()

        def shift(step):
            dz, dy = step[0] % RING, step[1] % RING
            z = lax.rem(d // RING + dz, RING)
            return z * RING + lax.rem(lax.rem(d, RING) + dy, RING)

        def slot(step):
            return (step[0] % RING) * RING + step[1] % RING

        steps = [(a, b) for a in range(RING) for b in range(RING)]

        def away(step):
            return (-step[0] % RING, -step[1] % RING)

        hops = (2, 3, 1, 0) if line == 4 else tuple(range(line - 1, -1, -1))

        def others(mine, count):
            return [lax.rem(mine + k, count) for k in range(1, count)]

        def sources(mine, count):
            return [lax.rem(mine + count - k, count) for k in range(1, count)]

        def push(*args):
            copy(*args).start()

        def left(ref, send):
            copy(ref, ref, send, h_r, at(spot, sib)).wait_send()

        with jax.named_scope("a_barrier"):
            loads = [
                pltpu.make_async_copy(src, dst, ld_s.at[k])
                for k, (src, dst) in enumerate((
                    (image_hbm.at[tile(s, half), :], image), (text_hbm, text), (hidden_hbm, hidden),
                    (w_in_hbm, wi_all.at[e]), (w_out_hbm, wo_all.at[e]), (scale_hbm, scale_ref),
                ))
            ]
            for load in loads:
                load.start()
            barrier = pltpu.get_barrier_semaphore()
            for near in ((0, 1), (0, -1), (1, 0), (-1, 0)):
                pl.semaphore_signal(
                    barrier, inc=1, device_id={"dp": shift(near)}, device_id_type=MESH)
            for q in others(e, n_el):
                pl.semaphore_signal(
                    barrier, inc=1, device_id={"section": q // n_mp, "mp": lax.rem(q, n_mp)},
                    device_id_type=MESH,
                )
            loads[0].wait()
            own_unit, _ = unit_rows(image[...])
            cols[0:half, :] = own_unit.astype(BF16)
            pl.semaphore_wait(barrier, n_el + 3)

        quarter = half // 4
        spans = {"A": (0, 2), "B": (2, 2), "A0": (0, 1), "A1": (1, 1), "B0": (2, 1), "B1": (3, 1)}
        ahead = {"Y-": (0, -1), "Y+": (0, 1), "Z-": (-1, 0), "Z+": (1, 0)}
        quads = {
            "a": [((0, 2), "B0"), ((0, 2), "B1"), ((2, 0), "A0"), ((2, 0), "A1")],
            "b": [(k, name) for k in ((1, 2), (3, 2)) for name in ("A0", "A1")]
            + [(k, name) for k in ((2, 1), (2, 3)) for name in ("B0", "B1")],
            "c": [(k, name) for k in ((1, 2), (3, 2)) for name in ("B0", "B1")],
            "d": [(k, name) for k in ((2, 1), (2, 3)) for name in ("A0", "A1")],
            "e": [((2, 2), name) for name in ("A0", "A1", "B0", "B1")],
        }
        ports = {}

        def port(step, name):
            key = (slot(step), name)
            for group, members in quads.items():
                if any(key == (slot(k), other) for k, other in members):
                    key = group
            return ports.setdefault(key, len(ports))

        def landed_all(group):
            count = len(quads[group])
            k, name = quads[group][0]
            arrived(cols.at[0 : count * quarter, :], gat_r.at[port(k, name)])

        def piece_of(step, name):
            first, count = spans[name]
            base = slot(step) * half + first * quarter
            return cols.at[base : base + count * quarter, :]

        def forward(step, name, *directions):
            for way in directions:
                move = ahead[way]
                lands = (step[0] - move[0], step[1] - move[1])
                push(piece_of(step, name), piece_of(lands, name), gat_s,
                     gat_r.at[port(lands, name)], {"dp": shift(move)})

        def landed(step, name):
            arrived(piece_of(step, name), gat_r.at[port(step, name)])

        for way in ("Y-", "Y+"):
            forward((0, 0), "A", way)
        for way in ("Z-", "Z+"):
            forward((0, 0), "B", way)
        for way in ("Y-", "Y+"):
            forward((0, 0), "B", way)
        for way in ("Z-", "Z+"):
            forward((0, 0), "A", way)

        for load in loads[2:]:
            load.wait()
        mult = scale_ref[0]
        mult2 = mult * LOG2E
        h_own[s] = hidden[tile(e, chunk), :]
        mate = (1 - s) * n_mp + m
        push(hidden.at[tile(mate, chunk), :], h_own.at[s], h_s, h_r, {"section": 1 - s})
        w_in, w_out = wi_all.at[e], wo_all.at[e]
        ww = ((w_in, wi_all), (w_out, wo_all))
        z_at, y_at = d // RING, lax.rem(d, RING)
        cell = (z_at * RING + y_at, y_at * RING + z_at)
        band = (z_at, y_at)
        cross = far(2) * CORES + core
        bit = w_in.shape[0] // n_dp

        def along(which, step):
            return {"dp": shift((0, step) if which == 0 else (step, 0))}

        for which in (0, 1):
            part = tile(cell[which], bit)
            push(ww[which][0].at[part, :], ww[which][1].at[e, part, :], wc_s.at[which],
                 wc_r.at[which, 0], at(far(2), core))
        depth = w_in.shape[0]
        whole = (pl.ds(0, depth // 2), pl.ds(depth // 2, depth // 2))
        early = (pl.ds(0, depth // 4),)
        later = (pl.ds(depth // 4, depth // 4), pl.ds(depth // 2, depth // 2))

        def neighbour(which, toward, part):
            push(ww[which][0].at[part, :], ww[which][1].at[e, part, :], ww_s.at[which],
                 ww_r.at[which, 1 if toward == 1 else 0], at(far(toward), core))

        def both_ways(which, parts):
            for part in parts:
                neighbour(which, line - 1, part)
                neighbour(which, 1, part)

        both_ways(0, whole)
        both_ways(1, early)

        for which in (0, 1):
            push(ww[which][0], ww[which][1].at[e], ww_s.at[which], ww_r.at[which, 2],
                 at(spot, sib))

        def cross_first(which):
            mine_bit = ww[which][1].at[cross, tile(cell[which], bit), :]
            arrived(mine_bit, wc_r.at[which, 0])
            for k in range(1, RING):
                push(mine_bit, mine_bit, wc_s.at[which], wc_r.at[which, 1],
                     along(which, k))

        def cross_second(which):
            arrived(ww[which][1].at[cross, 0 : (RING - 1) * bit, :], wc_r.at[which, 1])
            group = ww[which][1].at[cross, tile(band[which], RING * bit), :]
            for k in range(1, RING):
                push(group, group, wc_s.at[which], wc_r.at[which, 2],
                     along(1 - which, k))

        def cross_third(which):
            arrived(ww[which][1].at[cross, 0 : (RING - 1) * RING * bit, :], wc_r.at[which, 2])
            push(ww[which][1].at[cross], ww[which][1].at[cross], ww_s.at[which],
                 ww_r.at[which, 2 if which else 3], at(spot, sib))

        def relay_weight(which, step):
            index = far(step) * CORES + core
            buf = ww[which][1].at[index]
            arrived(buf, ww_r.at[which, 0 if step == 1 else 1])
            push(buf, buf, ww_s.at[which], ww_r.at[which, 2], at(spot, sib))

        def sigmoid(pre):
            return 1.0 / (1.0 + jnp.exp(-GELU * pre))

        with jax.named_scope("b_pre"):
            loads[1].wait()
            for i, hop in enumerate(hops):
                unit, _ = unit_rows(text[tile(far(hop), pair), :])
                text_low[i * pair : (i + 1) * pair, :] = unit.astype(BF16)

            @pl.loop(0, line)
            def _(r):
                pre = dot_nn(hidden[tile(r, pair), :], w_in[...])
                sigm = sigmoid(pre)
                act_all[tile(r, pair), :] = (pre * sigm).astype(BF16)
                slope_all[tile(r, pair), :] = sigm + GELU * pre * sigm * (1.0 - sigm)

        def group_scores(*group, fresh=False):
            piece = [cols[slot(k) * half : (slot(k) + 1) * half, :] for k in group]
            piece = piece[0] if len(piece) == 1 else jnp.concatenate(piece, axis=0)
            peak = total = None
            for r in range(line):
                part = pl.ds(r * pair, pair)
                value = mult2 * dot_nt(text_low[part, :], piece)
                blocks = [value[:, k * half : (k + 1) * half] for k in range(len(group))]
                for k, block in zip(group, blocks):
                    scores[slot(k), part, :] = block
                best = blocks[0]
                for block in blocks[1:]:
                    best = jnp.maximum(best, block)
                if not fresh:
                    best = jnp.maximum(best, row_max[part, :])
                    mass = row_sum[part, :] * jnp.exp2(row_max[part, :] - best)
                    for block in blocks:
                        mass = mass + jnp.exp2(block - best)
                    row_sum[part, :] = mass
                else:
                    row_sum[part, :] = jnp.ones(best.shape, F32)
                row_max[part, :] = best
                high = jnp.max(value, axis=0, keepdims=True)
                if peak is None:
                    peak = high
                    total = jnp.sum(jnp.exp2(value - peak), axis=0, keepdims=True)
                else:
                    high = jnp.maximum(peak, high)
                    total = total * jnp.exp2(peak - high) + jnp.sum(
                        jnp.exp2(value - high), axis=0, keepdims=True)
                    peak = high
            level = peak + jnp.log(total) * LOG2E
            for k, step in enumerate(group):
                p = shift(step)
                col_st[pl.ds(p, 1), :] = level[:, k * half : (k + 1) * half]

        with jax.named_scope("c_own"):
            group_scores((0, 0), fresh=True)

        with jax.named_scope("c_blocks"):
            landed((0, 1), "A")
            forward((0, 1), "A0", "Y-")
            landed((1, 0), "B")
            forward((1, 0), "B0", "Z-")
            landed((0, 3), "A")
            forward((0, 3), "A1", "Y+")
            landed((3, 0), "B")
            forward((3, 0), "B1", "Z+")
            for dy in (1, 3):
                forward((0, dy), "A", "Z-", "Z+")
            for dz in (1, 3):
                forward((dz, 0), "B", "Y-", "Y+")
            landed((0, 1), "B")
            forward((0, 1), "B0", "Y-")
            landed((1, 0), "A")
            forward((1, 0), "A0", "Z-")
            landed((0, 3), "B")
            forward((0, 3), "B1", "Y+")
            landed((3, 0), "A")
            forward((3, 0), "A1", "Z+")
            group_scores((0, 1), (0, 3))
            group_scores((1, 0), (3, 0))
            for name in ("A0", "A1"):
                landed((0, 2), name)
                forward((0, 2), name, "Z-", "Z+")
            for name in ("B0", "B1"):
                landed((2, 0), name)
                forward((2, 0), name, "Y-", "Y+")
            for dy in (1, 3):
                landed((1, dy), "A")
                forward((1, dy), "A0", "Z-")
                landed((3, dy), "A")
                forward((3, dy), "A1", "Z+")
            for dz in (1, 3):
                landed((dz, 1), "B")
                forward((dz, 1), "B0", "Y-")
                landed((dz, 3), "B")
                forward((dz, 3), "B1", "Y+")
            cross_first(0)
            cross_first(1)
            group_scores((1, 1), (1, 3))
            group_scores((3, 1), (3, 3))
            landed_all("a")
            group_scores((0, 2), (2, 0))
            landed_all("b")
            forward((1, 2), "A0", "Z-")
            forward((3, 2), "A1", "Z+")
            forward((2, 1), "B0", "Y-")
            forward((2, 3), "B1", "Y+")
            landed_all("c")
            group_scores((1, 2), (3, 2))
            landed_all("d")
            group_scores((2, 1), (2, 3))
            landed_all("e")
            group_scores((2, 2))

        with jax.named_scope("d_colsend"):
            col_rx[d] = col_st[...]
            for p in others(d, n_dp):
                push(col_st, col_rx.at[d], cs_s, cs_r, {"dp": p})

        with jax.named_scope("e_rowstat"):
            for r in range(n_el):
                part = pl.ds(r * chunk, chunk)
                place = far(hops[r // CORES]) * CORES + r % CORES
                peak = jnp.max(row_max[part, :], axis=1, keepdims=True)
                acc = jnp.sum(row_sum[part, :] * jnp.exp2(row_max[part, :] - peak), axis=1,
                              keepdims=True)
                level = peak + jnp.log(acc) * LOG2E
                row_st[pl.ds(place, 1), :] = jnp.broadcast_to(level, (chunk, LANES)).T[0:1, :]
            row_rx[e] = row_st[...]
            for q in others(e, n_el):
                push(row_st, row_rx.at[e], rs_s, rs_r,
                     {"section": q // n_mp, "mp": lax.rem(q, n_mp)})
            both_ways(1, later)

        def merge(rx, count):
            peak = rx[0]
            for k in range(1, count):
                peak = jnp.maximum(peak, rx[k])
            acc = jnp.zeros(peak.shape, F32)
            for k in range(count):
                acc = acc + jnp.exp2(rx[k] - peak)
            return peak + (jnp.log(acc) * LOG2E + 1.0)

        def slopes(index):
            pre = dot_nn(h_own[index // n_mp], wi_all[index])
            sigm = sigmoid(pre)
            slope_own[index] = sigm + GELU * pre * sigm * (1.0 - sigm)

        with jax.named_scope("f_cross"):
            cross_second(0)
            cross_second(1)
            relay_weight(0, 1)
            relay_weight(0, line - 1)
            arrived(h_own.at[1 - s], h_r)
            for step in (0, 1, line - 1):
                slopes(far(step) * CORES + core)

        with jax.named_scope("f_rows"):
            arrived(row_rx.at[0 : n_el - 1], rs_r)
            row_mix[...] = merge(row_rx, n_el)
            for r in range(n_el):
                part = slice(r * chunk, (r + 1) * chunk)
                place = far(hops[r // CORES]) * CORES + r % CORES
                base = jnp.broadcast_to(row_mix[pl.ds(place, 1), :], (LANES, chunk)).T
                for k in range(n_dp):
                    row_part[k, part, :] = jnp.exp2(scores[k, part, :] - base)

        with jax.named_scope("f_merge"):
            arrived(col_rx.at[0 : n_dp - 1], cs_r)
            col_lse[...] = merge(col_rx, n_dp)

        def score_rows(i):
            part = slice(i * pair, (i + 1) * pair)
            offset = (m - far(hops[i])) * pair + s * half
            for step in steps:
                k = slot(step)
                value = scores[k, part, :]
                low = col_lse[pl.ds(shift(step), 1), :]
                both = row_part[k, part, :] + jnp.exp2(value - low)
                if k == 0:
                    diagonal = lax.broadcasted_iota(jnp.int32, (pair, half), 0) == (
                        lax.broadcasted_iota(jnp.int32, (pair, half), 1) + offset)
                    both = both - jnp.where(diagonal, 1.0, 0.0)
                sgrad[part, k * half : (k + 1) * half] = both.astype(BF16)

        def join(where):
            arrived(t_sr.at[where], ts_r.at[where])
            return t_keep[where] + t_sr[where].astype(F32)


        with jax.named_scope("g_scorerows"):
            score_rows(0)
            for i, hop in enumerate(hops):
                where = far(hop)
                t_full[...] = dot_nn(sgrad[i * pair : (i + 1) * pair, :], cols[...])
                if i + 1 < line:
                    score_rows(i + 1)
                t_sx[where] = t_full[tile(sib, chunk), :].astype(BF16)
                push(t_sx.at[where], t_sr.at[where], ts_s, ts_r.at[where], at(spot, sib))
                t_keep[where] = t_full[tile(core, chunk), :]
                if i > 0:
                    last = far(hops[i - 1])
                    t_tx[last] = join(last).astype(BF16)
                    push(t_tx.at[last], t_rx.at[spot - (spot > last).astype(jnp.int32)], tc_s, tc_r,
                         at(last, core))

        with jax.named_scope("g_relay"):
            cross_third(0)
            cross_third(1)

        fold = half // 2

        with jax.named_scope("h_image"):
            for g in (2, 1, 3, 0):
                part = dot_tn(sgrad[:, g * RING * half : (g + 1) * RING * half], text_low[...])
                for k in range(RING):
                    low = part[k * half : k * half + fold, :]
                    high = part[k * half + fold : (k + 1) * half, :]
                    if g == 0:
                        i_own[0, k] = low
                    else:
                        i_tx[0, g, k] = low.astype(BF16)
                    if k == 0:
                        i_own[1, g] = high
                    else:
                        i_tx[1, k, g] = high.astype(BF16)
                if g > 0:
                    push(i_tx.at[0, g], i_rx.at[0, RING - g], im_s, im_r.at[0, 0], along(1, g))
                for k in (2, 1, 3):
                    push(i_tx.at[1, k, g], i_rx.at[1, RING - k, g], im_s, im_r.at[1, 0],
                         along(0, k))
                if g == 1:
                    relay_weight(1, 1)
                    relay_weight(1, line - 1)

        def image_second():
            for which in (0, 1):
                arrived(i_rx.at[which, 1:RING], im_r.at[which, 0])
                for g in (2, 1, 3, 0):
                    total = i_own[which, g]
                    for k in range(1, RING):
                        total = total + i_rx[which, k, g].astype(F32)
                    if g == 0:
                        i_own[which, 0] = total
                    else:
                        i_st[which, g] = total.astype(BF16)
                        push(i_st.at[which, g], i_end.at[which, RING - g],
                             im_s, im_r.at[which, 1], along(which, g))

        mine = tile(e, chunk)

        with jax.named_scope("j_weights"):
            arrived(wi_all.at[0:3], ww_r.at[0, 2])
            for step in (0, 1, line - 1):
                slopes(far(step) * CORES + sib)
            slopes(cross)
            arrived(wi_all.at[0], ww_r.at[0, 3])
            slopes(far(2) * CORES + sib)
            arrived(wo_all.at[0:line], ww_r.at[1, 2])

        with jax.named_scope("i_topgrad"):
            total = join(spot)
            arrived(t_rx.at[0 : line - 1], tc_r)
            for k in range(line - 1):
                total = total + t_rx[k].astype(F32)
            unit, length = unit_rows(text[mine, :])
            g_st[n_sec - 1] = unit_backward(unit, length, mult * total).astype(BF16)

        def spread(layer):
            for step in (2, 1, 3) if line == 4 else range(1, line):
                place = far(step)

                @pl.when(place // chips == layer)
                def _():
                    copy(g_st.at[layer], g_all.at[e], gs_s, gs_r.at[e], at(place, core)).start()

            @pl.when(s == layer)
            def _():
                g_all[e] = g_st[layer]
                copy(g_st.at[layer], g_all.at[e], gs_s, gs_r.at[e],
                     at(spot, sib)).start()

        def feed_forward(layer):
            first = layer * n_mp
            total = g_st[layer].astype(F32)
            grads = []
            for j in range(n_mp):
                back = dot_nt(g_st[layer], wo_all[first + j])
                grads.append((back * slope_own[first + j]).astype(BF16))
            for j in range(n_mp):
                total = total + dot_nt(grads[j], wi_all[first + j])
            if layer > 0:
                g_st[layer - 1] = total.astype(BF16)
                spread(layer - 1)
            else:
                for t in range(n_sec):
                    in_st[t] = total[:, t * width : (t + 1) * width].astype(BF16)

        def slab(k):
            return input_out.at[tile(k, chunk), :]

        with jax.named_scope("k_ffn"):
            for layer in range(n_sec - 1, -1, -1):
                feed_forward(layer)
                if layer == n_sec - 1:
                    spread(layer)

        def weight_rows(k):
            back = dot_nt(g_all[k], w_out[...])
            pre_all[tile(k, chunk), :] = (back * slope_all[tile(k, chunk), :]).astype(BF16)

        with jax.named_scope("m_weightrows"):
            weight_rows(e)
            for hop in (1, 3, 2) if line == 4 else range(1, line):
                index = far(hop) * CORES + core
                arrived(g_all.at[index], gs_r.at[index])
                push(g_all.at[index], g_all.at[index], gs_s, gs_r.at[index],
                     at(spot, sib))
                weight_rows(index)
            input_out[mine, :] = in_st[s]
            push(in_st.at[s], slab(e), in_s, in_r.at[0], at(spot, sib))
            for hop in hops[:-1]:
                where = far(hop)
                push(in_st.at[where // chips], slab(e), in_s, in_r.at[line - hop],
                     at(where, core))
            image_second()
            for hop in (0, 1, 3, 2) if line == 4 else range(line):
                index = far(hop) * CORES + sib
                arrived(g_all.at[index], gs_r.at[index])
                weight_rows(index)

        def send_weights(which):
            for k in (2, 1, 3):
                other = lax.rem(band[which] + k, RING)
                push(w_tx.at[which, tile(other, RING * share), :], w_rx.at[which, RING - k],
                     w_s, w_r.at[which, 0], along(1 - which, k))

        def weight_second(which):
            total = w_full[which, tile(band[which], RING * share), :]
            arrived(w_rx.at[which, 1:RING], w_r.at[which, 0])
            for k in (1, 3, 2):
                total = total + w_rx[which, k].astype(F32)
            w_sum[which] = total
            w_st[which] = total.astype(BF16)
            for k in (2, 1, 3):
                other = lax.rem(band[1 - which] + k, RING)
                push(w_st.at[which, tile(other, share), :], w_end.at[which, RING - k],
                     w_s, w_r.at[which, 1], along(which, k))

        def weight_last(which, out):
            total = w_sum[which, tile(band[1 - which], share), :]
            arrived(w_end.at[which, 1:RING], w_r.at[which, 1])
            for k in (1, 3, 2):
                total = total + w_end[which, k].astype(F32)
            out[...] = total

        with jax.named_scope("n_wgrad"):
            g_rows = g_all[...].reshape(rows, feats)
            grad = dot_tn(g_rows, act_all[...])
            for p in range(n_dp):
                q = (p % RING) * RING + p // RING
                w_full[1, q * share : (q + 1) * share, :] = grad[p * share : (p + 1) * share, :]
                w_tx[1, q * share : (q + 1) * share, :] = grad[
                    p * share : (p + 1) * share, :].astype(BF16)
            send_weights(1)
            grad = dot_tn(hidden[...], pre_all[...])
            w_full[0] = grad
            w_tx[0] = grad.astype(BF16)
            send_weights(0)

        with jax.named_scope("q_image"):
            image_half = tile(s, half)
            unit, length = unit_rows(image[...])
            for which in (0, 1):
                total = i_own[which, 0]
                arrived(i_end.at[which, 1:RING], im_r.at[which, 1])
                for k in (1, 3, 2):
                    total = total + i_end[which, k].astype(F32)
                part = slice(which * fold, (which + 1) * fold)
                image_out[tile(2 * s + which, fold), :] = unit_backward(
                    unit[part, :], length[part, :], mult * total).astype(BF16)
            push(image_out.at[image_half, :], image_out.at[image_half, :], io_s, io_r,
                 {"section": 1 - s})

        with jax.named_scope("o_inrelay"):
            for hop in hops[:-1]:
                index = far(hop) * CORES + core
                arrived(slab(index), in_r.at[hop])
                push(slab(index), slab(index), in_s, in_r.at[0], at(spot, sib))

        with jax.named_scope("p_wsecond"):
            weight_second(1)
            weight_second(0)

        with jax.named_scope("q_wsum"):
            weight_last(1, second_out)
            weight_last(0, first_out)

        with jax.named_scope("r_drain"):
            arrived(input_out.at[0 : line * chunk, :], in_r.at[0])
            arrived(image_out.at[tile(1 - s, half), :], io_r)
            left(hidden.at[0:chunk, :], h_s)
            left(cols.at[0 : 15 * half, :], gat_s)
            left(col_rx.at[0 : n_dp - 1], cs_s)
            left(row_rx.at[0 : n_el - 1], rs_s)
            for which in (0, 1):
                left(ww[which][1].at[0:6], ww_s.at[which])
                left(ww[which][1].at[0], wc_s.at[which])
            left(t_sx, ts_s)
            left(t_tx.at[0 : line - 1], tc_s)
            left(g_all.at[0 : 2 * n_sec + line - 1], gs_s)
            left(input_out.at[0 : (2 * line - 1) * chunk, :], in_s)
            left(text.at[0 : 2 * (RING - 1) * (RING + 1) * share, :], w_s)
            left(cols.at[0 : 15 * half, :], im_s)
            left(image_out.at[0:half, :], io_s)

    return kernel


def solution(mesh):
    n_sec, n_dp, n_mp = mesh.shape["section"], mesh.shape["dp"], mesh.shape["mp"]

    def body(text, image, scale, hidden, w_in, w_out):
        rows, feats = text.shape
        own = image.shape[0]
        hid = w_in.shape[2]
        half, share = own // n_sec, feats // n_dp
        columns = half * n_dp
        line = n_sec * n_mp // CORES
        n_el = n_sec * n_mp
        chunk = rows // n_el
        dma = pltpu.SemaphoreType.DMA
        vmem = pl.BlockSpec(memory_space=pltpu.VMEM)
        hbm = pl.BlockSpec(memory_space=pltpu.HBM)
        out = pl.pallas_call(
            make_kernel(n_sec, n_dp, n_mp),
            out_shape=(
                pltpu.VMEM((own, feats), BF16),
                pltpu.VMEM((rows, feats // n_sec), BF16),
                pltpu.VMEM((share, hid), F32),
                pltpu.VMEM((share, hid), F32),
            ),
            in_specs=[hbm, hbm, hbm, hbm, hbm, hbm],
            out_specs=(vmem,) * 4,
            scratch_shapes=[
                pltpu.SMEM((1,), F32),
                pltpu.VMEM((rows, feats), BF16),
                pltpu.VMEM((half, feats), BF16),
                pltpu.VMEM((rows, feats), BF16),
                pltpu.VMEM((rows, feats), BF16),
                pltpu.VMEM((columns, feats), BF16),
                pltpu.VMEM((n_dp, rows, half), F32),
                pltpu.VMEM((rows, columns), BF16),
                pltpu.VMEM((rows, LANES), F32),
                pltpu.VMEM((rows, LANES), F32),
                pltpu.VMEM((n_dp, rows, half), F32),
                pltpu.VMEM((n_dp, half), F32),
                pltpu.VMEM((n_el, chunk), F32),
                pltpu.VMEM((n_el, n_el, chunk), F32),
                pltpu.VMEM((n_el, chunk), F32),
                pltpu.VMEM((n_dp, half), F32),
                pltpu.VMEM((n_dp, n_dp, half), F32),
                pltpu.VMEM((n_el, feats, hid), BF16),
                pltpu.VMEM((n_el, hid, feats), BF16),
                pltpu.VMEM((n_sec, chunk, feats), BF16),
                pltpu.VMEM((CORES * chunk, feats), F32),
                pltpu.VMEM((line, chunk, feats), F32),
                pltpu.VMEM((line, chunk, feats), BF16),
                pltpu.VMEM((line, chunk, feats), BF16),
                pltpu.VMEM((line, chunk, feats), BF16),
                pltpu.VMEM((line, chunk, feats), BF16),
                pltpu.VMEM((n_sec, chunk, feats), BF16),
                pltpu.VMEM((n_el, chunk, feats), BF16),
                pltpu.VMEM((n_el, chunk, hid), F32),
                pltpu.VMEM((n_sec, chunk, feats // n_sec), BF16),
                pltpu.VMEM((rows, hid), BF16),
                pltpu.VMEM((rows, hid), F32),
                pltpu.VMEM((rows, hid), BF16),
                pltpu.VMEM((2, feats, hid), F32),
                pltpu.VMEM((2, feats, hid), BF16),
                pltpu.VMEM((2, RING, RING * share, hid), BF16),
                pltpu.VMEM((2, RING * share, hid), F32),
                pltpu.VMEM((2, RING * share, hid), BF16),
                pltpu.VMEM((2, RING, share, hid), BF16),
                pltpu.VMEM((2, RING, RING, half // 2, feats), BF16),
                pltpu.VMEM((2, RING, RING, half // 2, feats), BF16),
                pltpu.VMEM((2, RING, half // 2, feats), F32),
                pltpu.VMEM((2, RING, half // 2, feats), BF16),
                pltpu.VMEM((2, RING, half // 2, feats), BF16),
                dma, dma((25,)), dma, dma, dma, dma, dma((2,)), dma((2, 4)), dma, dma,
                dma, dma((line,)), dma, dma, dma, dma((n_el,)), dma, dma((line,)),
                dma((6,)), dma((2,)), dma((2, 3)), dma, dma((2, 2)), dma, dma((2, 2)), dma, dma,
            ],
            compiler_params=pltpu.CompilerParams(
                collective_id=0, has_side_effects=True, vmem_limit_bytes=62000000
            ),
        )(text, image, scale, hidden[0], w_in[0], w_out[0])
        image_grad, input_grad, first, second = pl.pallas_call(
            leave,
            out_shape=tuple(jax.ShapeDtypeStruct(x.shape, x.dtype) for x in out),
            in_specs=[vmem] * 4,
            out_specs=(hbm,) * 4,
            scratch_shapes=[dma((4,))],
            compiler_params=pltpu.CompilerParams(vmem_limit_bytes=4000000),
        )(*out)
        return (image_grad, input_grad, first[None], second[None])

    return jax.shard_map(
        body,
        mesh=mesh,
        in_specs=(
            P("dp", None),
            P(("dp", "mp"), None),
            P(),
            P("section", "dp", None),
            P("section", None, "mp"),
            P("section", "mp", None),
        ),
        out_specs=(
            P(("dp", "mp"), None),
            P("dp", "section"),
            P("section", "dp", "mp"),
            P("section", "dp", "mp"),
        ),
        check_vma=False,
    )
```

```python
import jax
import jax.numpy as jnp
from jax import lax
from jax.experimental import pallas as pl
from jax.experimental.pallas import tpu as pltpu
from jax.sharding import PartitionSpec as P

MESH = pl.DeviceIdType.MESH
F32 = jnp.float32
BF16 = jnp.bfloat16
GELU = 1.702
LOG2E = 1.4426950408889634
LANES = 128
CORES = 2
RING = 4


def unit_rows(values):
    wide = values.astype(F32)
    length = jnp.sqrt(jnp.sum(wide * wide, axis=1, keepdims=True) + 1.0)
    return (wide / length, length)


def unit_backward(unit, length, grad_unit):
    return (grad_unit - unit * jnp.sum(unit * grad_unit, axis=1, keepdims=True)) / length


def dot_nn(a, b):
    return lax.dot_general(a, b, (((1,), (0,)), ((), ())), preferred_element_type=F32)


def dot_nt(a, b):
    return lax.dot_general(a, b, (((1,), (1,)), ((), ())), preferred_element_type=F32)


def dot_tn(a, b):
    return lax.dot_general(a, b, (((0,), (0,)), ((), ())), preferred_element_type=F32)


def tile(index, size):
    return pl.ds(pl.multiple_of(index * size, size), size)


def leave(*refs):
    copies = [pltpu.make_async_copy(refs[k], refs[4 + k], refs[8].at[k]) for k in range(4)]
    for c in copies:
        c.start()
    for c in copies:
        c.wait()


def make_kernel(n_sec, n_dp, n_mp):
    chips = n_mp // CORES
    line = n_sec * chips
    n_el = n_sec * n_mp

    def kernel(
        text_hbm, image_hbm, scale_hbm, hidden_hbm, w_in_hbm, w_out_hbm,
        image_out, input_out, first_out, second_out,
        scale_ref, text, image, hidden, text_low, cols, scores, sgrad, row_max, row_sum, row_part, col_lse, row_st, row_rx, row_mix, col_st, col_rx,
        wi_all, wo_all, h_own, t_full, t_keep, t_sx, t_sr, t_tx, t_rx,
        g_st, g_all, slope_own, in_st, act_all, slope_all, pre_all,
        w_full, w_tx, w_rx, w_sum, w_st, w_end, i_tx, i_rx, i_own, i_st, i_end,
        gat_s, gat_r, cs_s, cs_r, rs_s, rs_r, ww_s, ww_r, h_s, h_r,
        ts_s, ts_r, tc_s, tc_r, gs_s, gs_r, in_s, in_r,
        ld_s, wc_s, wc_r, w_s, w_r, im_s, im_r, io_s, io_r,
    ):
        s = lax.axis_index("section")
        d = lax.axis_index("dp")
        m = lax.axis_index("mp")
        rows, feats = text.shape
        own = image_hbm.shape[0]
        half = own // n_sec
        chunk = rows // n_el
        pair = rows // line
        share = feats // n_dp
        width = feats // n_sec
        core = lax.rem(m, CORES)
        sib = 1 - core
        spot = s * chips + m // CORES
        e = s * n_mp + m

        def at(place, who):
            return {"section": place // chips, "mp": lax.rem(place, chips) * CORES + who}

        def far(step):
            return lax.rem(spot + step, line)

        def copy(src, dst, send, recv, where):
            return pltpu.make_async_remote_copy(
                src_ref=src, dst_ref=dst, send_sem=send, recv_sem=recv,
                device_id=where, device_id_type=MESH,
            )

        def arrived(ref, recv):
            copy(ref, ref, h_s, recv, at(spot, sib)).wait_recv()

        def shift(step):
            dz, dy = step[0] % RING, step[1] % RING
            z = lax.rem(d // RING + dz, RING)
            return z * RING + lax.rem(lax.rem(d, RING) + dy, RING)

        def slot(step):
            return (step[0] % RING) * RING + step[1] % RING

        steps = [(a, b) for a in range(RING) for b in range(RING)]

        def away(step):
            return (-step[0] % RING, -step[1] % RING)

        hops = (2, 3, 1, 0) if line == 4 else tuple(range(line - 1, -1, -1))

        def others(mine, count):
            return [lax.rem(mine + k, count) for k in range(1, count)]

        def sources(mine, count):
            return [lax.rem(mine + count - k, count) for k in range(1, count)]

        def push(*args):
            copy(*args).start()

        def left(ref, send):
            copy(ref, ref, send, h_r, at(spot, sib)).wait_send()

        with jax.named_scope("a_barrier"):
            loads = [
                pltpu.make_async_copy(src, dst, ld_s.at[k])
                for k, (src, dst) in enumerate((
                    (image_hbm.at[tile(s, half), :], image), (text_hbm, text), (hidden_hbm, hidden),
                    (w_in_hbm, wi_all.at[e]), (w_out_hbm, wo_all.at[e]), (scale_hbm, scale_ref),
                ))
            ]
            for load in loads:
                load.start()
            barrier = pltpu.get_barrier_semaphore()
            for near in ((0, 1), (0, -1), (1, 0), (-1, 0)):
                pl.semaphore_signal(
                    barrier, inc=1, device_id={"dp": shift(near)}, device_id_type=MESH)
            for q in others(e, n_el):
                pl.semaphore_signal(
                    barrier, inc=1, device_id={"section": q // n_mp, "mp": lax.rem(q, n_mp)},
                    device_id_type=MESH,
                )
            loads[0].wait()
            own_unit, _ = unit_rows(image[...])
            cols[0:half, :] = own_unit.astype(BF16)
            pl.semaphore_wait(barrier, n_el + 3)

        quarter = half // 4
        spans = {"A": (0, 2), "B": (2, 2), "A0": (0, 1), "A1": (1, 1), "B0": (2, 1), "B1": (3, 1)}
        ahead = {"Y-": (0, -1), "Y+": (0, 1), "Z-": (-1, 0), "Z+": (1, 0)}
        quads = {
            "a": [((0, 2), "B0"), ((0, 2), "B1"), ((2, 0), "A0"), ((2, 0), "A1")],
            "b": [(k, name) for k in ((1, 2), (3, 2)) for name in ("A0", "A1")]
            + [(k, name) for k in ((2, 1), (2, 3)) for name in ("B0", "B1")],
            "c": [(k, name) for k in ((1, 2), (3, 2)) for name in ("B0", "B1")],
            "d": [(k, name) for k in ((2, 1), (2, 3)) for name in ("A0", "A1")],
            "e": [((2, 2), name) for name in ("A0", "A1", "B0", "B1")],
        }
        ports = {}

        def port(step, name):
            key = (slot(step), name)
            for group, members in quads.items():
                if any(key == (slot(k), other) for k, other in members):
                    key = group
            return ports.setdefault(key, len(ports))

        def landed_all(group):
            count = len(quads[group])
            k, name = quads[group][0]
            arrived(cols.at[0 : count * quarter, :], gat_r.at[port(k, name)])

        def piece_of(step, name):
            first, count = spans[name]
            base = slot(step) * half + first * quarter
            return cols.at[base : base + count * quarter, :]

        def forward(step, name, *directions):
            for way in directions:
                move = ahead[way]
                lands = (step[0] - move[0], step[1] - move[1])
                push(piece_of(step, name), piece_of(lands, name), gat_s,
                     gat_r.at[port(lands, name)], {"dp": shift(move)})

        def landed(step, name):
            arrived(piece_of(step, name), gat_r.at[port(step, name)])

        for way in ("Y-", "Y+"):
            forward((0, 0), "A", way)
        for way in ("Z-", "Z+"):
            forward((0, 0), "B", way)
        for way in ("Y-", "Y+"):
            forward((0, 0), "B", way)
        for way in ("Z-", "Z+"):
            forward((0, 0), "A", way)

        for load in loads[2:]:
            load.wait()
        mult = scale_ref[0]
        mult2 = mult * LOG2E
        h_own[s] = hidden[tile(e, chunk), :]
        mate = (1 - s) * n_mp + m
        push(hidden.at[tile(mate, chunk), :], h_own.at[s], h_s, h_r, {"section": 1 - s})
        w_in, w_out = wi_all.at[e], wo_all.at[e]
        ww = ((w_in, wi_all), (w_out, wo_all))
        z_at, y_at = d // RING, lax.rem(d, RING)
        cell = (z_at * RING + y_at, y_at * RING + z_at)
        band = (z_at, y_at)
        cross = far(2) * CORES + core
        bit = w_in.shape[0] // n_dp

        def along(which, step):
            return {"dp": shift((0, step) if which == 0 else (step, 0))}

        for which in (0, 1):
            part = tile(cell[which], bit)
            push(ww[which][0].at[part, :], ww[which][1].at[e, part, :], wc_s.at[which],
                 wc_r.at[which, 0], at(far(2), core))
        depth = w_in.shape[0]
        whole = (pl.ds(0, depth // 2), pl.ds(depth // 2, depth // 2))
        early = (pl.ds(0, depth // 4),)
        later = (pl.ds(depth // 4, depth // 4), pl.ds(depth // 2, depth // 2))

        def neighbour(which, toward, part):
            push(ww[which][0].at[part, :], ww[which][1].at[e, part, :], ww_s.at[which],
                 ww_r.at[which, 1 if toward == 1 else 0], at(far(toward), core))

        def both_ways(which, parts):
            for part in parts:
                neighbour(which, line - 1, part)
                neighbour(which, 1, part)

        both_ways(0, whole)
        both_ways(1, early)

        for which in (0, 1):
            push(ww[which][0], ww[which][1].at[e], ww_s.at[which], ww_r.at[which, 2],
                 at(spot, sib))

        def cross_first(which):
            mine_bit = ww[which][1].at[cross, tile(cell[which], bit), :]
            arrived(mine_bit, wc_r.at[which, 0])
            for k in range(1, RING):
                push(mine_bit, mine_bit, wc_s.at[which], wc_r.at[which, 1],
                     along(which, k))

        def cross_second(which):
            arrived(ww[which][1].at[cross, 0 : (RING - 1) * bit, :], wc_r.at[which, 1])
            group = ww[which][1].at[cross, tile(band[which], RING * bit), :]
            for k in range(1, RING):
                push(group, group, wc_s.at[which], wc_r.at[which, 2],
                     along(1 - which, k))

        def cross_third(which):
            arrived(ww[which][1].at[cross, 0 : (RING - 1) * RING * bit, :], wc_r.at[which, 2])
            push(ww[which][1].at[cross], ww[which][1].at[cross], ww_s.at[which],
                 ww_r.at[which, 2 if which else 3], at(spot, sib))

        def relay_weight(which, step):
            index = far(step) * CORES + core
            buf = ww[which][1].at[index]
            arrived(buf, ww_r.at[which, 0 if step == 1 else 1])
            push(buf, buf, ww_s.at[which], ww_r.at[which, 2], at(spot, sib))

        def sigmoid(pre):
            return 1.0 / (1.0 + jnp.exp(-GELU * pre))

        with jax.named_scope("b_pre"):
            loads[1].wait()
            for i, hop in enumerate(hops):
                unit, _ = unit_rows(text[tile(far(hop), pair), :])
                text_low[i * pair : (i + 1) * pair, :] = unit.astype(BF16)

            @pl.loop(0, line)
            def _(r):
                pre = dot_nn(hidden[tile(r, pair), :], w_in[...])
                sigm = sigmoid(pre)
                act_all[tile(r, pair), :] = (pre * sigm).astype(BF16)
                slope_all[tile(r, pair), :] = sigm + GELU * pre * sigm * (1.0 - sigm)

        def group_scores(*group, fresh=False):
            piece = [cols[slot(k) * half : (slot(k) + 1) * half, :] for k in group]
            piece = piece[0] if len(piece) == 1 else jnp.concatenate(piece, axis=0)
            peak = total = None
            for r in range(line):
                part = pl.ds(r * pair, pair)
                value = mult2 * dot_nt(text_low[part, :], piece)
                blocks = [value[:, k * half : (k + 1) * half] for k in range(len(group))]
                for k, block in zip(group, blocks):
                    scores[slot(k), part, :] = block
                best = blocks[0]
                for block in blocks[1:]:
                    best = jnp.maximum(best, block)
                if not fresh:
                    best = jnp.maximum(best, row_max[part, :])
                    mass = row_sum[part, :] * jnp.exp2(row_max[part, :] - best)
                    for block in blocks:
                        mass = mass + jnp.exp2(block - best)
                    row_sum[part, :] = mass
                else:
                    row_sum[part, :] = jnp.ones(best.shape, F32)
                row_max[part, :] = best
                high = jnp.max(value, axis=0, keepdims=True)
                if peak is None:
                    peak = high
                    total = jnp.sum(jnp.exp2(value - peak), axis=0, keepdims=True)
                else:
                    high = jnp.maximum(peak, high)
                    total = total * jnp.exp2(peak - high) + jnp.sum(
                        jnp.exp2(value - high), axis=0, keepdims=True)
                    peak = high
            level = peak + jnp.log(total) * LOG2E
            for k, step in enumerate(group):
                p = shift(step)
                col_st[pl.ds(p, 1), :] = level[:, k * half : (k + 1) * half]

        with jax.named_scope("c_own"):
            group_scores((0, 0), fresh=True)

        with jax.named_scope("c_blocks"):
            landed((0, 1), "A")
            forward((0, 1), "A0", "Y-")
            landed((1, 0), "B")
            forward((1, 0), "B0", "Z-")
            landed((0, 3), "A")
            forward((0, 3), "A1", "Y+")
            landed((3, 0), "B")
            forward((3, 0), "B1", "Z+")
            for dy in (1, 3):
                forward((0, dy), "A", "Z-", "Z+")
            for dz in (1, 3):
                forward((dz, 0), "B", "Y-", "Y+")
            landed((0, 1), "B")
            forward((0, 1), "B0", "Y-")
            landed((1, 0), "A")
            forward((1, 0), "A0", "Z-")
            landed((0, 3), "B")
            forward((0, 3), "B1", "Y+")
            landed((3, 0), "A")
            forward((3, 0), "A1", "Z+")
            group_scores((0, 1), (0, 3))
            group_scores((1, 0), (3, 0))
            for name in ("A0", "A1"):
                landed((0, 2), name)
                forward((0, 2), name, "Z-", "Z+")
            for name in ("B0", "B1"):
                landed((2, 0), name)
                forward((2, 0), name, "Y-", "Y+")
            for dy in (1, 3):
                landed((1, dy), "A")
                forward((1, dy), "A0", "Z-")
                landed((3, dy), "A")
                forward((3, dy), "A1", "Z+")
            for dz in (1, 3):
                landed((dz, 1), "B")
                forward((dz, 1), "B0", "Y-")
                landed((dz, 3), "B")
                forward((dz, 3), "B1", "Y+")
            cross_first(0)
            cross_first(1)
            group_scores((1, 1), (1, 3))
            group_scores((3, 1), (3, 3))
            landed_all("a")
            group_scores((0, 2), (2, 0))
            landed_all("b")
            forward((1, 2), "A0", "Z-")
            forward((3, 2), "A1", "Z+")
            forward((2, 1), "B0", "Y-")
            forward((2, 3), "B1", "Y+")
            landed_all("c")
            group_scores((1, 2), (3, 2))
            landed_all("d")
            group_scores((2, 1), (2, 3))
            landed_all("e")
            group_scores((2, 2))

        with jax.named_scope("d_colsend"):
            col_rx[d] = col_st[...]
            for p in others(d, n_dp):
                push(col_st, col_rx.at[d], cs_s, cs_r, {"dp": p})

        with jax.named_scope("e_rowstat"):
            for r in range(n_el):
                part = pl.ds(r * chunk, chunk)
                place = far(hops[r // CORES]) * CORES + r % CORES
                peak = jnp.max(row_max[part, :], axis=1, keepdims=True)
                acc = jnp.sum(row_sum[part, :] * jnp.exp2(row_max[part, :] - peak), axis=1,
                              keepdims=True)
                level = peak + jnp.log(acc) * LOG2E
                row_st[pl.ds(place, 1), :] = jnp.broadcast_to(level, (chunk, LANES)).T[0:1, :]
            row_rx[e] = row_st[...]
            for q in others(e, n_el):
                push(row_st, row_rx.at[e], rs_s, rs_r,
                     {"section": q // n_mp, "mp": lax.rem(q, n_mp)})
            both_ways(1, later)

        def merge(rx, count):
            peak = rx[0]
            for k in range(1, count):
                peak = jnp.maximum(peak, rx[k])
            acc = jnp.zeros(peak.shape, F32)
            for k in range(count):
                acc = acc + jnp.exp2(rx[k] - peak)
            return peak + (jnp.log(acc) * LOG2E + 1.0)

        def slopes(index):
            pre = dot_nn(h_own[index // n_mp], wi_all[index])
            sigm = sigmoid(pre)
            slope_own[index] = sigm + GELU * pre * sigm * (1.0 - sigm)

        with jax.named_scope("f_cross"):
            cross_second(0)
            cross_second(1)
            relay_weight(0, 1)
            relay_weight(0, line - 1)
            arrived(h_own.at[1 - s], h_r)
            for step in (0, 1, line - 1):
                slopes(far(step) * CORES + core)

        with jax.named_scope("f_rows"):
            arrived(row_rx.at[0 : n_el - 1], rs_r)
            row_mix[...] = merge(row_rx, n_el)
            for r in range(n_el):
                part = slice(r * chunk, (r + 1) * chunk)
                place = far(hops[r // CORES]) * CORES + r % CORES
                base = jnp.broadcast_to(row_mix[pl.ds(place, 1), :], (LANES, chunk)).T
                for k in range(n_dp):
                    row_part[k, part, :] = jnp.exp2(scores[k, part, :] - base)

        with jax.named_scope("f_merge"):
            arrived(col_rx.at[0 : n_dp - 1], cs_r)
            col_lse[...] = merge(col_rx, n_dp)

        def score_rows(i):
            part = slice(i * pair, (i + 1) * pair)
            offset = (m - far(hops[i])) * pair + s * half
            for step in steps:
                k = slot(step)
                value = scores[k, part, :]
                low = col_lse[pl.ds(shift(step), 1), :]
                both = row_part[k, part, :] + jnp.exp2(value - low)
                if k == 0:
                    diagonal = lax.broadcasted_iota(jnp.int32, (pair, half), 0) == (
                        lax.broadcasted_iota(jnp.int32, (pair, half), 1) + offset)
                    both = both - jnp.where(diagonal, 1.0, 0.0)
                sgrad[part, k * half : (k + 1) * half] = both.astype(BF16)

        def join(where):
            arrived(t_sr.at[where], ts_r.at[where])
            return t_keep[where] + t_sr[where].astype(F32)


        with jax.named_scope("g_scorerows"):
            score_rows(0)
            for i, hop in enumerate(hops):
                where = far(hop)
                t_full[...] = dot_nn(sgrad[i * pair : (i + 1) * pair, :], cols[...])
                if i + 1 < line:
                    score_rows(i + 1)
                t_sx[where] = t_full[tile(sib, chunk), :].astype(BF16)
                push(t_sx.at[where], t_sr.at[where], ts_s, ts_r.at[where], at(spot, sib))
                t_keep[where] = t_full[tile(core, chunk), :]
                if i > 0:
                    last = far(hops[i - 1])
                    t_tx[last] = join(last).astype(BF16)
                    push(t_tx.at[last], t_rx.at[spot - (spot > last).astype(jnp.int32)], tc_s, tc_r,
                         at(last, core))

        with jax.named_scope("g_relay"):
            cross_third(0)
            cross_third(1)

        fold = half // 2

        with jax.named_scope("h_image"):
            for g in (2, 1, 3, 0):
                part = dot_tn(sgrad[:, g * RING * half : (g + 1) * RING * half], text_low[...])
                for k in range(RING):
                    low = part[k * half : k * half + fold, :]
                    high = part[k * half + fold : (k + 1) * half, :]
                    if g == 0:
                        i_own[0, k] = low
                    else:
                        i_tx[0, g, k] = low.astype(BF16)
                    if k == 0:
                        i_own[1, g] = high
                    else:
                        i_tx[1, k, g] = high.astype(BF16)
                if g > 0:
                    push(i_tx.at[0, g], i_rx.at[0, RING - g], im_s, im_r.at[0, 0], along(1, g))
                for k in (2, 1, 3):
                    push(i_tx.at[1, k, g], i_rx.at[1, RING - k, g], im_s, im_r.at[1, 0],
                         along(0, k))
                if g == 1:
                    relay_weight(1, 1)
                    relay_weight(1, line - 1)

        def image_second():
            for which in (0, 1):
                arrived(i_rx.at[which, 1:RING], im_r.at[which, 0])
                for g in (2, 1, 3, 0):
                    total = i_own[which, g]
                    for k in range(1, RING):
                        total = total + i_rx[which, k, g].astype(F32)
                    if g == 0:
                        i_own[which, 0] = total
                    else:
                        i_st[which, g] = total.astype(BF16)
                        push(i_st.at[which, g], i_end.at[which, RING - g],
                             im_s, im_r.at[which, 1], along(which, g))

        mine = tile(e, chunk)

        with jax.named_scope("j_weights"):
            arrived(wi_all.at[0:3], ww_r.at[0, 2])
            for step in (0, 1, line - 1):
                slopes(far(step) * CORES + sib)
            slopes(cross)
            arrived(wi_all.at[0], ww_r.at[0, 3])
            slopes(far(2) * CORES + sib)
            arrived(wo_all.at[0:line], ww_r.at[1, 2])

        with jax.named_scope("i_topgrad"):
            total = join(spot)
            arrived(t_rx.at[0 : line - 1], tc_r)
            for k in range(line - 1):
                total = total + t_rx[k].astype(F32)
            unit, length = unit_rows(text[mine, :])
            g_st[n_sec - 1] = unit_backward(unit, length, mult * total).astype(BF16)

        def spread(layer):
            for step in (2, 1, 3) if line == 4 else range(1, line):
                place = far(step)

                @pl.when(place // chips == layer)
                def _():
                    copy(g_st.at[layer], g_all.at[e], gs_s, gs_r.at[e], at(place, core)).start()

            @pl.when(s == layer)
            def _():
                g_all[e] = g_st[layer]
                copy(g_st.at[layer], g_all.at[e], gs_s, gs_r.at[e],
                     at(spot, sib)).start()

        def feed_forward(layer):
            first = layer * n_mp
            total = g_st[layer].astype(F32)
            grads = []
            for j in range(n_mp):
                back = dot_nt(g_st[layer], wo_all[first + j])
                grads.append((back * slope_own[first + j]).astype(BF16))
            for j in range(n_mp):
                total = total + dot_nt(grads[j], wi_all[first + j])
            if layer > 0:
                g_st[layer - 1] = total.astype(BF16)
                spread(layer - 1)
            else:
                for t in range(n_sec):
                    in_st[t] = total[:, t * width : (t + 1) * width].astype(BF16)

        def slab(k):
            return input_out.at[tile(k, chunk), :]

        with jax.named_scope("k_ffn"):
            for layer in range(n_sec - 1, -1, -1):
                feed_forward(layer)
                if layer == n_sec - 1:
                    spread(layer)

        def weight_rows(k):
            back = dot_nt(g_all[k], w_out[...])
            pre_all[tile(k, chunk), :] = (back * slope_all[tile(k, chunk), :]).astype(BF16)

        def some_rows(steps, who):
            places = [far(step) * CORES + who for step in steps]
            g_rows = jnp.concatenate([g_all[k] for k in places], axis=0)
            act = jnp.concatenate([act_all[tile(k, chunk), :] for k in places], axis=0)
            hid_rows = jnp.concatenate([hidden[tile(k, chunk), :] for k in places], axis=0)
            pre = jnp.concatenate([pre_all[tile(k, chunk), :] for k in places], axis=0)
            return (lambda: dot_tn(hid_rows, pre), lambda: dot_tn(g_rows, act))

        with jax.named_scope("m_weightrows"):
            weight_rows(e)
            image_second()
            for hop in (1, 3, 2) if line == 4 else range(1, line):
                index = far(hop) * CORES + core
                arrived(g_all.at[index], gs_r.at[index])
                push(g_all.at[index], g_all.at[index], gs_s, gs_r.at[index],
                     at(spot, sib))
                weight_rows(index)
            input_out[mine, :] = in_st[s]
            push(in_st.at[s], slab(e), in_s, in_r.at[0], at(spot, sib))
            for hop in hops[:-1]:
                where = far(hop)
                push(in_st.at[where // chips], slab(e), in_s, in_r.at[line - hop],
                     at(where, core))
            ours = some_rows(range(line), core)
            for which in (1, 0):
                w_full[which] = ours[which]()
            for hop in (0, 1, 3, 2) if line == 4 else range(line):
                index = far(hop) * CORES + sib
                arrived(g_all.at[index], gs_r.at[index])
                weight_rows(index)

        def send_weights(which):
            for k in (2, 1, 3):
                other = lax.rem(band[which] + k, RING)
                push(w_tx.at[which, tile(other, RING * share), :], w_rx.at[which, RING - k],
                     w_s, w_r.at[which, 0], along(1 - which, k))

        def weight_second(which):
            total = w_full[which, tile(band[which], RING * share), :]
            arrived(w_rx.at[which, 1:RING], w_r.at[which, 0])
            for k in (1, 3, 2):
                total = total + w_rx[which, k].astype(F32)
            w_sum[which] = total
            w_st[which] = total.astype(BF16)
            for k in (2, 1, 3):
                other = lax.rem(band[1 - which] + k, RING)
                push(w_st.at[which, tile(other, share), :], w_end.at[which, RING - k],
                     w_s, w_r.at[which, 1], along(which, k))

        def weight_last(which, out):
            total = w_sum[which, tile(band[1 - which], share), :]
            arrived(w_end.at[which, 1:RING], w_r.at[which, 1])
            for k in (1, 3, 2):
                total = total + w_end[which, k].astype(F32)
            out[...] = total

        with jax.named_scope("n_wgrad"):
            theirs = some_rows(range(line), sib)
            grad = w_full[1] + theirs[1]()
            for p in range(n_dp):
                q = (p % RING) * RING + p // RING
                w_full[1, q * share : (q + 1) * share, :] = grad[p * share : (p + 1) * share, :]
                w_tx[1, q * share : (q + 1) * share, :] = grad[
                    p * share : (p + 1) * share, :].astype(BF16)
            send_weights(1)
            grad = w_full[0] + theirs[0]()
            w_full[0] = grad
            w_tx[0] = grad.astype(BF16)
            send_weights(0)

        with jax.named_scope("q_image"):
            image_half = tile(s, half)
            unit, length = unit_rows(image[...])
            for which in (0, 1):
                total = i_own[which, 0]
                arrived(i_end.at[which, 1:RING], im_r.at[which, 1])
                for k in (1, 3, 2):
                    total = total + i_end[which, k].astype(F32)
                part = slice(which * fold, (which + 1) * fold)
                image_out[tile(2 * s + which, fold), :] = unit_backward(
                    unit[part, :], length[part, :], mult * total).astype(BF16)
            push(image_out.at[image_half, :], image_out.at[image_half, :], io_s, io_r,
                 {"section": 1 - s})

        with jax.named_scope("o_inrelay"):
            for hop in hops[:-1]:
                index = far(hop) * CORES + core
                arrived(slab(index), in_r.at[hop])
                push(slab(index), slab(index), in_s, in_r.at[0], at(spot, sib))

        with jax.named_scope("p_wsecond"):
            weight_second(1)
            weight_second(0)

        with jax.named_scope("q_wsum"):
            weight_last(1, second_out)
            weight_last(0, first_out)

        with jax.named_scope("r_drain"):
            arrived(input_out.at[0 : line * chunk, :], in_r.at[0])
            arrived(image_out.at[tile(1 - s, half), :], io_r)
            left(hidden.at[0:chunk, :], h_s)
            left(cols.at[0 : 15 * half, :], gat_s)
            left(col_rx.at[0 : n_dp - 1], cs_s)
            left(row_rx.at[0 : n_el - 1], rs_s)
            for which in (0, 1):
                left(ww[which][1].at[0:6], ww_s.at[which])
                left(ww[which][1].at[0], wc_s.at[which])
            left(t_sx, ts_s)
            left(t_tx.at[0 : line - 1], tc_s)
            left(g_all.at[0 : 2 * n_sec + line - 1], gs_s)
            left(input_out.at[0 : (2 * line - 1) * chunk, :], in_s)
            left(text.at[0 : 2 * (RING - 1) * (RING + 1) * share, :], w_s)
            left(cols.at[0 : 15 * half, :], im_s)
            left(image_out.at[0:half, :], io_s)

    return kernel


def solution(mesh):
    n_sec, n_dp, n_mp = mesh.shape["section"], mesh.shape["dp"], mesh.shape["mp"]

    def body(text, image, scale, hidden, w_in, w_out):
        rows, feats = text.shape
        own = image.shape[0]
        hid = w_in.shape[2]
        half, share = own // n_sec, feats // n_dp
        columns = half * n_dp
        line = n_sec * n_mp // CORES
        n_el = n_sec * n_mp
        chunk = rows // n_el
        dma = pltpu.SemaphoreType.DMA
        vmem = pl.BlockSpec(memory_space=pltpu.VMEM)
        hbm = pl.BlockSpec(memory_space=pltpu.HBM)
        out = pl.pallas_call(
            make_kernel(n_sec, n_dp, n_mp),
            out_shape=(
                pltpu.VMEM((own, feats), BF16),
                pltpu.VMEM((rows, feats // n_sec), BF16),
                pltpu.VMEM((share, hid), F32),
                pltpu.VMEM((share, hid), F32),
            ),
            in_specs=[hbm, hbm, hbm, hbm, hbm, hbm],
            out_specs=(vmem,) * 4,
            scratch_shapes=[
                pltpu.SMEM((1,), F32),
                pltpu.VMEM((rows, feats), BF16),
                pltpu.VMEM((half, feats), BF16),
                pltpu.VMEM((rows, feats), BF16),
                pltpu.VMEM((rows, feats), BF16),
                pltpu.VMEM((columns, feats), BF16),
                pltpu.VMEM((n_dp, rows, half), F32),
                pltpu.VMEM((rows, columns), BF16),
                pltpu.VMEM((rows, LANES), F32),
                pltpu.VMEM((rows, LANES), F32),
                pltpu.VMEM((n_dp, rows, half), F32),
                pltpu.VMEM((n_dp, half), F32),
                pltpu.VMEM((n_el, chunk), F32),
                pltpu.VMEM((n_el, n_el, chunk), F32),
                pltpu.VMEM((n_el, chunk), F32),
                pltpu.VMEM((n_dp, half), F32),
                pltpu.VMEM((n_dp, n_dp, half), F32),
                pltpu.VMEM((n_el, feats, hid), BF16),
                pltpu.VMEM((n_el, hid, feats), BF16),
                pltpu.VMEM((n_sec, chunk, feats), BF16),
                pltpu.VMEM((CORES * chunk, feats), F32),
                pltpu.VMEM((line, chunk, feats), F32),
                pltpu.VMEM((line, chunk, feats), BF16),
                pltpu.VMEM((line, chunk, feats), BF16),
                pltpu.VMEM((line, chunk, feats), BF16),
                pltpu.VMEM((line, chunk, feats), BF16),
                pltpu.VMEM((n_sec, chunk, feats), BF16),
                pltpu.VMEM((n_el, chunk, feats), BF16),
                pltpu.VMEM((n_el, chunk, hid), F32),
                pltpu.VMEM((n_sec, chunk, feats // n_sec), BF16),
                pltpu.VMEM((rows, hid), BF16),
                pltpu.VMEM((rows, hid), F32),
                pltpu.VMEM((rows, hid), BF16),
                pltpu.VMEM((2, feats, hid), F32),
                pltpu.VMEM((2, feats, hid), BF16),
                pltpu.VMEM((2, RING, RING * share, hid), BF16),
                pltpu.VMEM((2, RING * share, hid), F32),
                pltpu.VMEM((2, RING * share, hid), BF16),
                pltpu.VMEM((2, RING, share, hid), BF16),
                pltpu.VMEM((2, RING, RING, half // 2, feats), BF16),
                pltpu.VMEM((2, RING, RING, half // 2, feats), BF16),
                pltpu.VMEM((2, RING, half // 2, feats), F32),
                pltpu.VMEM((2, RING, half // 2, feats), BF16),
                pltpu.VMEM((2, RING, half // 2, feats), BF16),
                dma, dma((25,)), dma, dma, dma, dma, dma((2,)), dma((2, 4)), dma, dma,
                dma, dma((line,)), dma, dma, dma, dma((n_el,)), dma, dma((line,)),
                dma((6,)), dma((2,)), dma((2, 3)), dma, dma((2, 2)), dma, dma((2, 2)), dma, dma,
            ],
            compiler_params=pltpu.CompilerParams(
                collective_id=0, has_side_effects=True, vmem_limit_bytes=62000000
            ),
        )(text, image, scale, hidden[0], w_in[0], w_out[0])
        image_grad, input_grad, first, second = pl.pallas_call(
            leave,
            out_shape=tuple(jax.ShapeDtypeStruct(x.shape, x.dtype) for x in out),
            in_specs=[vmem] * 4,
            out_specs=(hbm,) * 4,
            scratch_shapes=[dma((4,))],
            compiler_params=pltpu.CompilerParams(vmem_limit_bytes=4000000),
        )(*out)
        return (image_grad, input_grad, first[None], second[None])

    return jax.shard_map(
        body,
        mesh=mesh,
        in_specs=(
            P("dp", None),
            P(("dp", "mp"), None),
            P(),
            P("section", "dp", None),
            P("section", None, "mp"),
            P("section", "mp", None),
        ),
        out_specs=(
            P(("dp", "mp"), None),
            P("dp", "section"),
            P("section", "dp", "mp"),
            P("section", "dp", "mp"),
        ),
        check_vma=False,
    )
```
